32 devices in a mesh: dp: 16 (over z, y, core), tensor: 2 (over x).
Axes of the slice: x: 2, y: 2, z: 4, core: 2. Of those that a mesh axis runs over, the one named last changes fastest.
Arguments:
- inputs: bfloat16 [32768, 512], P(('dp', 'tensor')), may hold values from -6 to 6
- norm_scale: float32 [2, 512], replicated, may hold values from 0.1 to 1.9
- norm_shift: float32 [2, 512], replicated, may hold values from -3 to 3
- head_weight: bfloat16 [3, 512, 512], P(None, None, 'tensor'), may hold values from -0.25 to 0.25
- query_bias: float32 [512], P('tensor'), may hold values from -3 to 3
- value_bias: float32 [512], P('tensor'), may hold values from -0.3 to 0.3
- out_weight: bfloat16 [512, 512], P('tensor'), may hold values from -4 to 4
- out_bias: float32 [512], replicated, may hold values from -2 to 2
- up_weight: bfloat16 [512, 2048], P(None, 'tensor'), may hold values from -0.25 to 0.25
- up_bias: float32 [2048], P('tensor'), may hold values from -3 to 3
- down_weight: bfloat16 [2048, 512], P('tensor'), may hold values from -0.125 to 0.125
- down_bias: float32 [512], replicated, may hold values from -2 to 2
- cotangent: bfloat16 [32768, 512], P(('dp', 'tensor')), may hold values from -6 to 6
Outputs:
- layer_out: bfloat16 [32768, 512], P(('dp', 'tensor'))
- input_grad: bfloat16 [32768, 512], P(('dp', 'tensor'))
- norm_scale_grad: float32 [2, 512], replicated
- norm_shift_grad: float32 [2, 512], replicated
- head_weight_grad: float32 [3, 512, 512], P(None, None, 'tensor')
- query_bias_grad: float32 [512], P('tensor')
- value_bias_grad: float32 [512], P('tensor')
- out_weight_grad: float32 [512, 512], P('tensor')
- out_bias_grad: float32 [512], replicated
- up_weight_grad: float32 [512, 2048], P(None, 'tensor')
- up_bias_grad: float32 [2048], P('tensor')
- down_weight_grad: float32 [2048, 512], P('tensor')
- down_bias_grad: float32 [512], replicated
The draws below stay inside these ranges and needn't reach their ends.
All inputs are finite; a program needn't handle non-finite values.
Results may differ from the reference program's by a relative error of at most 0.012.
Values may be sent and summed in bfloat16 or wider, within the bound.
A program may use at most 192 MiB of HBM per device.

```python
import jax
import jax.numpy as jnp
from jax import lax

D = 512
H = 8
HD = 64
FF = 2048
LEN = 1024
BLK = 256
HD_ALL = 512
TOKENS = 32768
SEQS = 32


def steps_of(stream_key, dims, cuts, least, top_value):
    loudness, own = 1.0, jax.random.fold_in(stream_key, 6)
    for dim, shards_of in cuts:
        draws = jnp.exp(jax.random.uniform(jax.random.fold_in(own, dim), (shards_of,), jnp.float32, least / len(cuts), top_value / len(cuts)))
        loudness = loudness * jnp.repeat(draws, dims[dim] // shards_of).reshape([-1 if axis == dim else 1 for axis in range(len(dims))])
    return loudness


def gaussian(own_key, shape, width, most, split=(), held_as=jnp.bfloat16):
    array = width * jax.random.normal(own_key, shape, jnp.float32)
    if split:
        array = array * steps_of(own_key, shape, split, -0.22, 0.18)
    return jnp.clip(array, -most, most).astype(held_as)


def setup_inputs(seed: int = 0) -> dict:
    splits = jax.random.split(jax.random.key(seed), 14)
    inputs = gaussian(splits[0], (TOKENS, D), 1.0, 6.0, ((0, 32),))
    norm_scale = jnp.clip(1.0 + 0.18 * jax.random.normal(splits[1], (2, D), jnp.float32), 0.1, 1.9)
    norm_shift = gaussian(splits[2], (2, D), 0.5, 3.0, (), jnp.float32)
    head_weight = gaussian(splits[3], (3, D, HD_ALL), D ** -0.5, 0.25, ((2, 2),))
    query_bias = gaussian(splits[4], (HD_ALL,), 0.5, 3.0, ((0, 2),), jnp.float32)
    value_bias = gaussian(splits[5], (HD_ALL,), 0.05, 0.3, ((0, 2),), jnp.float32)
    out_weight = gaussian(splits[6], (HD_ALL, D), (max(1, HD_ALL // 256)) ** -0.5, 4.0, ((0, 2),))
    out_bias = gaussian(splits[7], (D,), 0.3, 2.0, (), jnp.float32)
    up_weight = gaussian(splits[8], (D, FF), D ** -0.5, 0.25, ((1, 2),))
    up_bias = gaussian(splits[9], (FF,), 0.5, 3.0, ((0, 2),), jnp.float32)
    down_weight = gaussian(splits[10], (FF, D), FF ** -0.5, 0.125, ((0, 2),))
    down_bias = gaussian(splits[11], (D,), 0.3, 2.0, (), jnp.float32)
    cotangent = gaussian(splits[12], (TOKENS, D), 1.0, 6.0, ((0, 32),))
    return {"inputs": inputs, "norm_scale": norm_scale, "norm_shift": norm_shift, "head_weight": head_weight, "query_bias": query_bias, "value_bias": value_bias, "out_weight": out_weight, "out_bias": out_bias, "up_weight": up_weight, "up_bias": up_bias, "down_weight": down_weight, "down_bias": down_bias, "cotangent": cotangent}


@jax.custom_vjp
def low(v):
    return lax.optimization_barrier(v.astype(jnp.bfloat16)).astype(jnp.float32)

@jax.custom_vjp
def low_back(v):
    return v

def low_keep(v):
    return (low(v), None)

def low_pass(kept, grad):
    return (grad,)

def back_keep(v):
    return (v, None)

def back_low(kept, grad):
    return (low(grad),)
low.defvjp(low_keep, low_pass)
low_back.defvjp(back_keep, back_low)

def layer_norm(values, gain, shift):
    center = lax.optimization_barrier(jnp.mean(values, -1, keepdims=True))
    centered = values - center
    spread = lax.optimization_barrier(jnp.mean(centered * centered, -1, keepdims=True))
    return centered * lax.rsqrt(spread + 1e-05) * gain + shift

def layer(rows, norm_scale, norm_shift, head_weight, query_bias, value_bias, out_weight, out_bias, up_weight, up_bias, down_weight, down_bias):
    highest = lax.Precision.HIGHEST
    normed = low(layer_norm(rows, norm_scale[0], norm_shift[0]))
    queries = low_back(low(jnp.dot(normed, head_weight[0], precision=highest) + query_bias))
    key_rows = low_back(low(jnp.dot(normed, head_weight[1], precision=highest)))
    values = low_back(low(jnp.dot(normed, head_weight[2], precision=highest) + value_bias))

    def to_heads(table):
        return table.reshape(LEN, H, HD)
    scores = low_back(jnp.einsum('qhd,khd->hqk', to_heads(queries), to_heads(key_rows), precision=highest) * HD ** (-0.5))
    place = jnp.arange(LEN).astype(jnp.int32) // BLK
    allowed = place[None, :] <= place[:, None]
    masked = jnp.where(allowed[None], scores, -1e+30)
    largest = lax.optimization_barrier(jnp.max(masked, -1, keepdims=True))
    powers = jnp.exp(masked - largest)
    attn_probs = low(powers / lax.optimization_barrier(jnp.sum(powers, -1, keepdims=True)))
    mixed = jnp.einsum('hqk,khd->qhd', attn_probs, to_heads(values), precision=highest).reshape(LEN, H * HD)
    mixed = low_back(low(mixed))
    branch = low_back(jnp.dot(mixed, out_weight, precision=highest) + out_bias)
    residual = rows + branch
    normed_two = low(layer_norm(residual, norm_scale[1], norm_shift[1]))
    pre_act = low_back(jnp.dot(normed_two, up_weight, precision=highest) + up_bias)
    activated = low(jax.nn.gelu(pre_act, approximate=True))
    branch_two = low_back(jnp.dot(activated, down_weight, precision=highest) + down_bias)
    return residual + branch_two

def reference(inputs, norm_scale, norm_shift, head_weight, query_bias, value_bias, out_weight, out_bias, up_weight, up_bias, down_weight, down_bias, cotangent):
    params = (norm_scale.astype(jnp.float32), norm_shift.astype(jnp.float32), head_weight.astype(jnp.float32), query_bias.astype(jnp.float32), value_bias.astype(jnp.float32), out_weight.astype(jnp.float32), out_bias.astype(jnp.float32), up_weight.astype(jnp.float32), up_bias.astype(jnp.float32), down_weight.astype(jnp.float32), down_bias.astype(jnp.float32))
    seq_inputs = inputs.astype(jnp.float32).reshape(SEQS, LEN, D)
    seq_grads = cotangent.astype(jnp.float32).reshape(SEQS, LEN, D)

    def one_sequence(carry, pair):
        rows, grad_rows = pair
        result, pull = jax.vjp(layer, rows, *params)
        grads = pull(grad_rows)
        summed = tuple((carry[index] + grads[index + 1] for index in range(len(params))))
        return (summed, (result, grads[0]))
    start = tuple((jnp.zeros_like(param) for param in params))
    totals, outputs = lax.scan(one_sequence, start, (seq_inputs, seq_grads))
    results, input_grads = outputs
    return (results.reshape(TOKENS, D).astype(jnp.bfloat16), input_grads.reshape(TOKENS, D).astype(jnp.bfloat16), totals[0], totals[1], totals[2], totals[3], totals[4], totals[5], totals[6], totals[7], totals[8], totals[9], totals[10])
```

```python
from functools import partial

import jax
import jax.numpy as jnp
from jax import lax
from jax.sharding import PartitionSpec as P

HD = 64
BLK = 256
EPSILON = 1e-05
F32 = jnp.float32
BF16 = jnp.bfloat16


def layer_norm(values, gain, shift):
    center = jnp.mean(values, -1, keepdims=True)
    centered = values - center
    spread = jnp.mean(centered * centered, -1, keepdims=True)
    return centered * lax.rsqrt(spread + EPSILON) * gain + shift


def split_heads(t):
    return t.reshape(t.shape[0], t.shape[1] // HD, HD).transpose(1, 0, 2)


def merge_heads(t):
    return t.transpose(1, 0, 2).reshape(t.shape[1], t.shape[0] * t.shape[2])


def local(inputs, norm_scale, norm_shift, head_weight, query_bias, value_bias, out_weight, out_bias,
          up_weight, up_bias, down_weight, down_bias, cotangent):
    dot = partial(jnp.einsum, preferred_element_type=F32)
    gather = lambda w, d: lax.all_gather(w, "tensor", axis=d, tiled=True)
    hw = gather(head_weight, 2)
    qb, vb = gather(query_bias, 0), gather(value_bias, 0)
    ow = gather(out_weight, 0)
    uw, ub, dw = gather(up_weight, 1), gather(up_bias, 0), gather(down_weight, 0)
    x = inputs.astype(F32)
    n1 = layer_norm(x, norm_scale[0], norm_shift[0]).astype(BF16)
    q = (dot("td,dc->tc", n1, hw[0]) + qb).astype(BF16)
    k = dot("td,dc->tc", n1, hw[1]).astype(BF16)
    v = (dot("td,dc->tc", n1, hw[2]) + vb).astype(BF16)
    qh, kh, vh = split_heads(q), split_heads(k), split_heads(v)
    rows = x.shape[0]
    probs, outs = [], []
    for b in range(rows // BLK):
        hi = (b + 1) * BLK
        s = dot("hqd,hkd->hqk", qh[:, b * BLK:hi], kh[:, :hi]) * HD ** -0.5
        e = jnp.exp(s - jnp.max(s, -1, keepdims=True))
        p = (e / jnp.sum(e, -1, keepdims=True)).astype(BF16)
        probs.append(p)
        outs.append(dot("hqk,hkd->hqd", p, vh[:, :hi]).astype(BF16))
    mixed = merge_heads(jnp.concatenate(outs, 1))
    residual = x + (dot("tc,cd->td", mixed, ow) + out_bias)
    n2 = layer_norm(residual, norm_scale[1], norm_shift[1]).astype(BF16)
    pre = dot("td,df->tf", n2, uw) + ub
    act, gelu_pull = jax.vjp(partial(jax.nn.gelu, approximate=True), pre)
    act = act.astype(BF16)
    layer_out = (residual + (dot("tf,fd->td", act, dw) + down_bias)).astype(BF16)
    d_dw = dot("tf,td->fd", act, cotangent)
    gf = cotangent.astype(F32)
    d_db = jnp.sum(gf, 0)
    gpre = gelu_pull(dot("td,fd->tf", cotangent, dw))[0].astype(BF16)
    d_ub = jnp.sum(gpre.astype(F32), 0)
    d_uw = dot("td,tf->df", n2, gpre)
    g2 = dot("tf,df->td", gpre, uw)
    gres, sc2, sh2 = jax.vjp(layer_norm, residual, norm_scale[1], norm_shift[1])[1](g2)
    gres = gres + gf
    br = gres.astype(BF16)
    d_ob = jnp.sum(br.astype(F32), 0)
    d_ow = dot("tc,td->cd", mixed, br)
    gm = split_heads(dot("td,cd->tc", br, ow).astype(BF16))
    gq, gk, gv = [], 0.0, 0.0
    for b in range(rows // BLK):
        hi = (b + 1) * BLK
        pad = lambda t: jnp.pad(t, ((0, 0), (0, rows - hi), (0, 0)))
        p, g = probs[b], gm[:, b * BLK:hi]
        gp = dot("hqd,hkd->hqk", g, vh[:, :hi])
        pf = p.astype(F32)
        gs = (pf * (gp - jnp.sum(pf * gp, -1, keepdims=True))).astype(BF16)
        gq.append(dot("hqk,hkd->hqd", gs, kh[:, :hi]))
        gk = gk + pad(dot("hqk,hqd->hkd", gs, qh[:, b * BLK:hi]))
        gv = gv + pad(dot("hqk,hqd->hkd", p, g))
    gq = merge_heads((jnp.concatenate(gq, 1) * HD ** -0.5).astype(BF16))
    gk = merge_heads((gk * HD ** -0.5).astype(BF16))
    gv = merge_heads(gv.astype(BF16))
    d_hw = jnp.stack([dot("td,tc->dc", n1, g) for g in (gq, gk, gv)])
    d_qb, d_vb = jnp.sum(gq.astype(F32), 0), jnp.sum(gv.astype(F32), 0)
    g1 = dot("tc,dc->td", gq, hw[0]) + dot("tc,dc->td", gk, hw[1]) + dot("tc,dc->td", gv, hw[2])
    gin, sc1, sh1 = jax.vjp(layer_norm, x, norm_scale[0], norm_shift[0])[1](g1)
    input_grad = (gres + gin).astype(BF16)
    scat = lambda g, d: lax.psum_scatter(g, "tensor", scatter_dimension=d, tiled=True)
    big = (scat(d_hw, 2), scat(d_ow, 0), scat(d_uw, 1), scat(d_dw, 0))
    big = lax.psum(big, "dp")
    small = lax.psum((jnp.stack([sc1, sc2]), jnp.stack([sh1, sh2]), d_qb, d_vb, d_ob, d_ub, d_db), ("dp", "tensor"))
    mine = lambda g: lax.dynamic_slice_in_dim(
        g, lax.axis_index("tensor") * (g.shape[0] // lax.axis_size("tensor")), g.shape[0] // lax.axis_size("tensor"))
    return (layer_out, input_grad, small[0], small[1], big[0], mine(small[2]), mine(small[3]), big[1], small[4],
            big[2], mine(small[5]), big[3], small[6])


def solution(mesh):
    in_specs = (P(("dp", "tensor"), None), P(), P(), P(None, None, "tensor"), P("tensor"), P("tensor"), P("tensor", None),
                P(), P(None, "tensor"), P("tensor"), P("tensor", None), P(), P(("dp", "tensor"), None))
    out_specs = (P(("dp", "tensor"), None), P(("dp", "tensor"), None), P(), P(), P(None, None, "tensor"), P("tensor"),
                 P("tensor"), P("tensor", None), P(), P(None, "tensor"), P("tensor"), P("tensor", None), P())
    return jax.shard_map(local, mesh=mesh, in_specs=in_specs, out_specs=out_specs, check_vma=False)
```

```python
import functools
import jax, jax.numpy as jnp
from jax import lax
from jax.experimental import pallas as pl
from jax.experimental.pallas import tpu as pltpu

F32, BF16 = jnp.float32, jnp.bfloat16
NN, NT, TN = ((1,), (0,)), ((1,), (1,)), ((0,), (0,))
EPS = 1e-5
LOG2E = 1.4426950408889634
LN2 = 0.6931471805599453
C0, C1 = 0.7978845608, 0.044715
HD, BLK = 64, 256


def dot(a, b, dims=NN):
    return lax.dot_general(a, b, (dims, ((), ())), preferred_element_type=F32)


def normed(v):
    c = jnp.mean(v, -1, keepdims=True)
    d = v - c
    r = lax.rsqrt(jnp.mean(d * d, -1, keepdims=True) + EPS)
    return d * r, r


def ln_back(g, xhat, r, gain):
    gx = g * gain
    return r * (gx - jnp.mean(gx, -1, keepdims=True) - xhat * jnp.mean(gx * xhat, -1, keepdims=True))


class Refs:
    pass


def rows_of(r):
    return pl.ds(pl.multiple_of(r * BLK, BLK), BLK)


def ln1(z):
    def body(r, c):
        xh, _ = normed(z.x[rows_of(r), :].astype(F32))
        n = (xh * z.ns[0:1, :] + z.nsh[0:1, :]).astype(BF16)
        z.n1T[:, rows_of(r)] = n.T
        return c
    lax.fori_loop(0, z.nb, body, 0)


def column(row):
    return jnp.broadcast_to(row, (8, row.shape[-1])).T[:, 0:1]


def qkv(z, s):
    n = z.n1T
    hw = z.hw
    for qb in range(z.nb):
        sl = slice(qb * BLK, (qb + 1) * BLK)
        nt = n[:, sl]
        q = dot(hw[s, 0], nt, TN) + column(z.qb[s])
        z.qT[s, :, sl] = (q * (LOG2E / 8.0)).astype(BF16)
        z.kT[s, :, sl] = dot(hw[s, 1], nt, TN).astype(BF16)
        v = (dot(hw[s, 2], nt, TN) + column(z.vb[s])).astype(BF16)
        for h in range(z.nh):
            z.vT[s, h, 0:HD, sl] = v[h * HD:(h + 1) * HD]
            z.vT[s, h, HD:HD + 16, sl] = jnp.ones((16, BLK), BF16)


def attn_fwd(z, s):
    def body(h, c):
        hr = pl.ds(pl.multiple_of(h * HD, HD), HD)
        kh = z.kT[s, hr, :].T
        for qb in range(z.nb):
            nk = BLK * (qb + 1)
            off = BLK * (qb * (qb + 1) // 2)
            sl = slice(qb * BLK, nk)
            sc = dot(kh[:nk], z.qT[s, hr, sl])
            m = jnp.max(sc, 0, keepdims=True)
            e = jnp.exp2(sc - m).astype(BF16)
            z.E[s * z.nh + h, off:off + nk, :] = e
            o = dot(z.vT[s, h, :, 0:nk], e)
            rl = 1.0 / o[HD:HD + 1]
            z.rl[s * z.nh + h, 0:1, sl] = rl
            z.mixT[s, hr, sl] = (o[0:HD] * rl).astype(BF16)
        return c
    lax.fori_loop(0, z.nh, body, 0)


def out_proj(z):
    for r in range(z.nb):
        sl = slice(r * BLK, (r + 1) * BLK)
        t = dot(z.mixT[0, :, sl], z.ow[0], TN) + dot(z.mixT[1, :, sl], z.ow[1], TN)
        res = z.x[sl, :].astype(F32) + (t + z.ob[...])
        z.res[sl, :] = res
        xh, _ = normed(res)
        z.n2[sl, :] = (xh * z.ns[1:2, :] + z.nsh[1:2, :]).astype(BF16)


def ffn(z, s, first, last):
    def body(r, c):
        rr = rows_of(r)
        n2 = z.n2[rr, :]
        ct = z.cot[rr, :]
        fh = z.ub.shape[-1]
        FC = 512
        for f in range(0, fh, FC):
            fs = slice(f, f + FC)
            u = dot(n2, z.uw[s, :, fs]) + z.ub[s, :, fs]
            da = dot(ct, z.dw[s, fs, :], NT)
            u2 = u * u
            t = jnp.tanh(u * (C0 + (C0 * C1) * u2))
            hp = 0.5 + 0.5 * t
            a = (u * hp).astype(BF16)
            gp = hp + (u * (0.5 - 0.5 * t * t)) * (C0 + (3 * C0 * C1) * u2)
            dp = (da * gp).astype(BF16)
            z.act[s, rr, fs] = a
            z.dpre[s, rr, fs] = dp
        o = dot(z.act[s, rr, :], z.dw[s])
        g = dot(z.dpre[s, rr, :], z.uw[s], NT)
        if first:
            z.oacc[rr, :] = z.res[rr, :] + (o + z.db[...])
            z.g2[rr, :] = g
        elif not last:
            z.oacc[rr, :] = z.oacc[rr, :] + o
            z.g2[rr, :] = z.g2[rr, :] + g
        else:
            z.lo[rr, :] = (z.oacc[rr, :] + o).astype(BF16)
            g2 = z.g2[rr, :] + g
            xh, rs = normed(z.res[rr, :])
            gres = ct.astype(F32) + ln_back(g2, xh, rs, z.ns[1:2, :])
            br = gres.astype(BF16)
            z.res[rr, :] = gres
            z.br[rr, :] = br
            c = (c[0] + jnp.sum(g2 * xh, 0, keepdims=True), c[1] + jnp.sum(g2, 0, keepdims=True),
                 c[2] + jnp.sum(br.astype(F32), 0, keepdims=True), c[3] + jnp.sum(ct.astype(F32), 0, keepdims=True))
        return c
    zero = jnp.zeros((1, z.ns.shape[-1]), F32)
    c = lax.fori_loop(0, z.nb, body, (zero,) * 4 if last else 0)
    if last:
        z.small[1:2, :] = c[0]
        z.small[3:4, :] = c[1]
        z.small[4:5, :] = c[2]
        z.small[5:6, :] = c[3]


def rowsum(t):
    return dot(jnp.ones((8, t.shape[-1]), BF16), t, NT)[0:1]


def d_down(z, s):
    for f in range(0, z.ub.shape[-1], 256):
        z.GD[s, f:f + 256, :] = dot(z.act[s, :, f:f + 256], z.cot[...], TN).astype(BF16)


def d_up(z, s):
    fh = z.ub.shape[-1]
    ones = jnp.ones((8, z.dpre.shape[1]), BF16)
    for f in range(0, fh, 512):
        z.GU[s, :, f:f + 512] = dot(z.n2[...], z.dpre[s, :, f:f + 512], TN).astype(BF16)
        z.small[8 + 2 * s + f // 512:9 + 2 * s + f // 512, :] = dot(ones, z.dpre[s, :, f:f + 512])[0:1]


def d_out(z):
    for s in (0, 1):
        z.GO[s] = dot(z.mixT[s], z.br[...]).astype(BF16)
        for r in range(z.nb):
            sl = slice(r * BLK, (r + 1) * BLK)
            z.gmT[s, :, sl] = dot(z.ow[s], z.br[sl, :], NT).astype(BF16)


def attn_bwd(z, s, hook=None):
    def body(h, c):
        hr = pl.ds(pl.multiple_of(h * HD, HD), HD)
        hi = s * z.nh + h
        vh = z.vT[s, h, 0:HD, :].T
        gs = (z.gmT[s, hr, :].astype(F32) * z.rl[hi]).astype(BF16)
        delta = jnp.sum(gs.astype(F32) * z.mixT[s, hr, :].astype(F32), 0, keepdims=True)
        for qb in range(z.nb):
            nk = BLK * (qb + 1)
            off = BLK * (qb * (qb + 1) // 2)
            sl = slice(qb * BLK, nk)
            gq = gs[:, sl]
            e = z.E[hi, off:off + nk, :]
            dp = dot(vh[:nk], gq)
            ds = (e.astype(F32) * (dp - delta[:, sl])).astype(BF16)
            z.dT[s, pl.ds(pl.multiple_of(h * HD, HD), HD), sl] = (dot(z.kT[s, hr, 0:nk], ds) * 0.125).astype(BF16)
            dv = dot(gq, e, NT)
            dk = dot(z.qT[s, hr, sl], ds, NT)
            if qb:
                z.dva[:, 0:nk - BLK] = z.dva[:, 0:nk - BLK] + dv[:, 0:nk - BLK]
                z.dka[:, 0:nk - BLK] = z.dka[:, 0:nk - BLK] + dk[:, 0:nk - BLK]
            z.dva[:, sl] = dv[:, nk - BLK:nk]
            z.dka[:, sl] = dk[:, nk - BLK:nk]
        z.dT[s, pl.ds(pl.multiple_of(256 + h * HD, HD), HD), :] = (z.dka[...] * LN2).astype(BF16)
        z.dT[s, pl.ds(pl.multiple_of(512 + h * HD, HD), HD), :] = z.dva[...].astype(BF16)
        if hook is not None:
            hook(h)
        return c
    lax.fori_loop(0, z.nh, body, 0)


def d_head(z, s):
    for j in range(3):
        z.GH[s, j] = dot(z.n1T[...], z.dT[s, j * 256:(j + 1) * 256, :], NT).astype(BF16)
    for i, j in enumerate((0, 2)):
        z.small[6 + s:7 + s, i * 256:(i + 1) * 256] = rowsum(z.dT[s, j * 256:(j + 1) * 256, :])


def grad_in(z):
    zero = jnp.zeros((1, z.ns.shape[-1]), F32)
    sc, sh = zero, zero
    for r in range(z.nb):
        sl = slice(r * BLK, (r + 1) * BLK)
        gT = 0.0
        for s in (0, 1):
            for j in range(3):
                gT = gT + dot(z.hw[s, j], z.dT[s, j * 256:(j + 1) * 256, sl])
        g = gT.T
        xh, rs = normed(z.x[sl, :].astype(F32))
        z.ig[sl, :] = (z.res[sl, :] + ln_back(g, xh, rs, z.ns[0:1, :])).astype(BF16)
        sc = sc + jnp.sum(g * xh, 0, keepdims=True)
        sh = sh + jnp.sum(g, 0, keepdims=True)
    z.small[0:1, :] = sc
    z.small[2:3, :] = sh


def scratch(T):
    nb = T // BLK
    V = pltpu.VMEM
    return dict(
        n1T=V((512, T), BF16), qT=V((2, 256, T), BF16), kT=V((2, 256, T), BF16), vT=V((2, 4, 80, T), BF16),
        E=V((8, BLK * nb * (nb + 1) // 2, BLK), BF16), rl=V((8, 1, T), F32), mixT=V((2, 256, T), BF16),
        res=V((T, 512), F32), n2=V((T, 512), BF16), act=V((2, T, 1024), BF16), dpre=V((2, T, 1024), BF16),
        oacc=V((T, 512), F32), g2=V((T, 512), F32), br=V((T, 512), BF16), gmT=V((2, 256, T), BF16),
        dT=V((2, 768, T), BF16), dva=V((64, T), F32), dka=V((64, T), F32))


INS = ["x", "cot", "ns", "nsh", "hw", "qb", "vb", "ow", "ob", "uw", "ub", "dw", "db"]
OUTS = ["lo", "ig", "GH", "GO", "GU", "GD", "small"]


def run_all(z):
    ln1(z)
    for s in (0, 1):
        qkv(z, s)
        attn_fwd(z, s)
    out_proj(z)
    ffn(z, 0, True, False)
    d_down(z, 0)
    d_up(z, 0)
    ffn(z, 1, False, True)
    d_down(z, 1)
    d_up(z, 1)
    d_out(z)
    attn_bwd(z, 0)
    attn_bwd(z, 1)
    d_head(z, 0)
    d_head(z, 1)
    grad_in(z)


def call(args, T, phases=None):
    scr = scratch(T)
    names = list(scr)

    def kernel(*refs):
        z = Refs()
        for n, r in zip(INS + OUTS + names, refs):
            setattr(z, n, r)
        z.nb, z.nh = T // BLK, 4
        (phases or run_all)(z)

    S = jax.ShapeDtypeStruct
    outs = [S((T, 512), BF16), S((T, 512), BF16), S((2, 3, 512, 256), BF16), S((2, 256, 512), BF16),
            S((2, 512, 1024), BF16), S((2, 1024, 512), BF16), S((16, 512), F32)]
    vm = pl.BlockSpec(memory_space=pltpu.VMEM)
    return pl.pallas_call(kernel, out_shape=outs, in_specs=[vm] * len(INS), out_specs=[vm] * len(OUTS),
                          scratch_shapes=list(scr.values()),
                          compiler_params=pltpu.CompilerParams(vmem_limit_bytes=67043328))(*args)


def local(inputs, norm_scale, norm_shift, head_weight, query_bias, value_bias, out_weight, out_bias,
          up_weight, up_bias, down_weight, down_bias, cotangent):
    T = inputs.shape[0]
    gather = lambda w: lax.all_gather(w, "tensor", axis=0)
    row = lambda b: b.reshape(b.shape[:-1] + (1, b.shape[-1]))
    args = (inputs, cotangent, norm_scale, norm_shift, gather(head_weight), row(gather(query_bias)), row(gather(value_bias)),
            gather(out_weight), row(out_bias), gather(up_weight), row(gather(up_bias)), gather(down_weight), row(down_bias))
    lo, ig, GH, GO, GU, GD, sm = call(args, T)
    scat = lambda g: lax.psum_scatter(g.astype(F32), "tensor", scatter_dimension=0)
    big = lax.psum(tuple(scat(g) for g in (GH, GO, GU, GD)), "dp")
    sm = lax.psum(sm, ("dp", "tensor"))
    t = lax.axis_index("tensor")
    qv = sm[6:8].reshape(2, 2, 256)[t]
    ub = sm[8:12].reshape(2, 1024)[t]
    return (lo, ig, sm[0:2], sm[2:4], big[0], qv[0], qv[1], big[1], sm[4], big[2], ub, big[3], sm[5])


def solution(mesh):
    P = jax.sharding.PartitionSpec
    in_specs = (P(("dp", "tensor"), None), P(), P(), P(None, None, "tensor"), P("tensor"), P("tensor"), P("tensor", None),
                P(), P(None, "tensor"), P("tensor"), P("tensor", None), P(), P(("dp", "tensor"), None))
    out_specs = (P(("dp", "tensor"), None), P(("dp", "tensor"), None), P(), P(), P(None, None, "tensor"), P("tensor"),
                 P("tensor"), P("tensor", None), P(), P(None, "tensor"), P("tensor"), P("tensor", None), P())
    return jax.shard_map(local, mesh=mesh, in_specs=in_specs, out_specs=out_specs, check_vma=False)
```

```python
import jax
import jax.numpy as jnp
from jax import lax
from jax.experimental import pallas as pl
from jax.experimental.pallas import tpu as pltpu
from jax.sharding import PartitionSpec as P

F32, BF16 = jnp.float32, jnp.bfloat16
NN, NT, TN = ((1,), (0,)), ((1,), (1,)), ((0,), (0,))
EPS = 1e-5
LOG2E = 1.4426950408889634
LN2 = 0.6931471805599453
C0, C1 = 0.7978845608, 0.044715
HD, BLK, D, HALF, FH, NH = 64, 256, 512, 256, 1024, 4
MESH = pl.DeviceIdType.MESH
VMEM_BYTES = 67043328


def dot(a, b, dims=NN):
    return lax.dot_general(a, b, (dims, ((), ())), preferred_element_type=F32)


def normed(v):
    c = jnp.mean(v, -1, keepdims=True)
    d = v - c
    r = lax.rsqrt(jnp.mean(d * d, -1, keepdims=True) + EPS)
    return d * r, r


def ln_back(g, xhat, r, gain):
    gx = g * gain
    return r * (gx - jnp.mean(gx, -1, keepdims=True) - xhat * jnp.mean(gx * xhat, -1, keepdims=True))


def rows_of(r):
    return pl.ds(pl.multiple_of(r * BLK, BLK), BLK)


def column(row):
    return jnp.broadcast_to(row, (8, row.shape[-1])).T[:, 0:1]


class Refs:
    pass


def ln1(z):
    def body(r, c):
        xh, _ = normed(z.x[rows_of(r), :].astype(F32))
        n = (xh * z.ns[0:1, :] + z.nsh[0:1, :]).astype(BF16)
        z.n1T[:, rows_of(r)] = n.T
        return c

    lax.fori_loop(0, z.nb, body, 0)


def qkv(z, s):
    qb, vb = column(z.qb[s][...]), column(z.vb[s][...])
    for b in range(z.nb):
        sl = slice(b * BLK, (b + 1) * BLK)
        nt = z.n1T[:, sl]
        q = dot(z.hw[s, 0], nt, TN) + qb
        z.qT[s, :, sl] = (q * (LOG2E / 8.0)).astype(BF16)
        z.kT[s, :, sl] = dot(z.hw[s, 1], nt, TN).astype(BF16)
        v = (dot(z.hw[s, 2], nt, TN) + vb).astype(BF16)
        for h in range(NH):
            z.vT[s, h, 0:HD, sl] = v[h * HD : (h + 1) * HD]
            z.vT[s, h, HD : HD + 16, sl] = jnp.ones((16, BLK), BF16)


def attn_fwd(z, s, hook):
    def body(h, c):
        hr = pl.ds(pl.multiple_of(h * HD, HD), HD)
        kh = z.kT[s, hr, :].T
        for b in range(z.nb):
            nk = BLK * (b + 1)
            off = BLK * (b * (b + 1) // 2)
            sl = slice(b * BLK, nk)
            sc = dot(kh[:nk], z.qT[s, hr, sl])
            m = jnp.max(sc, 0, keepdims=True)
            e = jnp.exp2(sc - m).astype(BF16)
            z.E[s * NH + h, off : off + nk, :] = e
            o = dot(z.vT[s, h, :, 0:nk], e)
            rl = 1.0 / o[HD : HD + 1]
            z.rl[s * NH + h, 0:1, sl] = rl
            z.mixT[s, hr, sl] = (o[0:HD] * rl).astype(BF16)
        hook(h)
        return c

    lax.fori_loop(0, NH, body, 0)


def out_proj(z):
    for r in range(z.nb):
        sl = slice(r * BLK, (r + 1) * BLK)
        t = dot(z.mixT[0, :, sl], z.ow[0], TN) + dot(z.mixT[1, :, sl], z.ow[1], TN)
        res = z.x[sl, :].astype(F32) + (t + z.ob[...])
        z.res[sl, :] = res
        z.oacc[sl, :] = res + z.db[...]
        xh, _ = normed(res)
        z.n2[sl, :] = (xh * z.ns[1:2, :] + z.nsh[1:2, :]).astype(BF16)


def ffn(z, s, last, hook):
    def body(r, c):
        rr = rows_of(r)
        n2 = z.n2[rr, :]
        ct = z.cot[rr, :]
        for f in range(0, FH, 512):
            fs = slice(f, f + 512)
            u = dot(n2, z.uw[s, :, fs]) + z.ub[s][:, fs]
            da = dot(ct, z.dw[s, fs, :], NT)
            u2 = u * u
            t = jnp.tanh(u * (C0 + (C0 * C1) * u2))
            hp = 0.5 + 0.5 * t
            z.act[s, rr, fs] = (u * hp).astype(BF16)
            gp = hp + (u * (0.5 - 0.5 * t * t)) * (C0 + (3 * C0 * C1) * u2)
            z.dpre[s, rr, fs] = (da * gp).astype(BF16)
        g = dot(z.dpre[s, rr, :], z.uw[s], NT)
        if not last:
            z.g2[rr, :] = g
        else:
            g2 = z.g2[rr, :] + g
            xh, rs = normed(z.res[rr, :])
            gres = ct.astype(F32) + ln_back(g2, xh, rs, z.ns[1:2, :])
            br = gres.astype(BF16)
            z.res[rr, :] = gres
            z.br[rr, :] = br
            c = (
                c[0] + jnp.sum(g2 * xh, 0, keepdims=True),
                c[1] + jnp.sum(g2, 0, keepdims=True),
                c[2] + jnp.sum(br.astype(F32), 0, keepdims=True),
                c[3] + jnp.sum(ct.astype(F32), 0, keepdims=True),
            )
        hook(r)
        return c

    zero = jnp.zeros((1, D), F32)
    c = lax.fori_loop(0, z.nb, body, (zero,) * 4 if last else 0)
    if last:
        z.sm[1:2, :] = c[0]
        z.sm[3:4, :] = c[1]
        z.sm[4:5, :] = c[2]
        z.sm[5:6, :] = c[3]


def ffn_out(z):
    for r in range(z.nb):
        rr = slice(r * BLK, (r + 1) * BLK)
        o = dot(z.act[0, rr, :], z.dw[0]) + dot(z.act[1, rr, :], z.dw[1])
        z.lo[rr, :] = (z.oacc[rr, :] + o).astype(BF16)


def d_down(z, s, part):
    n = FH // 2
    for f in range(0, n, 256):
        a = part * n + f
        z.GD[part][s][f : f + 256, :] = dot(z.act[s, :, a : a + 256], z.cot[...], TN).astype(BF16)


def d_up(z, s, part):
    n = D // 2
    w = z.n2[:, part * n : (part + 1) * n]
    for f in range(0, FH, 512):
        z.GU[part][s][:, f : f + 512] = dot(w, z.dpre[s, :, f : f + 512], TN).astype(BF16)


def d_upb(z, s):
    ones = jnp.ones((8, z.dpre.shape[1]), BF16)
    for i in range(FH // 512):
        row = 9 + 8 * s + i
        z.sm[row : row + 1, :] = dot(ones, z.dpre[s, :, i * 512 : (i + 1) * 512])[0:1]


def d_out(z, s):
    z.GO[s][...] = dot(z.mixT[s], z.br[...]).astype(BF16)


def grad_mixed(z, s):
    for r in range(z.nb):
        sl = slice(r * BLK, (r + 1) * BLK)
        z.gmT[s, :, sl] = dot(z.ow[s], z.br[sl, :], NT).astype(BF16)


def attn_bwd(z, s, hook):
    def body(h, c):
        hr = pl.ds(pl.multiple_of(h * HD, HD), HD)
        hi = s * NH + h
        vh = z.vT[s, h, 0:HD, :].T
        gs = (z.gmT[s, hr, :].astype(F32) * z.rl[hi]).astype(BF16)
        delta = jnp.sum(gs.astype(F32) * z.mixT[s, hr, :].astype(F32), 0, keepdims=True)
        for b in range(z.nb):
            nk = BLK * (b + 1)
            off = BLK * (b * (b + 1) // 2)
            sl = slice(b * BLK, nk)
            gq = gs[:, sl]
            e = z.E[hi, off : off + nk, :]
            dp = dot(vh[:nk], gq)
            ds = (e.astype(F32) * (dp - delta[:, sl])).astype(BF16)
            z.dh[0:HD, sl] = (dot(z.kT[s, hr, 0:nk], ds) * 0.125).astype(BF16)
            dv = dot(gq, e, NT)
            dk = dot(z.qT[s, hr, sl], ds, NT)
            if b:
                z.dva[:, 0 : nk - BLK] = z.dva[:, 0 : nk - BLK] + dv[:, 0 : nk - BLK]
                z.dka[:, 0 : nk - BLK] = z.dka[:, 0 : nk - BLK] + dk[:, 0 : nk - BLK]
            z.dva[:, sl] = dv[:, nk - BLK : nk]
            z.dka[:, sl] = dk[:, nk - BLK : nk]
        z.dh[HD : 2 * HD, :] = (z.dka[...] * LN2).astype(BF16)
        z.dh[2 * HD : 3 * HD, :] = z.dva[...].astype(BF16)
        for j in range(3):
            z.dT[s, pl.ds(pl.multiple_of(j * HALF + h * HD, HD), HD), :] = z.dh[j * HD : (j + 1) * HD, :]
        g = dot(z.dh[...], z.n1T[...], NT).astype(BF16)
        for q in range(4):
            z.GH[s][h, q * 192 : (q + 1) * 192, :] = g[:, q * 128 : (q + 1) * 128]
        hook(h)
        return c

    lax.fori_loop(0, NH, body, 0)


def d_headb(z, s):
    ones = jnp.ones((8, z.dT.shape[2]), BF16)
    for i, j in enumerate((0, 2)):
        row = 8 + 8 * s
        z.sm[row : row + 1, i * HALF : (i + 1) * HALF] = dot(ones, z.dT[s, j * HALF : (j + 1) * HALF, :], NT)[0:1]


def grad_in(z):
    zero = jnp.zeros((1, D), F32)
    sc, sh = zero, zero
    for r in range(z.nb):
        sl = slice(r * BLK, (r + 1) * BLK)
        g = 0.0
        for s in (0, 1):
            for j in range(3):
                g = g + dot(z.hw[s, j], z.dT[s, j * HALF : (j + 1) * HALF, sl])
        g = g.T
        xh, rs = normed(z.x[sl, :].astype(F32))
        z.ig[sl, :] = (z.res[sl, :] + ln_back(g, xh, rs, z.ns[0:1, :])).astype(BF16)
        sc = sc + jnp.sum(g * xh, 0, keepdims=True)
        sh = sh + jnp.sum(g, 0, keepdims=True)
    z.sm[0:1, :] = sc
    z.sm[2:3, :] = sh


class Comm:
    def __init__(self, ndp, send, recv, local):
        self.send, self.recv, self.local = send, recv, local
        self.count, self.local_count, self.pending = 0, 0, []
        me = lax.axis_index("dp")
        self.levels = [1 << i for i in range(ndp.bit_length() - 1)]
        self.bit = {b: (me // b) % 2 for b in self.levels}
        self.dp = {b: me + b - 2 * b * self.bit[b] for b in self.levels}
        self.peer = 1 - lax.axis_index("tensor")

    def where(self, axis):
        return {"tensor": self.peer} if axis == "t" else {"dp": self.dp[axis]}

    def barrier_signal(self):
        sem = pltpu.get_barrier_semaphore()
        for axis in ["t"] + self.levels:
            pl.semaphore_signal(sem, inc=1, device_id=self.where(axis), device_id_type=MESH)

    def barrier_wait(self):
        pl.semaphore_wait(pltpu.get_barrier_semaphore(), 1 + len(self.levels))

    def copy(self, src, dst, axis, keep=True):
        i = self.count
        self.count += 1

        def make():
            return pltpu.make_async_remote_copy(
                src_ref=src(), dst_ref=dst(), send_sem=self.send.at[i], recv_sem=self.recv.at[i],
                device_id=self.where(axis), device_id_type=MESH)

        if keep:
            self.pending.append(make)
        return make

    def here(self, src, dst):
        i = self.local_count
        self.local_count += 1
        return lambda: pltpu.make_async_copy(src(), dst(), self.local.at[i])

    def drain(self):
        for make in self.pending:
            make().wait_send()


def add_rows(dst, src, at, n, cols):
    ch = next(c for c in (384, 256, 192, 128, 96, 64, 48, 32, 16, 8, 4) if n % c == 0 and c * cols <= 49152)

    def body(i, c):
        o = pl.ds(pl.multiple_of(at + i * ch, ch), ch)
        v = dst[o, :].astype(F32) + src[pl.ds(pl.multiple_of(i * ch, ch), ch), :].astype(F32)
        dst[o, :] = v.astype(dst.dtype)
        return c

    lax.fori_loop(0, n // ch, body, 0)


def job_scratch(rows, cols, pre, extra):
    V = pltpu.VMEM
    own = [V((rows >> (k + 1), cols), BF16) for k in range(4)]
    peer = [V((rows >> (k + 1), cols), BF16) for k in range(pre)]
    return own + peer + [V((rows >> pre, cols), BF16)] + [V((rows >> 4, cols), BF16) for _ in range(extra)] + [V((rows, cols), BF16)]


class Job:
    def __init__(self, c, own, peer, refs, rows, cols, pre, out):
        lv = c.levels
        extra = len(lv) - 4
        r_own, r_peer, r_t, r_x, full = refs[:4], refs[4 : 4 + pre], refs[4 + pre], refs[5 + pre : 5 + pre + extra], refs[-1]
        lo = [0]
        for k in range(4):
            lo.append(lo[k] + c.bit[lv[k]] * (rows >> (k + 1)))
        n = [rows >> k for k in range(5)]
        at = lambda k: pl.ds(pl.multiple_of(lo[k], n[k]) if k else 0, n[k])
        away = lambda k: pl.ds(pl.multiple_of(lo[k] + (1 - c.bit[lv[k]]) * n[k + 1], n[k + 1]), n[k + 1])
        half = lambda g, buf, k: c.copy(lambda: g().at[away(k)], lambda: buf, lv[k])
        s_own = [half(own, r_own[k], k) for k in range(4)]
        s_peer = [half(peer, r_peer[k], k) for k in range(pre)]
        s_t = c.copy(lambda: peer().at[at(pre)], lambda: r_t, "t")
        s_x = [c.copy(lambda: own().at[at(4)], lambda i=i: r_x[i], lv[4 + i], False) for i in range(extra)]
        s_g = [c.copy(lambda k=k: full.at[at(k + 1)], lambda k=k: full.at[at(k + 1)], lv[k]) for k in range(4)]
        s_out = c.here(lambda: full, lambda: out())
        self.wait_out = lambda: s_out().wait()

        def end(s, g, buf, k):
            s[k]().wait_recv()
            add_rows(g(), buf[k], lo[k + 1], n[k + 1], cols)

        def peer_step(i):
            if i:
                end(s_peer, peer, r_peer, i - 1)
            (s_peer[i] if i < pre else s_t)().start()

        def own_step(i):
            if i == 0:
                s_own[0]().start()
            elif i <= 4:
                end(s_own, own, r_own, i - 1)
                if i == pre:
                    s_t().wait_recv()
                    add_rows(own(), r_t, lo[pre], n[pre], cols)
                if i < 4:
                    s_own[i]().start()
                    return
                for j in range(extra):
                    s_x[j]().start()
                    s_x[j]().wait()
                    add_rows(own(), r_x[j], lo[4], n[4], cols)
                full[at(4), :] = own()[at(4), :]
                s_g[3]().start()
            else:
                k = 8 - i
                s_g[k]().wait_recv()
                if k:
                    s_g[k - 1]().start()
                else:
                    s_out().start()

        self.peer_steps = [lambda i=i: peer_step(i) for i in range(pre + 1)]
        self.own_steps = [lambda i=i: own_step(i) for i in range(9)]

    def own(self, m=1):
        for _ in range(m):
            self.own_steps.pop(0)()

    def peer(self, m=1):
        for _ in range(m):
            self.peer_steps.pop(0)()


class Small:
    def __init__(self, c, sm, bufs):
        s_a = c.copy(lambda: sm.at[0:8], lambda: bufs[0].at[0:8], "t", False)
        s_b = c.copy(lambda: sm.at[16:24], lambda: bufs[0].at[8:16], "t", False)
        s_l = [c.copy(lambda: sm.at[0:16], lambda i=i: bufs[i + 1], b, False) for i, b in enumerate(c.levels)]

        def step(i):
            if i == 0:
                s_a().start()
                s_b().start()
                return
            for s in (s_a, s_b) if i == 1 else (s_l[i - 2],):
                s().wait()
            sm[0:16, :] = sm[0:16, :] + bufs[i - 1][...]
            if i <= len(s_l):
                s_l[i - 1]().start()

        self.steps = [lambda i=i: step(i) for i in range(len(c.levels) + 2)]

    def go(self, m=1):
        for _ in range(m):
            self.steps.pop(0)()


INS = ["x_h", "cot_h", "hw_h", "ow_h", "uw_h", "dw_h", "ns", "nsh", "qb_o", "vb_o", "ob", "ub_o", "db"]
OUTS = ["lo_h", "ig_h", "FH_h", "FO_h", "FU_h", "FD_h", "smo"]
JOBS = [("D0", FH // 2, D, 1), ("D1", FH // 2, D, 1), ("U0", D // 2, FH, 2), ("U1", D // 2, FH, 2), ("O", HALF, D, 1),
        ("H0", 1536, 128, 1), ("H1", 1536, 128, 1)]


def scratch(T, ndp):
    nb = T // BLK
    V = pltpu.VMEM
    lv = ndp.bit_length() - 1
    s = dict(
        x=V((T, D), BF16), cot=V((T, D), BF16), hw=V((2, 3, D, HALF), BF16), ow=V((2, HALF, D), BF16),
        uw=V((2, D, FH), BF16), dw=V((2, FH, D), BF16),
        qb_p=V((1, HALF), F32), vb_p=V((1, HALF), F32), ub_p=V((1, FH), F32),
        n1T=V((D, T), BF16), qT=V((2, HALF, T), BF16), kT=V((2, HALF, T), BF16), vT=V((2, NH, 80, T), BF16),
        E=V((2 * NH, BLK * nb * (nb + 1) // 2, BLK), BF16), rl=V((2 * NH, 1, T), F32), mixT=V((2, HALF, T), BF16),
        res=V((T, D), F32), n2=V((T, D), BF16), act=V((2, T, FH), BF16), dpre=V((2, T, FH), BF16),
        oacc=V((T, D), F32), g2=V((T, D), F32), br=V((T, D), BF16), gmT=V((2, HALF, T), BF16),
        dh=V((3 * HD, T), BF16), dva=V((HD, T), F32), dka=V((HD, T), F32), sm=V((24, D), F32),
        GD0o=V((FH // 2, D), BF16), GD0p=V((FH // 2, D), BF16), GD1o=V((FH // 2, D), BF16), GD1p=V((FH // 2, D), BF16),
        GU0o=V((D // 2, FH), BF16), GU0p=V((D // 2, FH), BF16), GU1o=V((D // 2, FH), BF16), GU1p=V((D // 2, FH), BF16),
        GOo=V((HALF, D), BF16), GOp=V((HALF, D), BF16), GHo=V((NH, 768, 128), BF16), GHp=V((NH, 768, 128), BF16),
        s0=V((16, D), F32))
    for i in range(lv):
        s[f"s{i + 1}"] = V((16, D), F32)
    for name, rows, cols, pre in JOBS:
        for i, v in enumerate(job_scratch(rows, cols, pre, lv - 4)):
            s[f"{name}_{i}"] = v
    s["send"] = pltpu.SemaphoreType.DMA((96 + 32 * (lv - 4),))
    s["recv"] = pltpu.SemaphoreType.DMA((96 + 32 * (lv - 4),))
    s["local"] = pltpu.SemaphoreType.DMA((24,))
    return s


def run(z, ndp):
    c = Comm(ndp, z.send, z.recv, z.local)
    lv = c.levels
    c.barrier_signal()
    loads = {n: c.here(lambda n=n: getattr(z, n + "_h"), lambda n=n, d=d: d(getattr(z, n)))
             for n, d in (("x", lambda r: r), ("hw", lambda r: r.at[0]), ("cot", lambda r: r), ("ow", lambda r: r.at[0]),
                          ("uw", lambda r: r.at[0]), ("dw", lambda r: r.at[0]))}
    for n in ("x", "hw", "ow", "cot", "uw", "dw"):
        loads[n]().start()
    b0 = c.bit[1]

    def part(n):
        m = {"hw": D, "ow": HALF, "uw": D, "dw": FH}[n] // 2
        return pl.ds(pl.multiple_of(b0 * m, m), m)

    def view(r, n, lead):
        r = r.at[lead] if lead is not None else r
        return r.at[:, part(n)] if n == "hw" else r.at[part(n)]

    w1 = {n: c.copy(lambda n=n: view(getattr(z, n + "_h"), n, None), lambda n=n: view(getattr(z, n), n, 1), "t")
          for n in ("hw", "ow", "uw", "dw")}
    w2 = {n: c.copy(lambda n=n: view(getattr(z, n), n, 1), lambda n=n: view(getattr(z, n), n, 1), 1)
          for n in ("hw", "ow", "uw", "dw")}
    wb = [c.copy(lambda n=n: getattr(z, n + "_o"), lambda n=n: getattr(z, n + "_p"), "t") for n in ("qb", "vb", "ub")]

    def relay(n):
        w1[n]().wait_recv()
        w2[n]().start()

    def arrive(n):
        w2[n]().wait_recv()

    c.barrier_wait()
    w1["hw"]().start()
    for b in wb:
        b().start()
    for n in ("ow", "uw", "dw"):
        w1[n]().start()

    z.qb, z.vb, z.ub = (z.qb_o, z.qb_p), (z.vb_o, z.vb_p), (z.ub_o, z.ub_p)
    z.GD = ((z.GD0o, z.GD0p), (z.GD1o, z.GD1p))
    z.GU = ((z.GU0o, z.GU0p), (z.GU1o, z.GU1p))
    z.GO, z.GH = (z.GOo, z.GOp), (z.GHo, z.GHp)
    z.dT, z.lo, z.ig = z.dpre, z.br, z.n2
    ends = dict(D0=lambda: z.FD_h.at[0 : FH // 2], D1=lambda: z.FD_h.at[FH // 2 : FH], U0=lambda: z.FU_h.at[0 : D // 2],
                U1=lambda: z.FU_h.at[D // 2 : D], O=lambda: z.FO_h, H0=lambda: z.FH_h.at[0], H1=lambda: z.FH_h.at[1])
    flat = lambda r, i: (lambda: r.at[2 * i : 2 * i + 2].reshape(1536, 128))
    srcs = dict(D0=(lambda: z.GD0o, lambda: z.GD0p), D1=(lambda: z.GD1o, lambda: z.GD1p), U0=(lambda: z.GU0o, lambda: z.GU0p),
                U1=(lambda: z.GU1o, lambda: z.GU1p), O=(lambda: z.GOo, lambda: z.GOp),
                H0=(flat(z.GHo, 0), flat(z.GHp, 0)), H1=(flat(z.GHo, 1), flat(z.GHp, 1)))
    jobs = {}
    for name, rows, cols, pre in JOBS:
        refs = [getattr(z, f"{name}_{i}") for i in range(4 + pre + 1 + len(lv) - 4 + 1)]
        jobs[name] = Job(c, *srcs[name], refs, rows, cols, pre, ends[name])
    small = Small(c, z.sm, [getattr(z, f"s{i}") for i in range(len(lv) + 1)])
    D0, D1, U0, U1, O, H0, H1 = (jobs[n] for n in ("D0", "D1", "U0", "U1", "O", "H0", "H1"))
    s_lo, s_ig = c.here(lambda: z.lo, lambda: z.lo_h), c.here(lambda: z.ig, lambda: z.ig_h)

    def at(table):
        def hook(h):
            for k, fns in table.items():
                @pl.when(h == k)
                def _():
                    for fn in fns:
                        fn()
        return hook

    none = at({})
    z.sm[...] = jnp.zeros_like(z.sm)
    loads["x"]().wait()
    ln1(z)
    loads["hw"]().wait()
    qkv(z, 0)
    attn_fwd(z, 0, none)
    relay("hw")
    for b in wb:
        b().wait_recv()
    arrive("hw")
    qkv(z, 1)
    attn_fwd(z, 1, at({1: [lambda: relay("ow")]}))
    arrive("ow")
    loads["ow"]().wait()
    out_proj(z)
    for n in ("cot", "uw", "dw"):
        loads[n]().wait()
    ffn(z, 0, False, at({2: [lambda: relay("uw")]}))
    for part_ in (0, 1):
        d_down(z, 0, part_)
        (D0, D1)[part_].own()
    for part_ in (0, 1):
        d_up(z, 0, part_)
        (U0, U1)[part_].own()
    d_upb(z, 0)
    relay("dw")
    arrive("uw")
    arrive("dw")
    ffn(z, 1, True, none)
    d_down(z, 1, 0)
    D0.peer()
    d_down(z, 1, 1)
    D1.peer()
    D0.peer()
    d_up(z, 1, 0)
    U0.peer()
    D1.peer()
    d_up(z, 1, 1)
    U1.peer()
    U0.own()
    U0.peer()
    d_upb(z, 1)
    d_out(z, 1)
    O.peer()
    d_out(z, 0)
    O.own()
    grad_mixed(z, 1)
    grad_mixed(z, 0)
    U1.own()
    U1.peer()
    O.peer()
    attn_bwd(z, 1, at({
        0: [lambda: D0.own()],
        1: [lambda: (U0.peer(), H0.peer())],
        2: [lambda: (D1.own(), D0.own(), H0.peer())],
        3: [lambda: (U1.peer(), O.own(), H1.peer())]}))
    attn_bwd(z, 0, at({
        0: [lambda: (D0.own(), D1.own(), U0.own(), H1.peer())],
        1: [lambda: (D0.own(), D1.own(), U0.own(), U1.own(), O.own(), H0.own())],
        2: [lambda: (D0.own(), D1.own(), U0.own(), U1.own(), O.own(), H0.own())],
        3: [lambda: (H1.own(), D0.own(), D1.own(), U0.own(), U1.own(), O.own(), H0.own())]}))
    d_headb(z, 0)
    d_headb(z, 1)
    H1.own()
    every = (H1, H0, O, U1, U0, D1, D0)

    def push():
        for j in every:
            if j.own_steps:
                j.own()

    push()
    grad_in(z)
    s_ig().start()
    small.go()
    push()
    ffn_out(z)
    s_lo().start()
    while any(j.own_steps for j in every) or small.steps:
        if small.steps:
            small.go()
        push()
    z.smo[...] = z.sm[0:16, :]
    s_ig().wait()
    s_lo().wait()
    for j in every:
        j.wait_out()
    c.drain()


def main_call(args, T, ndp):
    scr = scratch(T, ndp)
    names = INS + OUTS + list(scr)

    def kernel(*refs):
        z = Refs()
        for n, r in zip(names, refs):
            setattr(z, n, r)
        z.nb = T // BLK
        run(z, ndp)

    S = jax.ShapeDtypeStruct
    outs = [S((T, D), BF16), S((T, D), BF16), S((2, 1536, 128), BF16), S((HALF, D), BF16), S((D, FH), BF16), S((FH, D), BF16),
            S((16, D), F32)]
    vm, hbm = pl.BlockSpec(memory_space=pltpu.VMEM), pl.BlockSpec(memory_space=pl.ANY)
    return pl.pallas_call(
        kernel, out_shape=outs, in_specs=[hbm] * 6 + [vm] * 7, out_specs=[hbm] * 6 + [vm], scratch_shapes=list(scr.values()),
        compiler_params=pltpu.CompilerParams(vmem_limit_bytes=VMEM_BYTES, collective_id=0, has_side_effects=True),
        name="layer")(*args)


def widen(FH_, FO_, FU_, FD_):
    def kernel(h, o, u, d, ho, oo, uo, do):
        oo[...] = o[...].astype(F32)
        uo[...] = u[...].astype(F32)
        do[...] = d[...].astype(F32)
        for q in range(4):
            for j in range(3):
                for p in range(2):
                    rows = [h[p, i * 768 + q * 192 + j * HD : i * 768 + q * 192 + (j + 1) * HD, :] for i in range(2)]
                    t = jnp.concatenate(rows, 0).astype(F32).T
                    ho[j, q * 128 : (q + 1) * 128, p * 128 : (p + 1) * 128] = t

    S = jax.ShapeDtypeStruct
    vm = pl.BlockSpec(memory_space=pltpu.VMEM)
    return pl.pallas_call(
        kernel, out_shape=[S((3, D, HALF), F32), S((HALF, D), F32), S((D, FH), F32), S((FH, D), F32)],
        in_specs=[vm] * 4, out_specs=[vm] * 4, name="widen")(FH_, FO_, FU_, FD_)


def solution(mesh):
    ndp = mesh.shape["dp"]

    def local(inputs, norm_scale, norm_shift, head_weight, query_bias, value_bias, out_weight, out_bias, up_weight, up_bias,
              down_weight, down_bias, cotangent):
        row = lambda b: b.reshape(1, b.shape[0])
        args = (inputs, cotangent, head_weight, out_weight, up_weight, down_weight, norm_scale, norm_shift, row(query_bias),
                row(value_bias), row(out_bias), row(up_bias), row(down_bias))
        lo, ig, gh, go, gu, gd, sm = main_call(args, inputs.shape[0], ndp)
        gh, go, gu, gd = widen(gh, go, gu, gd)
        return (lo, ig, sm[0:2], sm[2:4], gh, sm[8, 0:HALF], sm[8, HALF:D], go, sm[4], gu, sm[9:11].reshape(FH), gd, sm[5])

    rows, t0, t1 = P(("dp", "tensor"), None), P("tensor"), P(None, "tensor")
    tc = P("tensor", None)
    in_specs = (rows, P(), P(), P(None, None, "tensor"), t0, t0, tc, P(), t1, t0, tc, P(), rows)
    out_specs = (rows, rows, P(), P(), P(None, None, "tensor"), t0, t0, tc, P(), t1, t0, tc, P())
    return jax.shard_map(local, mesh=mesh, in_specs=in_specs, out_specs=out_specs, check_vma=False)
```

```python
import jax
import jax.numpy as jnp
from jax import lax
from jax.experimental import pallas as pl
from jax.experimental.pallas import tpu as pltpu
from jax.sharding import PartitionSpec as P

F32, BF16 = jnp.float32, jnp.bfloat16
NN, NT, TN = ((1,), (0,)), ((1,), (1,)), ((0,), (0,))
EPS = 1e-5
LOG2E = 1.4426950408889634
LN2 = 0.6931471805599453
C0, C1 = 0.7978845608, 0.044715
HD, BLK, D, HALF, FH, NH = 64, 256, 512, 256, 1024, 4
MESH = pl.DeviceIdType.MESH
VMEM_BYTES = 67043328


def dot(a, b, dims=NN):
    return lax.dot_general(a, b, (dims, ((), ())), preferred_element_type=F32)


def normed(v):
    c = jnp.mean(v, -1, keepdims=True)
    d = v - c
    r = lax.rsqrt(jnp.mean(d * d, -1, keepdims=True) + EPS)
    return d * r, r


def ln_back(g, xhat, r, gain):
    gx = g * gain
    return r * (gx - jnp.mean(gx, -1, keepdims=True) - xhat * jnp.mean(gx * xhat, -1, keepdims=True))


def rows_of(r):
    return pl.ds(pl.multiple_of(r * BLK, BLK), BLK)


def column(row):
    return jnp.broadcast_to(row, (8, row.shape[-1])).T[:, 0:1]


class Refs:
    pass


def ln1(z):
    def body(r, c):
        xh, _ = normed(z.x[rows_of(r), :].astype(F32))
        n = (xh * z.ns[0:1, :] + z.nsh[0:1, :]).astype(BF16)
        z.n1T[:, rows_of(r)] = n.T
        return c

    lax.fori_loop(0, z.nb, body, 0)


def qkv(z, s, h0, h1):
    cs = slice(h0 * HD, h1 * HD)
    qb, vb = column(z.qb[s][:, cs]), column(z.vb[s][:, cs])
    for b in range(z.nb):
        sl = slice(b * BLK, (b + 1) * BLK)
        nt = z.n1T[:, sl]
        q = dot(z.hw[s, 0, :, cs], nt, TN) + qb
        z.qT[s, cs, sl] = (q * (LOG2E / 8.0)).astype(BF16)
        z.kT[s, cs, sl] = dot(z.hw[s, 1, :, cs], nt, TN).astype(BF16)
        v = (dot(z.hw[s, 2, :, cs], nt, TN) + vb).astype(BF16)
        for h in range(h0, h1):
            z.vT[s, h, 0:HD, sl] = v[(h - h0) * HD : (h - h0 + 1) * HD]
            z.vT[s, h, HD : HD + 16, sl] = jnp.ones((16, BLK), BF16)


def attn_fwd(z, s, h0, h1, hook):
    def body(h, c):
        hr = pl.ds(pl.multiple_of(h * HD, HD), HD)
        kh = z.kT[s, hr, :].T
        for b in range(z.nb):
            nk = BLK * (b + 1)
            off = BLK * (b * (b + 1) // 2)
            sl = slice(b * BLK, nk)
            sc = dot(kh[:nk], z.qT[s, hr, sl])
            m = jnp.max(sc, 0, keepdims=True)
            e = jnp.exp2(sc - m).astype(BF16)
            z.E[s * NH + h, off : off + nk, :] = e
            o = dot(z.vT[s, h, :, 0:nk], e)
            rl = 1.0 / o[HD : HD + 1]
            z.rl[s * NH + h, 0:1, sl] = rl
            z.mixT[s, hr, sl] = (o[0:HD] * rl).astype(BF16)
        hook(h)
        return c

    lax.fori_loop(h0, h1, body, 0)


def out_proj(z):
    for r in range(z.nb):
        sl = slice(r * BLK, (r + 1) * BLK)
        t = dot(z.mixT[0, :, sl], z.ow[0], TN) + dot(z.mixT[1, :, sl], z.ow[1], TN)
        res = z.x[sl, :].astype(F32) + (t + z.ob[...])
        z.res[sl, :] = res
        z.oacc[sl, :] = res + z.db[...]
        xh, _ = normed(res)
        z.n2[sl, :] = (xh * z.ns[1:2, :] + z.nsh[1:2, :]).astype(BF16)


def ffn(z, part, s, hook):
    first, last = (part, s) == (0, 0), (part, s) == (1, 1)
    fs = slice(part * 512, part * 512 + 512)

    def body(r, c):
        rr = rows_of(r)
        ct = z.cot[rr, :]
        u = dot(z.n2[rr, :], z.uw[s, :, fs]) + z.ub[s][:, fs]
        da = dot(ct, z.dw[s, fs, :], NT)
        u2 = u * u
        t = jnp.tanh(u * (C0 + (C0 * C1) * u2))
        hp = 0.5 + 0.5 * t
        z.act[s, rr, fs] = (u * hp).astype(BF16)
        gp = hp + (u * (0.5 - 0.5 * t * t)) * (C0 + (3 * C0 * C1) * u2)
        dp = (da * gp).astype(BF16)
        z.dpre[s, rr, fs] = dp
        g = dot(dp, z.uw[s, :, fs], NT)
        g2 = g if first else z.g2[rr, :] + g
        if not last:
            z.g2[rr, :] = g2
        else:
            xh, rs = normed(z.res[rr, :])
            gres = ct.astype(F32) + ln_back(g2, xh, rs, z.ns[1:2, :])
            br = gres.astype(BF16)
            z.res[rr, :] = gres
            z.br[rr, :] = br
            c = (
                c[0] + jnp.sum(g2 * xh, 0, keepdims=True),
                c[1] + jnp.sum(g2, 0, keepdims=True),
                c[2] + jnp.sum(br.astype(F32), 0, keepdims=True),
                c[3] + jnp.sum(ct.astype(F32), 0, keepdims=True),
            )
        hook(r)
        return c

    zero = jnp.zeros((1, D), F32)
    c = lax.fori_loop(0, z.nb, body, (zero,) * 4 if last else 0)
    if last:
        z.sm[1:2, :] = c[0]
        z.sm[3:4, :] = c[1]
        z.sm[4:5, :] = c[2]
        z.sm[5:6, :] = c[3]


def ffn_out(z, blocks):
    for r in blocks:
        rr = slice(r * BLK, (r + 1) * BLK)
        o = dot(z.act[0, rr, :], z.dw[0]) + dot(z.act[1, rr, :], z.dw[1])
        z.lo[rr, :] = (z.oacc[rr, :] + o).astype(BF16)


def d_down(z, part, s):
    for f in range(0, 512, 256):
        a = part * 512 + f
        z.GD[part][s][f : f + 256, :] = dot(z.act[s, :, a : a + 256], z.cot[...], TN).astype(BF16)


def d_up(z, part, s):
    z.GU[part][s][...] = dot(z.n2[...], z.dpre[s, :, part * 512 : part * 512 + 512], TN).astype(BF16)


def d_upb(z, s):
    ones = jnp.ones((8, z.dpre.shape[1]), BF16)
    for i in range(FH // 512):
        row = 9 + 8 * s + i
        z.sm[row : row + 1, :] = dot(ones, z.dpre[s, :, i * 512 : (i + 1) * 512])[0:1]


def d_out(z, s):
    z.GO[s][...] = dot(z.mixT[s], z.br[...]).astype(BF16)


def grad_mixed(z, s):
    for r in range(z.nb):
        sl = slice(r * BLK, (r + 1) * BLK)
        z.gmT[s, :, sl] = dot(z.ow[s], z.br[sl, :], NT).astype(BF16)


def attn_bwd(z, s, hook):
    def body(h, c):
        hr = pl.ds(pl.multiple_of(h * HD, HD), HD)
        hi = s * NH + h
        vh = z.vT[s, h, 0:HD, :].T
        gs = (z.gmT[s, hr, :].astype(F32) * z.rl[hi]).astype(BF16)
        delta = jnp.sum(gs.astype(F32) * z.mixT[s, hr, :].astype(F32), 0, keepdims=True)
        for b in range(z.nb):
            nk = BLK * (b + 1)
            off = BLK * (b * (b + 1) // 2)
            sl = slice(b * BLK, nk)
            gq = gs[:, sl]
            e = z.E[hi, off : off + nk, :]
            dp = dot(vh[:nk], gq)
            ds = (e.astype(F32) * (dp - delta[:, sl])).astype(BF16)
            z.dh[0:HD, sl] = (dot(z.kT[s, hr, 0:nk], ds) * 0.125).astype(BF16)
            dv = dot(gq, e, NT)
            dk = dot(z.qT[s, hr, sl], ds, NT)
            if b:
                z.dva[:, 0 : nk - BLK] = z.dva[:, 0 : nk - BLK] + dv[:, 0 : nk - BLK]
                z.dka[:, 0 : nk - BLK] = z.dka[:, 0 : nk - BLK] + dk[:, 0 : nk - BLK]
            z.dva[:, sl] = dv[:, nk - BLK : nk]
            z.dka[:, sl] = dk[:, nk - BLK : nk]
        z.dh[HD : 2 * HD, :] = (z.dka[...] * LN2).astype(BF16)
        z.dh[2 * HD : 3 * HD, :] = z.dva[...].astype(BF16)
        for j in range(3):
            z.dT[s, pl.ds(pl.multiple_of(j * HALF + h * HD, HD), HD), :] = z.dh[j * HD : (j + 1) * HD, :]
        g = dot(z.dh[...], z.n1T[...], NT).astype(BF16)
        for q in range(4):
            z.GH[s][h, q * 192 : (q + 1) * 192, :] = g[:, q * 128 : (q + 1) * 128]
        hook(h)
        return c

    lax.fori_loop(0, NH, body, 0)


def d_headb(z, s):
    ones = jnp.ones((8, z.dT.shape[2]), BF16)
    for i, j in enumerate((0, 2)):
        row = 8 + 8 * s
        z.sm[row : row + 1, i * HALF : (i + 1) * HALF] = dot(ones, z.dT[s, j * HALF : (j + 1) * HALF, :], NT)[0:1]


def grad_in(z):
    zero = jnp.zeros((1, D), F32)
    sc, sh = zero, zero
    for r in range(z.nb):
        sl = slice(r * BLK, (r + 1) * BLK)
        g = 0.0
        for s in (0, 1):
            for j in range(3):
                g = g + dot(z.hw[s, j], z.dT[s, j * HALF : (j + 1) * HALF, sl])
        g = g.T
        xh, rs = normed(z.x[sl, :].astype(F32))
        z.ig[sl, :] = (z.res[sl, :] + ln_back(g, xh, rs, z.ns[0:1, :])).astype(BF16)
        sc = sc + jnp.sum(g * xh, 0, keepdims=True)
        sh = sh + jnp.sum(g, 0, keepdims=True)
    z.sm[0:1, :] = sc
    z.sm[2:3, :] = sh


class Comm:
    def __init__(self, ndp, groups, send, recv, local):
        self.send, self.recv, self.local = send, recv, local
        self.count, self.local_count, self.pending = 0, 0, []
        me = lax.axis_index("dp")
        self.levels = [1 << i for i in range(ndp.bit_length() - 1)]
        self.bit = {b: (me // b) % 2 for b in self.levels}
        self.me = me
        self.greet = ["t"] + [([b], 1) for b in self.levels] + [(g, d) for g in groups for d in range(1, 1 << len(g)) if d & (d - 1)]
        self.peer = 1 - lax.axis_index("tensor")

    def where(self, axis):
        if axis == "t":
            return {"tensor": self.peer}
        bits, delta = axis
        return {"dp": self.me + sum(b - 2 * b * self.bit[b] for i, b in enumerate(bits) if delta >> i & 1)}

    def barrier_signal(self):
        sem = pltpu.get_barrier_semaphore()
        for axis in self.greet:
            pl.semaphore_signal(sem, inc=1, device_id=self.where(axis), device_id_type=MESH)

    def barrier_wait(self):
        pl.semaphore_wait(pltpu.get_barrier_semaphore(), len(self.greet))

    def copy(self, src, dst, axis, keep=True):
        i = self.count
        self.count += 1

        def make():
            return pltpu.make_async_remote_copy(
                src_ref=src(), dst_ref=dst(), send_sem=self.send.at[i], recv_sem=self.recv.at[i],
                device_id=self.where(axis), device_id_type=MESH)

        if keep:
            self.pending.append(make)
        return make

    def here(self, src, dst):
        i = self.local_count
        self.local_count += 1
        return lambda: pltpu.make_async_copy(src(), dst(), self.local.at[i])

    def drain(self):
        for make in self.pending:
            make().wait_send()


def add_rows(dst, srcs, at, n, cols):
    ch = next(c for c in (384, 256, 192, 128, 96, 64, 48, 32, 16, 8, 4) if n % c == 0 and c * cols <= 49152)

    def body(i, c):
        o = pl.ds(pl.multiple_of(at + i * ch, ch), ch)
        f = pl.ds(pl.multiple_of(i * ch, ch), ch)
        if len(srcs) == 1:
            dst[o, :] = dst[o, :] + srcs[0][f, :]
        else:
            dst[o, :] = pairwise([dst[o, :].astype(F32)] + [s[f, :].astype(F32) for s in srcs]).astype(dst.dtype)
        return c

    lax.fori_loop(0, n // ch, body, 0)


def pairwise(v):
    while len(v) > 1:
        v = [v[i] + v[i + 1] for i in range(0, len(v), 2)]
    return v[0]


def sizes_of(rows, stages):
    n = [rows]
    for bits in stages:
        n.append(n[-1] >> len(bits))
    return n


def job_scratch(rows, cols, stages, pre, extra):
    V = pltpu.VMEM
    n = sizes_of(rows, stages)
    bufs = lambda ss: [V((n[k + 1], cols), BF16) for k in range(ss) for _ in range((1 << len(stages[k])) - 1)]
    return bufs(len(stages)) + bufs(pre) + [V((n[pre], cols), BF16)] + [V((n[-1], cols), BF16) for _ in range(extra)] + [V((rows, cols), BF16)]


class Job:
    def __init__(self, c, own, peer, refs, rows, cols, stages, pre, out):
        S = len(stages)
        done = sum(len(b) for b in stages)
        extra = c.levels[done:]
        n = sizes_of(rows, stages)
        refs = list(refs)
        take = lambda m: [refs.pop(0) for _ in range(m)]
        r_own = [take((1 << len(b)) - 1) for b in stages]
        r_peer = [take((1 << len(b)) - 1) for b in stages[:pre]]
        r_t, r_x, full = take(1)[0], take(len(extra)), refs.pop(0)

        def code(bits, delta):
            return sum((c.bit[b] if not delta >> i & 1 else 1 - c.bit[b]) * (1 << i) for i, b in enumerate(bits))

        lo = [0]
        for k, b in enumerate(stages):
            lo.append(lo[k] + code(b, 0) * n[k + 1])
        at = lambda k: pl.ds(pl.multiple_of(lo[k], n[k]) if k else 0, n[k])
        theirs = lambda k, d: pl.ds(pl.multiple_of(lo[k] + code(stages[k], d) * n[k + 1], n[k + 1]), n[k + 1])

        def scatter(g, bufs, k):
            return [c.copy(lambda d=d: g().at[theirs(k, d)], lambda d=d: bufs[d - 1], (stages[k], d)) for d in range(1, len(bufs) + 1)]

        s_own = [scatter(own, r_own[k], k) for k in range(S)]
        s_peer = [scatter(peer, r_peer[k], k) for k in range(pre)]
        s_t = c.copy(lambda: peer().at[at(pre)], lambda: r_t, "t")
        s_x = [c.copy(lambda: own().at[at(S)], lambda i=i: r_x[i], ([b], 1), False) for i, b in enumerate(extra)]
        s_g = [[c.copy(lambda k=k: full.at[at(k + 1)], lambda k=k: full.at[at(k + 1)], (stages[k], d)) for d in range(1, 1 << len(stages[k]))]
               for k in range(S)]
        s_out = c.here(lambda: full, lambda: out())
        self.wait_out = lambda: s_out().wait()
        start = lambda ss: [s().start() for s in ss]
        arrived = lambda ss: [s().wait_recv() for s in ss]

        def end(s, g, buf, k):
            arrived(s[k])
            add_rows(g(), buf[k], lo[k + 1], n[k + 1], cols)

        def peer_step(i):
            if i:
                end(s_peer, peer, r_peer, i - 1)
            start(s_peer[i] if i < pre else [s_t])

        def own_step(i):
            if i == 0:
                start(s_own[0])
            elif i <= S:
                end(s_own, own, r_own, i - 1)
                if i == pre:
                    assert not self.peer_steps
                    s_t().wait_recv()
                    add_rows(own(), [r_t], lo[pre], n[pre], cols)
                if i < S:
                    start(s_own[i])
                    return
                for j in range(len(extra)):
                    s_x[j]().start()
                    s_x[j]().wait()
                    add_rows(own(), [r_x[j]], lo[S], n[S], cols)
                full[at(S), :] = own()[at(S), :]
                start(s_g[S - 1])
            else:
                k = 2 * S - i
                arrived(s_g[k])
                if k:
                    start(s_g[k - 1])
                else:
                    s_out().start()

        self.peer_steps = [lambda i=i: peer_step(i) for i in range(pre + 1)]
        self.own_steps = [lambda i=i: own_step(i) for i in range(2 * S + 1)]

    def own(self):
        self.own_steps.pop(0)()

    def peer(self):
        self.peer_steps.pop(0)()


SMALL_STAGES = [[1], [2], [4, 8]]


class Small:
    def __init__(self, c, sm, bufs):
        bufs = list(bufs)
        r_t = bufs.pop(0)
        st = SMALL_STAGES + [[b] for b in c.levels[4:]]
        s_t = [c.copy(lambda: sm.at[0:8], lambda: r_t.at[0:8], "t", False), c.copy(lambda: sm.at[16:24], lambda: r_t.at[8:16], "t", False)]
        rs, ss = [[r_t]], [s_t]
        for bits in st:
            r = [bufs.pop(0) for _ in range((1 << len(bits)) - 1)]
            rs.append(r)
            ss.append([c.copy(lambda: sm.at[0:16], lambda b=b: b, (bits, d + 1), False) for d, b in enumerate(r)])

        def step(i):
            if i:
                for s in ss[i - 1]:
                    s().wait()
                sm[0:16, :] = pairwise([sm[0:16, :]] + [r[...] for r in rs[i - 1]])
            if i < len(ss):
                for s in ss[i]:
                    s().start()

        self.steps = [lambda i=i: step(i) for i in range(len(ss) + 1)]

    def own(self):
        self.steps.pop(0)()


INS = ["x_h", "cot_h", "hw_h", "ow_h", "uw_h", "dw_h", "ns", "nsh", "qb_o", "vb_o", "ob", "ub_o", "db"]
OUTS = ["lo_h", "ig_h", "FH_h", "FO_h", "FU_h", "FD_h", "smo"]
Y4, Z14, G8 = [[1], [2], [4, 8]], [[1], [4], [2], [8]], [[1], [2, 4, 8]]
JOBS = [("D0", 512, 512, [[1], [2], [4, 8]], 1),
        ("U0", 512, 512, [[1], [2], [4, 8]], 2),
        ("D1", 512, 512, [[1], [2], [4, 8]], 1),
        ("U1", 512, 512, [[1], [2], [4, 8]], 2),
        ("O", 256, 512, [[1], [2], [4, 8]], 1),
        ("H0", 1536, 128, [[1], [2], [4, 8]], 1),
        ("H1", 1536, 128, [[1], [2], [4, 8]], 1)]

HOOKS = {
    "f0_0": ["WhwA"],
    "f0_2": ["WhwB", "Wow", "WhwA"],
    "qkv1a": ["Wu0"],
    "f1_0": ["WhwB"],
    "f1_1": ["Wow", "Wd0"],
    "f1_2": ["Wu0", "Wu1"],
    "f1_3": ["Wd0", "Wd1"],
    "ffn00_1": ["Wu1"],
    "dD00": ["D0o"],
    "dU00": ["Wd1", "U0o"],
    "ffn01_2": ["U0o"],
    "dD01": ["D0p"],
    "dU01": ["U0p"],
    "ffn10_0": ["D0p"],
    "ffn10_1": ["U0p"],
    "dD10": ["D1o"],
    "dU10": ["U1o"],
    "ffn11_1": ["U1o", "U0p"],
    "ffn11_3": ["D0o"],
    "dD11": ["D1p"],
    "dU11": ["U1p"],
    "dO1": ["Op"],
    "dO0": ["D1p", "U0o", "U1p", "Op", "Oo"],
    "b1_0": ["D0o"],
    "b1_1": ["U1p", "H0p", "U0o"],
    "b1_2": ["H0p", "D1o", "D0o"],
    "b1_3": ["H1p", "U0o", "Oo"],
    "b0_0": ["H1p", "D1o", "D0o", "U1o"],
    "b0_1": ["U0o", "H0o"],
    "b0_2": ["U0o", "Oo", "H0o", "D1o"],
    "b0_3": ["D0o", "H1o"],
    "hb": ["U1o"],
    "gin": ["D0o", "Oo", "H0o", "H1o", "So", "D1o"],
    "tail": ["So", "U1o", "So", "H1o", "Oo", "H0o", "D1o", "D1o", "H1o", "U1o", "So", "U1o", "H0o", "Oo", "Oo", "H1o", "H0o", "So", "H0o", "H1o", "H1o"],
}
BEFORE = {
}


def scratch(T, ndp):
    nb = T // BLK
    V = pltpu.VMEM
    lv = ndp.bit_length() - 1
    s = dict(
        x=V((T, D), BF16), cot=V((T, D), BF16), hw=V((2, 3, D, HALF), BF16), ow=V((2, HALF, D), BF16),
        uw=V((2, D, FH), BF16), dw=V((2, FH, D), BF16),
        qb_p=V((1, HALF), F32), vb_p=V((1, HALF), F32), ub_p=V((1, FH), F32),
        n1T=V((D, T), BF16), qT=V((2, HALF, T), BF16), kT=V((2, HALF, T), BF16), vT=V((2, NH, 80, T), BF16),
        E=V((2 * NH, BLK * nb * (nb + 1) // 2, BLK), BF16), rl=V((2 * NH, 1, T), F32), mixT=V((2, HALF, T), BF16),
        res=V((T, D), F32), n2=V((T, D), BF16), act=V((2, T, FH), BF16), dpre=V((2, T, FH), BF16),
        oacc=V((T, D), F32), g2=V((T, D), F32), br=V((T, D), BF16), gmT=V((2, HALF, T), BF16),
        dh=V((3 * HD, T), BF16), dva=V((HD, T), F32), dka=V((HD, T), F32), sm=V((24, D), F32),
        GD0o=V((FH // 2, D), BF16), GD0p=V((FH // 2, D), BF16), GD1o=V((FH // 2, D), BF16), GD1p=V((FH // 2, D), BF16),
        GU0o=V((D, FH // 2), BF16), GU0p=V((D, FH // 2), BF16), GU1o=V((D, FH // 2), BF16), GU1p=V((D, FH // 2), BF16),
        GOo=V((HALF, D), BF16), GOp=V((HALF, D), BF16), GHo=V((NH, 768, 128), BF16), GHp=V((NH, 768, 128), BF16),
        s0=V((16, D), F32))
    for i in range(5 + lv - 4):
        s[f"s{i + 1}"] = V((16, D), F32)
    for name, rows, cols, stages, pre in JOBS:
        for i, v in enumerate(job_scratch(rows, cols, stages, pre, lv - 4)):
            s[f"{name}_{i}"] = v
    s["send"] = pltpu.SemaphoreType.DMA((160 + 16 * (lv - 4),))
    s["recv"] = pltpu.SemaphoreType.DMA((160 + 16 * (lv - 4),))
    s["local"] = pltpu.SemaphoreType.DMA((24,))
    return s


def run(z, ndp):
    c = Comm(ndp, [[4, 8], [2, 4, 8]], z.send, z.recv, z.local)
    lv = c.levels
    c.barrier_signal()
    slot0 = lambda r: r.at[0]
    loads = {n: c.here(lambda n=n: getattr(z, n + "_h"), lambda n=n, d=d: d(getattr(z, n)))
             for n, d in (("x", lambda r: r), ("hw", slot0), ("cot", lambda r: r), ("ow", slot0), ("uw", slot0), ("dw", slot0))}
    for n in ("x", "hw", "ow", "cot", "uw", "dw"):
        loads[n]().start()

    pieces = {"hwA": ("hw", D, 0, slice(0, 128)), "hwB": ("hw", D, 0, slice(128, 256)), "ow": ("ow", HALF, 0, slice(None)),
              "u0": ("uw", D, 0, slice(0, 512)), "d0": ("dw", 512, 0, slice(None)), "u1": ("uw", D, 0, slice(512, 1024)),
              "d1": ("dw", 512, 512, slice(None))}

    def view(name, flip, lead):
        n, m, base, cols = pieces[name]
        q = (c.bit[1] if not flip & 1 else 1 - c.bit[1]) + 2 * (c.bit[2] if not flip & 2 else 1 - c.bit[2])
        rows = pl.ds(pl.multiple_of(base + q * (m // 4), m // 4), m // 4)
        r = getattr(z, n).at[1] if lead else getattr(z, n + "_h")
        return r.at[:, rows, cols] if n == "hw" else r.at[rows, cols]

    W = {}
    for name in pieces:
        put = lambda flip, name=name: view(name, flip, True)
        W[name] = dict(
            x=c.copy(lambda name=name: view(name, 0, False), lambda put=put: put(0), "t"),
            s=c.copy(lambda put=put: put(0), lambda put=put: put(0), ([1], 1)),
            y=c.copy(lambda put=put: put(0), lambda put=put: put(0), ([2], 1)),
            r=c.copy(lambda put=put: put(2), lambda put=put: put(2), ([1], 1)))
    wb = [c.copy(lambda n=n: getattr(z, n + "_o"), lambda n=n: getattr(z, n + "_p"), "t") for n in ("qb", "vb", "ub")]

    def relay1(n):
        W[n]["x"]().wait_recv()
        W[n]["y"]().start()
        W[n]["s"]().start()

    def relay2(n):
        W[n]["y"]().wait_recv()
        W[n]["r"]().start()

    def arrive(n):
        W[n]["s"]().wait_recv()
        W[n]["r"]().wait_recv()

    c.barrier_wait()
    W["hwA"]["x"]().start()
    for b in wb:
        b().start()
    for n in list(pieces)[1:]:
        W[n]["x"]().start()

    z.qb, z.vb, z.ub = (z.qb_o, z.qb_p), (z.vb_o, z.vb_p), (z.ub_o, z.ub_p)
    z.GD = ((z.GD0o, z.GD0p), (z.GD1o, z.GD1p))
    z.GU = ((z.GU0o, z.GU0p), (z.GU1o, z.GU1p))
    z.GO, z.GH = (z.GOo, z.GOp), (z.GHo, z.GHp)
    z.dT, z.lo, z.ig = z.dpre, z.br, z.n2
    ends = dict(D0=lambda: z.FD_h.at[0 : FH // 2], D1=lambda: z.FD_h.at[FH // 2 : FH], U0=lambda: z.FU_h.at[:, 0 : FH // 2],
                U1=lambda: z.FU_h.at[:, FH // 2 : FH], O=lambda: z.FO_h, H0=lambda: z.FH_h.at[0], H1=lambda: z.FH_h.at[1])
    flat = lambda r, i: (lambda: r.at[2 * i : 2 * i + 2].reshape(1536, 128))
    srcs = dict(D0=(lambda: z.GD0o, lambda: z.GD0p), D1=(lambda: z.GD1o, lambda: z.GD1p), U0=(lambda: z.GU0o, lambda: z.GU0p),
                U1=(lambda: z.GU1o, lambda: z.GU1p), O=(lambda: z.GOo, lambda: z.GOp),
                H0=(flat(z.GHo, 0), flat(z.GHp, 0)), H1=(flat(z.GHo, 1), flat(z.GHp, 1)))
    jobs = {}
    for name, rows, cols, stages, pre in JOBS:
        refs = [getattr(z, f"{name}_{i}") for i in range(len(job_scratch(rows, cols, stages, pre, len(lv) - 4)))]
        jobs[name] = Job(c, *srcs[name], refs, rows, cols, stages, pre, ends[name])
    jobs["S"] = small = Small(c, z.sm, [getattr(z, f"s{i}") for i in range(6 + len(lv) - 4)])
    s_lo, s_ig = c.here(lambda: z.lo, lambda: z.lo_h), c.here(lambda: z.ig, lambda: z.ig_h)

    relays = {n: [relay1, relay2] for n in W}

    def go(words):
        for word in words:
            if word[1:] in relays:
                relays[word[1:]].pop(0)(word[1:])
            else:
                (jobs[word[:-1]].own if word[-1] == "o" else jobs[word[:-1]].peer)()

    def at(name, n):
        table = {k: HOOKS.get(f"{name}_{k}", ()) for k in (range(n) if isinstance(n, int) else n)}

        def hook(h):
            for k, what in table.items():
                if what:
                    @pl.when(h == k)
                    def _():
                        go(what)
        return hook

    def before(name):
        go(BEFORE.get(name, ()))

    def after(name):
        go(HOOKS.get(name, ()))

    z.sm[...] = jnp.zeros_like(z.sm)
    loads["x"]().wait()
    ln1(z)
    loads["hw"]().wait()
    qkv(z, 0, 0, NH)
    after("qkv0")
    attn_fwd(z, 0, 0, NH, at("f0", 4))
    before("qkv1a")
    for b in wb:
        b().wait_recv()
    arrive("hwA")
    qkv(z, 1, 0, 2)
    after("qkv1a")
    attn_fwd(z, 1, 0, 2, at("f1", range(0, 2)))
    before("qkv1b")
    arrive("hwB")
    qkv(z, 1, 2, 4)
    after("qkv1b")
    attn_fwd(z, 1, 2, 4, at("f1", range(2, 4)))
    before("out")
    arrive("ow")
    loads["ow"]().wait()
    out_proj(z)
    for n in ("cot", "uw", "dw"):
        loads[n]().wait()
    after("out")
    for part in (0, 1):
        for s in (0, 1):
            name = f"ffn{part}{s}"
            before(name + "_0")
            if s:
                arrive(f"u{part}")
                arrive(f"d{part}")
            ffn(z, part, s, at(name, z.nb))
            d_down(z, part, s)
            after(f"dD{part}{s}")
            d_up(z, part, s)
            if part:
                d_upb(z, s)
            after(f"dU{part}{s}")
    for s in (1, 0):
        d_out(z, s)
        after(f"dO{s}")
    grad_mixed(z, 1)
    grad_mixed(z, 0)
    after("gm")
    attn_bwd(z, 1, at("b1", NH))
    attn_bwd(z, 0, at("b0", NH))
    d_headb(z, 0)
    d_headb(z, 1)
    after("hb")
    grad_in(z)
    s_ig().start()
    after("gin")
    ffn_out(z, (0, 1))
    after("fo0")
    ffn_out(z, (2, 3))
    s_lo().start()
    after("fo1")
    after("tail")
    while small.steps:
        small.own()
    assert not any(v for v in relays.values()) and not any(jobs[n].own_steps for n in jobs if n != "S")
    z.smo[...] = z.sm[0:16, :]
    s_ig().wait()
    s_lo().wait()
    for n in jobs:
        if n != "S":
            jobs[n].wait_out()
    c.drain()


def main_call(args, T, ndp):
    scr = scratch(T, ndp)
    names = INS + OUTS + list(scr)

    def kernel(*refs):
        z = Refs()
        for n, r in zip(names, refs):
            setattr(z, n, r)
        z.nb = T // BLK
        run(z, ndp)

    S = jax.ShapeDtypeStruct
    outs = [S((T, D), BF16), S((T, D), BF16), S((2, 1536, 128), BF16), S((HALF, D), BF16), S((D, FH), BF16), S((FH, D), BF16),
            S((16, D), F32)]
    vm, hbm = pl.BlockSpec(memory_space=pltpu.VMEM), pl.BlockSpec(memory_space=pl.ANY)
    return pl.pallas_call(
        kernel, out_shape=outs, in_specs=[hbm] * 6 + [vm] * 7, out_specs=[hbm] * 6 + [vm], scratch_shapes=list(scr.values()),
        compiler_params=pltpu.CompilerParams(vmem_limit_bytes=VMEM_BYTES, collective_id=0, has_side_effects=True),
        name="layer")(*args)


def widen(FH_, FO_, FU_, FD_, sm):
    def kernel(h, o, u, d, m, ho, oo, uo, do, sc, sh, qb, vb, ob, ub, db):
        oo[...] = o[...].astype(F32)
        uo[...] = u[...].astype(F32)
        do[...] = d[...].astype(F32)
        for q in range(4):
            for j in range(3):
                for p in range(2):
                    rows = [h[p, i * 768 + q * 192 + j * HD : i * 768 + q * 192 + (j + 1) * HD, :] for i in range(2)]
                    t = jnp.concatenate(rows, 0).astype(F32).T
                    ho[j, q * 128 : (q + 1) * 128, p * 128 : (p + 1) * 128] = t
        sc[...] = m[0:2, :]
        sh[...] = m[2:4, :]
        qb[...] = m[8:9, 0:HALF]
        vb[...] = m[8:9, HALF:D]
        ob[...] = m[4:5, :]
        ub[:, 0:D] = m[9:10, :]
        ub[:, D:FH] = m[10:11, :]
        db[...] = m[5:6, :]

    S = jax.ShapeDtypeStruct
    vm = pl.BlockSpec(memory_space=pltpu.VMEM)
    shapes = [(3, D, HALF), (HALF, D), (D, FH), (FH, D), (2, D), (2, D), (1, HALF), (1, HALF), (1, D), (1, FH), (1, D)]
    return pl.pallas_call(kernel, out_shape=[S(t, F32) for t in shapes], in_specs=[vm] * 5, out_specs=[vm] * 11, name="widen")(
        FH_, FO_, FU_, FD_, sm)


def solution(mesh):
    ndp = mesh.shape["dp"]

    def local(inputs, norm_scale, norm_shift, head_weight, query_bias, value_bias, out_weight, out_bias, up_weight, up_bias,
              down_weight, down_bias, cotangent):
        row = lambda b: b.reshape(1, b.shape[0])
        args = (inputs, cotangent, head_weight, out_weight, up_weight, down_weight, norm_scale, norm_shift, row(query_bias),
                row(value_bias), row(out_bias), row(up_bias), row(down_bias))
        lo, ig, gh, go, gu, gd, sm = main_call(args, inputs.shape[0], ndp)
        gh, go, gu, gd, sc, sh, qb, vb, ob, ub, db = widen(gh, go, gu, gd, sm)
        flat = lambda v: v.reshape(v.shape[1])
        return (lo, ig, sc, sh, gh, flat(qb), flat(vb), go, flat(ob), gu, flat(ub), gd, flat(db))

    rows, t0, t1 = P(("dp", "tensor"), None), P("tensor"), P(None, "tensor")
    tc = P("tensor", None)
    in_specs = (rows, P(), P(), P(None, None, "tensor"), t0, t0, tc, P(), t1, t0, tc, P(), rows)
    out_specs = (rows, rows, P(), P(), P(None, None, "tensor"), t0, t0, tc, P(), t1, t0, tc, P())
    return jax.shard_map(local, mesh=mesh, in_specs=in_specs, out_specs=out_specs, check_vma=False)
```

```python
import jax
import jax.numpy as jnp
from jax import lax
from jax.experimental import pallas as pl
from jax.experimental.pallas import tpu as pltpu
from jax.sharding import PartitionSpec as P

F32, BF16 = jnp.float32, jnp.bfloat16
NN, NT, TN = ((1,), (0,)), ((1,), (1,)), ((0,), (0,))
EPS = 1e-5
LOG2E = 1.4426950408889634
LN2 = 0.6931471805599453
C0, C1 = 0.7978845608, 0.044715
HD, BLK, D, HALF, FH, NH = 64, 256, 512, 256, 1024, 4
MESH = pl.DeviceIdType.MESH
VMEM_BYTES = 67043328


def dot(a, b, dims=NN):
    return lax.dot_general(a, b, (dims, ((), ())), preferred_element_type=F32)


def normed(v):
    c = jnp.mean(v, -1, keepdims=True)
    d = v - c
    r = lax.rsqrt(jnp.mean(d * d, -1, keepdims=True) + EPS)
    return d * r, r


def ln_back(g, xhat, r, gain):
    gx = g * gain
    return r * (gx - jnp.mean(gx, -1, keepdims=True) - xhat * jnp.mean(gx * xhat, -1, keepdims=True))


def rows_of(r):
    return pl.ds(pl.multiple_of(r * BLK, BLK), BLK)


def column(row):
    return jnp.broadcast_to(row, (8, row.shape[-1])).T[:, 0:1]


class Refs:
    pass


def ln1(z):
    def body(r, c):
        xh, _ = normed(z.x[rows_of(r), :].astype(F32))
        n = (xh * z.ns[0:1, :] + z.nsh[0:1, :]).astype(BF16)
        z.n1T[:, rows_of(r)] = n.T
        return c

    lax.fori_loop(0, z.nb, body, 0)


def qkv(z, s, h0, h1):
    cs = slice(h0 * HD, h1 * HD)
    qb, vb = column(z.qb[s][:, cs]), column(z.vb[s][:, cs])
    for b in range(z.nb):
        sl = slice(b * BLK, (b + 1) * BLK)
        nt = z.n1T[:, sl]
        q = dot(z.hw[s, 0, :, cs], nt, TN) + qb
        z.qT[s, cs, sl] = (q * (LOG2E / 8.0)).astype(BF16)
        z.kT[s, cs, sl] = dot(z.hw[s, 1, :, cs], nt, TN).astype(BF16)
        v = (dot(z.hw[s, 2, :, cs], nt, TN) + vb).astype(BF16)
        for h in range(h0, h1):
            z.vT[s, h, 0:HD, sl] = v[(h - h0) * HD : (h - h0 + 1) * HD]
            z.vT[s, h, HD : HD + 16, sl] = jnp.ones((16, BLK), BF16)


def attn_fwd(z, s, h0, h1, hook):
    def body(p, c):
        hrs = [pl.ds(pl.multiple_of(p * 2 * HD + j * HD, HD), HD) for j in (0, 1)]
        khs = [z.kT[s, hr, :].T for hr in hrs]

        def scores(j, b):
            return dot(khs[j][: BLK * (b + 1)], z.qT[s, hrs[j], b * BLK : (b + 1) * BLK])

        items = [(j, b) for j in (0, 1) for b in range(z.nb)]
        ahead = scores(*items[0])
        for i, (j, b) in enumerate(items):
            sc = ahead
            if i + 1 < len(items):
                ahead = scores(*items[i + 1])
            h, hr = 2 * p + j, hrs[j]
            nk = BLK * (b + 1)
            off = BLK * (b * (b + 1) // 2)
            sl = slice(b * BLK, nk)
            m = jnp.max(sc, 0, keepdims=True)
            e = jnp.exp2(sc - m).astype(BF16)
            z.E[s * NH + h, off : off + nk, :] = e
            o = dot(z.vT[s, h, :, 0:nk], e)
            rl = 1.0 / o[HD : HD + 1]
            z.rl[s * NH + h, 0:1, sl] = rl
            z.mixT[s, hr, sl] = (o[0:HD] * rl).astype(BF16)
        hook(p)
        return c

    lax.fori_loop(h0 // 2, h1 // 2, body, 0)


def out_proj(z):
    for r in range(z.nb):
        sl = slice(r * BLK, (r + 1) * BLK)
        t = dot(z.mixT[0, :, sl], z.ow[0], TN) + dot(z.mixT[1, :, sl], z.ow[1], TN)
        res = z.x[sl, :].astype(F32) + (t + z.ob[...])
        z.res[sl, :] = res
        z.oacc[sl, :] = res + z.db[...]
        xh, _ = normed(res)
        z.n2[sl, :] = (xh * z.ns[1:2, :] + z.nsh[1:2, :]).astype(BF16)


def ffn(z, part, s, hook):
    first, last = (part, s) == (0, 1), (part, s) == (1, 0)
    fs = slice(part * 512, part * 512 + 512)

    def products(rr):
        ct = z.cot[rr, :]
        return ct, dot(z.n2[rr, :], z.uw[s, :, fs]) + z.ub[s][:, fs], dot(ct, z.dw[s, fs, :], NT)

    def body(p, c):
        blocks = [rows_of(2 * p), rows_of(2 * p + 1)]
        ahead = products(blocks[0])
        for i, rr in enumerate(blocks):
            ct, u, da = ahead
            if i == 0:
                ahead = products(blocks[1])
            u2 = u * u
            t = jnp.tanh(u * (C0 + (C0 * C1) * u2))
            hp = 0.5 + 0.5 * t
            z.act[s, rr, fs] = (u * hp).astype(BF16)
            gp = hp + (u * (0.5 - 0.5 * t * t)) * (C0 + (3 * C0 * C1) * u2)
            dp = (da * gp).astype(BF16)
            z.dpre[s, rr, fs] = dp
            g = dot(dp, z.uw[s, :, fs], NT)
            g2 = g if first else z.g2[rr, :] + g
            if not last:
                z.g2[rr, :] = g2
            else:
                xh, rs = normed(z.res[rr, :])
                gres = ct.astype(F32) + ln_back(g2, xh, rs, z.ns[1:2, :])
                br = gres.astype(BF16)
                z.res[rr, :] = gres
                z.br[rr, :] = br
                c = (
                    c[0] + jnp.sum(g2 * xh, 0, keepdims=True),
                    c[1] + jnp.sum(g2, 0, keepdims=True),
                    c[2] + jnp.sum(br.astype(F32), 0, keepdims=True),
                    c[3] + jnp.sum(ct.astype(F32), 0, keepdims=True),
                )
        hook(p)
        return c

    zero = jnp.zeros((1, D), F32)
    c = lax.fori_loop(0, z.nb // 2, body, (zero,) * 4 if last else 0)
    if last:
        z.sm[1:2, :] = c[0]
        z.sm[3:4, :] = c[1]
        z.sm[4:5, :] = c[2]
        z.sm[5:6, :] = c[3]


def ffn_out(z, blocks):
    for r in blocks:
        rr = slice(r * BLK, (r + 1) * BLK)
        o = dot(z.act[0, rr, :], z.dw[0]) + dot(z.act[1, rr, :], z.dw[1])
        z.lo[rr, :] = (z.oacc[rr, :] + o).astype(BF16)


def d_down(z, part, s):
    for f in range(0, 512, 256):
        a = part * 512 + f
        z.GD[part][s][f : f + 256, :] = dot(z.act[s, :, a : a + 256], z.cot[...], TN).astype(BF16)


def d_up(z, part, s):
    z.GU[part][s][...] = dot(z.n2[...], z.dpre[s, :, part * 512 : part * 512 + 512], TN).astype(BF16)


def d_upb(z, s):
    ones = jnp.ones((8, z.dpre.shape[1]), BF16)
    for i in range(FH // 512):
        row = 9 + 8 * s + i
        z.sm[row : row + 1, :] = dot(ones, z.dpre[s, :, i * 512 : (i + 1) * 512])[0:1]


def d_out(z, s):
    z.GO[s][...] = dot(z.mixT[s], z.br[...]).astype(BF16)


def grad_mixed(z, s):
    for r in range(z.nb):
        sl = slice(r * BLK, (r + 1) * BLK)
        z.gmT[s, :, sl] = dot(z.ow[s], z.br[sl, :], NT).astype(BF16)


def attn_bwd(z, s, hook):
    def body(h, c):
        hr = pl.ds(pl.multiple_of(h * HD, HD), HD)
        hi = s * NH + h
        vh = z.vT[s, h, 0:HD, :].T
        gs = (z.gmT[s, hr, :].astype(F32) * z.rl[hi]).astype(BF16)
        delta = jnp.sum(gs.astype(F32) * z.mixT[s, hr, :].astype(F32), 0, keepdims=True)
        dprob = lambda b: dot(vh[: BLK * (b + 1)], gs[:, b * BLK : (b + 1) * BLK])
        ahead = dprob(0)
        for b in range(z.nb):
            dp = ahead
            if b + 1 < z.nb:
                ahead = dprob(b + 1)
            nk = BLK * (b + 1)
            off = BLK * (b * (b + 1) // 2)
            sl = slice(b * BLK, nk)
            gq = gs[:, sl]
            e = z.E[hi, off : off + nk, :]
            dv = dot(gq, e, NT)
            ds = (e.astype(F32) * (dp - delta[:, sl])).astype(BF16)
            z.dh[0:HD, sl] = (dot(z.kT[s, hr, 0:nk], ds) * 0.125).astype(BF16)
            dk = dot(z.qT[s, hr, sl], ds, NT)
            if b:
                z.dva[:, 0 : nk - BLK] = z.dva[:, 0 : nk - BLK] + dv[:, 0 : nk - BLK]
                z.dka[:, 0 : nk - BLK] = z.dka[:, 0 : nk - BLK] + dk[:, 0 : nk - BLK]
            z.dva[:, sl] = dv[:, nk - BLK : nk]
            z.dka[:, sl] = dk[:, nk - BLK : nk]
        z.dh[HD : 2 * HD, :] = (z.dka[...] * LN2).astype(BF16)
        z.dh[2 * HD : 3 * HD, :] = z.dva[...].astype(BF16)
        for j in range(3):
            z.dT[s, pl.ds(pl.multiple_of(j * HALF + h * HD, HD), HD), :] = z.dh[j * HD : (j + 1) * HD, :]
        g = dot(z.dh[...], z.n1T[...], NT).astype(BF16)
        for q in range(4):
            z.GH[s][h, q * 192 : (q + 1) * 192, :] = g[:, q * 128 : (q + 1) * 128]
        hook(h)
        return c

    lax.fori_loop(0, NH, body, 0)


def d_headb(z, s):
    ones = jnp.ones((8, z.dT.shape[2]), BF16)
    for i, j in enumerate((0, 2)):
        row = 8 + 8 * s
        z.sm[row : row + 1, i * HALF : (i + 1) * HALF] = dot(ones, z.dT[s, j * HALF : (j + 1) * HALF, :], NT)[0:1]


def grad_in(z, hook):
    zero = jnp.zeros((1, D), F32)
    sc, sh = zero, zero
    for r in range(z.nb):
        sl = slice(r * BLK, (r + 1) * BLK)
        g = 0.0
        for s in (0, 1):
            for j in range(3):
                g = g + dot(z.hw[s, j], z.dT[s, j * HALF : (j + 1) * HALF, sl])
        g = g.T
        xh, rs = normed(z.x[sl, :].astype(F32))
        z.ig[sl, :] = (z.res[sl, :] + ln_back(g, xh, rs, z.ns[0:1, :])).astype(BF16)
        sc = sc + jnp.sum(g * xh, 0, keepdims=True)
        sh = sh + jnp.sum(g, 0, keepdims=True)
        if r == z.nb - 1:
            z.sm[0:1, :] = sc
            z.sm[2:3, :] = sh
        hook(f"gin{r}")


class Comm:
    def __init__(self, ndp, groups, send, recv, local):
        self.send, self.recv, self.local = send, recv, local
        self.count, self.local_count, self.pending = 0, 0, []
        me = lax.axis_index("dp")
        self.levels = [1 << i for i in range(ndp.bit_length() - 1)]
        self.bit = {b: (me // b) % 2 for b in self.levels}
        self.me = me
        self.greet = ["t"] + [([b], 1) for b in self.levels] + [(g, d) for g in groups for d in range(1, 1 << len(g)) if d & (d - 1)]
        self.peer = 1 - lax.axis_index("tensor")

    def where(self, axis):
        if axis == "t":
            return {"tensor": self.peer}
        bits, delta = axis
        return {"dp": self.me + sum(b - 2 * b * self.bit[b] for i, b in enumerate(bits) if delta >> i & 1)}

    def barrier_signal(self):
        sem = pltpu.get_barrier_semaphore()
        for axis in self.greet:
            pl.semaphore_signal(sem, inc=1, device_id=self.where(axis), device_id_type=MESH)

    def barrier_wait(self):
        pl.semaphore_wait(pltpu.get_barrier_semaphore(), len(self.greet))

    def copy(self, src, dst, axis, keep=True):
        i = self.count
        self.count += 1

        def make():
            return pltpu.make_async_remote_copy(
                src_ref=src(), dst_ref=dst(), send_sem=self.send.at[i], recv_sem=self.recv.at[i],
                device_id=self.where(axis), device_id_type=MESH)

        if keep:
            self.pending.append(make)
        return make

    def here(self, src, dst):
        i = self.local_count
        self.local_count += 1
        return lambda: pltpu.make_async_copy(src(), dst(), self.local.at[i])

    def drain(self):
        for make in self.pending:
            make().wait_send()


def add_rows(dst, srcs, at, n, cols):
    ch = next(c for c in (384, 256, 192, 128, 96, 64, 48, 32, 16, 8, 4) if n % c == 0 and c * cols <= 49152)

    def body(i, c):
        o = pl.ds(pl.multiple_of(at + i * ch, ch), ch)
        f = pl.ds(pl.multiple_of(i * ch, ch), ch)
        if len(srcs) == 1:
            dst[o, :] = dst[o, :] + srcs[0][f, :]
        else:
            dst[o, :] = pairwise([dst[o, :].astype(F32)] + [s[f, :].astype(F32) for s in srcs]).astype(dst.dtype)
        return c

    lax.fori_loop(0, n // ch, body, 0)


def pairwise(v):
    while len(v) > 1:
        v = [v[i] + v[i + 1] for i in range(0, len(v), 2)]
    return v[0]


def sizes_of(rows, stages):
    n = [rows]
    for bits in stages:
        n.append(n[-1] >> len(bits))
    return n


def job_scratch(rows, cols, stages, pre, extra):
    V = pltpu.VMEM
    n = sizes_of(rows, stages)
    bufs = lambda ss: [V((n[k + 1], cols), BF16) for k in range(ss) for _ in range((1 << len(stages[k])) - 1)]
    return bufs(len(stages)) + bufs(pre) + [V((n[pre], cols), BF16)] + [V((n[-1], cols), BF16) for _ in range(extra)] + [V((rows, cols), BF16)]


class Job:
    def __init__(self, c, own, peer, refs, rows, cols, stages, pre, out):
        S = len(stages)
        done = sum(len(b) for b in stages)
        extra = c.levels[done:]
        n = sizes_of(rows, stages)
        refs = list(refs)
        take = lambda m: [refs.pop(0) for _ in range(m)]
        r_own = [take((1 << len(b)) - 1) for b in stages]
        r_peer = [take((1 << len(b)) - 1) for b in stages[:pre]]
        r_t, r_x, full = take(1)[0], take(len(extra)), refs.pop(0)

        def code(bits, delta):
            return sum((c.bit[b] if not delta >> i & 1 else 1 - c.bit[b]) * (1 << i) for i, b in enumerate(bits))

        lo = [0]
        for k, b in enumerate(stages):
            lo.append(lo[k] + code(b, 0) * n[k + 1])
        at = lambda k: pl.ds(pl.multiple_of(lo[k], n[k]) if k else 0, n[k])
        theirs = lambda k, d: pl.ds(pl.multiple_of(lo[k] + code(stages[k], d) * n[k + 1], n[k + 1]), n[k + 1])

        def scatter(g, bufs, k):
            return [c.copy(lambda d=d: g().at[theirs(k, d)], lambda d=d: bufs[d - 1], (stages[k], d)) for d in range(1, len(bufs) + 1)]

        s_own = [scatter(own, r_own[k], k) for k in range(S)]
        s_peer = [scatter(peer, r_peer[k], k) for k in range(pre)]
        s_t = c.copy(lambda: peer().at[at(pre)], lambda: r_t, "t")
        s_x = [c.copy(lambda: own().at[at(S)], lambda i=i: r_x[i], ([b], 1), False) for i, b in enumerate(extra)]
        s_g = [[c.copy(lambda k=k: full.at[at(k + 1)], lambda k=k: full.at[at(k + 1)], (stages[k], d)) for d in range(1, 1 << len(stages[k]))]
               for k in range(S)]
        s_out = c.here(lambda: full, lambda: out())
        self.wait_out = lambda: s_out().wait()
        start = lambda ss: [s().start() for s in ss]
        arrived = lambda ss: [s().wait_recv() for s in ss]

        def end(s, g, buf, k):
            arrived(s[k])
            add_rows(g(), buf[k], lo[k + 1], n[k + 1], cols)

        def peer_step(i):
            if i:
                end(s_peer, peer, r_peer, i - 1)
            start(s_peer[i] if i < pre else [s_t])

        def own_step(i):
            if i == 0:
                start(s_own[0])
            elif i <= S:
                end(s_own, own, r_own, i - 1)
                if i == pre:
                    assert not self.peer_steps
                    s_t().wait_recv()
                    add_rows(own(), [r_t], lo[pre], n[pre], cols)
                if i < S:
                    start(s_own[i])
                    return
                for j in range(len(extra)):
                    s_x[j]().start()
                    s_x[j]().wait()
                    add_rows(own(), [r_x[j]], lo[S], n[S], cols)
                full[at(S), :] = own()[at(S), :]
                start(s_g[S - 1])
            else:
                k = 2 * S - i
                arrived(s_g[k])
                if k:
                    start(s_g[k - 1])
                else:
                    s_out().start()

        self.peer_steps = [lambda i=i: peer_step(i) for i in range(pre + 1)]
        self.own_steps = [lambda i=i: own_step(i) for i in range(2 * S + 1)]

    def own(self):
        self.own_steps.pop(0)()

    def peer(self):
        self.peer_steps.pop(0)()


SMALL_STAGES = [[1], [2], [4, 8]]


class Small:
    def __init__(self, c, sm, bufs):
        bufs = list(bufs)
        r_t = bufs.pop(0)
        st = SMALL_STAGES + [[b] for b in c.levels[4:]]
        s_t = [c.copy(lambda: sm.at[0:8], lambda: r_t.at[0:8], "t", False), c.copy(lambda: sm.at[16:24], lambda: r_t.at[8:16], "t", False)]
        rs, ss = [[r_t]], [s_t]
        for bits in st:
            r = [bufs.pop(0) for _ in range((1 << len(bits)) - 1)]
            rs.append(r)
            ss.append([c.copy(lambda: sm.at[0:16], lambda b=b: b, (bits, d + 1), False) for d, b in enumerate(r)])

        def step(i):
            if i:
                for s in ss[i - 1]:
                    s().wait()
                sm[0:16, :] = pairwise([sm[0:16, :]] + [r[...] for r in rs[i - 1]])
            if i < len(ss):
                for s in ss[i]:
                    s().start()

        self.steps = [lambda i=i: step(i) for i in range(len(ss) + 1)]

    def own(self):
        self.steps.pop(0)()


INS = ["x_h", "cot_h", "hw_h", "ow_h", "uw_h", "dw_h", "ns", "nsh", "qb_o", "vb_o", "ob", "ub_o", "db"]
OUTS = ["lo_h", "ig_h", "FH_h", "FO_h", "FU_h", "FD_h", "smo"]
Y4, Z14, G8 = [[1], [2], [4, 8]], [[1], [4], [2], [8]], [[1], [2, 4, 8]]
JOBS = [("D0", 512, 512, [[1], [2], [4, 8]], 1),
        ("U0", 512, 512, [[1], [2], [4, 8]], 2),
        ("D1", 512, 512, [[1], [2], [4, 8]], 1),
        ("U1", 512, 512, [[1], [2], [4, 8]], 2),
        ("O", 256, 512, [[1], [2], [4, 8]], 1),
        ("H0", 768, 128, [[1], [2], [4, 8]], 1),
        ("H1", 768, 128, [[1], [2], [4, 8]], 1),
        ("H2", 768, 128, [[1], [2], [4, 8]], 2),
        ("H3", 768, 128, [[1], [2], [4, 8]], 1)]

HOOKS = {
    "f0_0": ["WhwA"],
    "f0_1": ["WhwB", "Wow"],
    "qkv1a": ["Wu0"],
    "f1_0": ["Wd0", "WhwB", "Wow"],
    "qkv1b": ["Wu1", "Wu0"],
    "f1_1": ["Wd0", "Wd1"],
    "ffn01_0": ["Wu1"],
    "dD01": ["D0p"],
    "dU01": ["Wd1", "U0p"],
    "ffn00_0": ["D0p"],
    "ffn00_1": ["U0p"],
    "dD00": ["D0o"],
    "dU00": ["U0o"],
    "ffn11_1": ["U0o"],
    "dD11": ["U0p", "D1p"],
    "dU11": ["U1p"],
    "ffn10_0": ["D0o", "D1p", "U1p"],
    "dD10": ["D1o"],
    "dU10": ["U0o", "U1o"],
    "dO1": ["Op"],
    "gm": ["U1o", "D0o", "Op"],
    "b1_0": ["H0p"],
    "b1_1": ["U0o", "U1p", "H0p", "H1p", "D1o"],
    "b1_2": ["D0o", "Oo", "H2p"],
    "b1_3": ["H1p", "H3p", "H2p", "U1o", "Oo"],
    "b0_0": ["D1o", "H0o", "H3p"],
    "b0_1": ["U0o", "H2p", "H1o", "H0o", "D0o", "Oo"],
    "b0_2": ["U1o", "H2o", "H1o"],
    "b0_3": ["D1o", "U0o", "H2o", "H3o"],
    "gin0": ["H0o", "Oo"],
    "gin1": ["U0o", "H3o"],
    "gin3": ["D0o", "So", "U1o"],
    "fo1": ["H1o"],
    "fo2": ["D0o"],
    "fo3": ["H2o", "So"],
    "tail": ["D1o", "H3o", "H0o", "So", "Oo", "U1o", "H1o", "H2o", "U1o", "H3o", "D1o", "H0o", "So", "H1o", "Oo", "H2o", "Oo", "H0o", "H3o", "D1o", "H1o", "H0o", "H2o", "H1o", "So", "H3o", "H2o", "H3o"],
}
BEFORE = {
    "qkv1a": ["WhwA"],
}


def scratch(T, ndp):
    nb = T // BLK
    V = pltpu.VMEM
    lv = ndp.bit_length() - 1
    s = dict(
        x=V((T, D), BF16), cot=V((T, D), BF16), hw=V((2, 3, D, HALF), BF16), ow=V((2, HALF, D), BF16),
        uw=V((2, D, FH), BF16), dw=V((2, FH, D), BF16),
        qb_p=V((1, HALF), F32), vb_p=V((1, HALF), F32), ub_p=V((1, FH), F32),
        n1T=V((D, T), BF16), qT=V((2, HALF, T), BF16), kT=V((2, HALF, T), BF16), vT=V((2, NH, 80, T), BF16),
        E=V((2 * NH, BLK * nb * (nb + 1) // 2, BLK), BF16), rl=V((2 * NH, 1, T), F32), mixT=V((2, HALF, T), BF16),
        res=V((T, D), F32), n2=V((T, D), BF16), act=V((2, T, FH), BF16), dpre=V((2, T, FH), BF16),
        oacc=V((T, D), F32), g2=V((T, D), F32), br=V((T, D), BF16), gmT=V((2, HALF, T), BF16),
        dh=V((3 * HD, T), BF16), dva=V((HD, T), F32), dka=V((HD, T), F32), sm=V((24, D), F32),
        GD0o=V((FH // 2, D), BF16), GD0p=V((FH // 2, D), BF16), GD1o=V((FH // 2, D), BF16), GD1p=V((FH // 2, D), BF16),
        GU0o=V((D, FH // 2), BF16), GU0p=V((D, FH // 2), BF16), GU1o=V((D, FH // 2), BF16), GU1p=V((D, FH // 2), BF16),
        GOo=V((HALF, D), BF16), GOp=V((HALF, D), BF16), GHo=V((NH, 768, 128), BF16), GHp=V((NH, 768, 128), BF16),
        s0=V((16, D), F32))
    for i in range(5 + lv - 4):
        s[f"s{i + 1}"] = V((16, D), F32)
    for name, rows, cols, stages, pre in JOBS:
        for i, v in enumerate(job_scratch(rows, cols, stages, pre, lv - 4)):
            s[f"{name}_{i}"] = v
    s["send"] = pltpu.SemaphoreType.DMA((224 + 24 * (lv - 4),))
    s["recv"] = pltpu.SemaphoreType.DMA((224 + 24 * (lv - 4),))
    s["local"] = pltpu.SemaphoreType.DMA((32,))
    return s


def run(z, ndp):
    c = Comm(ndp, [[4, 8], [2, 4, 8]], z.send, z.recv, z.local)
    lv = c.levels
    c.barrier_signal()
    slot0 = lambda r: r.at[0]
    loads = {n: c.here(lambda n=n: getattr(z, n + "_h"), lambda n=n, d=d: d(getattr(z, n)))
             for n, d in (("x", lambda r: r), ("hw", slot0), ("cot", lambda r: r), ("ow", slot0), ("uw", slot0), ("dw", slot0))}
    for n in ("x", "hw", "ow", "cot", "uw", "dw"):
        loads[n]().start()

    pieces = {"hwA": ("hw", D, 0, slice(0, 128)), "hwB": ("hw", D, 0, slice(128, 256)), "ow": ("ow", HALF, 0, slice(None)),
              "u0": ("uw", D, 0, slice(0, 512)), "d0": ("dw", 512, 0, slice(None)), "u1": ("uw", D, 0, slice(512, 1024)),
              "d1": ("dw", 512, 512, slice(None))}

    def view(name, flip, lead):
        n, m, base, cols = pieces[name]
        q = (c.bit[1] if not flip & 1 else 1 - c.bit[1]) + 2 * (c.bit[2] if not flip & 2 else 1 - c.bit[2])
        rows = pl.ds(pl.multiple_of(base + q * (m // 4), m // 4), m // 4)
        r = getattr(z, n).at[1] if lead else getattr(z, n + "_h")
        return r.at[:, rows, cols] if n == "hw" else r.at[rows, cols]

    W = {}
    for name in pieces:
        put = lambda flip, name=name: view(name, flip, True)
        W[name] = dict(
            x=c.copy(lambda name=name: view(name, 0, False), lambda put=put: put(0), "t"),
            s=c.copy(lambda put=put: put(0), lambda put=put: put(0), ([1], 1)),
            y=c.copy(lambda put=put: put(0), lambda put=put: put(0), ([2], 1)),
            r=c.copy(lambda put=put: put(2), lambda put=put: put(2), ([1], 1)))
    wb = [c.copy(lambda n=n: getattr(z, n + "_o"), lambda n=n: getattr(z, n + "_p"), "t") for n in ("qb", "vb", "ub")]

    def relay1(n):
        W[n]["x"]().wait_recv()
        W[n]["y"]().start()
        W[n]["s"]().start()

    def relay2(n):
        W[n]["y"]().wait_recv()
        W[n]["r"]().start()

    def arrive(n):
        W[n]["s"]().wait_recv()
        W[n]["r"]().wait_recv()

    c.barrier_wait()
    W["hwA"]["x"]().start()
    for b in wb:
        b().start()
    for n in list(pieces)[1:]:
        W[n]["x"]().start()

    z.qb, z.vb, z.ub = (z.qb_o, z.qb_p), (z.vb_o, z.vb_p), (z.ub_o, z.ub_p)
    z.GD = ((z.GD0o, z.GD0p), (z.GD1o, z.GD1p))
    z.GU = ((z.GU0o, z.GU0p), (z.GU1o, z.GU1p))
    z.GO, z.GH = (z.GOo, z.GOp), (z.GHo, z.GHp)
    z.dT, z.lo, z.ig = z.dpre, z.br, z.n2
    ends = dict(D0=lambda: z.FD_h.at[0 : FH // 2], D1=lambda: z.FD_h.at[FH // 2 : FH], U0=lambda: z.FU_h.at[:, 0 : FH // 2],
                U1=lambda: z.FU_h.at[:, FH // 2 : FH], O=lambda: z.FO_h)
    srcs = dict(D0=(lambda: z.GD0o, lambda: z.GD0p), D1=(lambda: z.GD1o, lambda: z.GD1p), U0=(lambda: z.GU0o, lambda: z.GU0p),
                U1=(lambda: z.GU1o, lambda: z.GU1p), O=(lambda: z.GOo, lambda: z.GOp))
    for i in range(NH):
        ends[f"H{i}"] = lambda i=i: z.FH_h.at[i]
        srcs[f"H{i}"] = (lambda i=i: z.GHo.at[i], lambda i=i: z.GHp.at[i])
    jobs = {}
    for name, rows, cols, stages, pre in JOBS:
        refs = [getattr(z, f"{name}_{i}") for i in range(len(job_scratch(rows, cols, stages, pre, len(lv) - 4)))]
        jobs[name] = Job(c, *srcs[name], refs, rows, cols, stages, pre, ends[name])
    jobs["S"] = small = Small(c, z.sm, [getattr(z, f"s{i}") for i in range(6 + len(lv) - 4)])
    s_lo, s_ig = c.here(lambda: z.lo, lambda: z.lo_h), c.here(lambda: z.ig, lambda: z.ig_h)

    relays = {n: [relay1, relay2] for n in W}

    def go(words):
        for word in words:
            if word[1:] in relays:
                relays[word[1:]].pop(0)(word[1:])
            else:
                (jobs[word[:-1]].own if word[-1] == "o" else jobs[word[:-1]].peer)()

    def at(name, n):
        table = {k: HOOKS.get(f"{name}_{k}", ()) for k in (range(n) if isinstance(n, int) else n)}

        def hook(h):
            for k, what in table.items():
                if what:
                    @pl.when(h == k)
                    def _():
                        go(what)
        return hook

    def before(name):
        go(BEFORE.get(name, ()))

    def after(name):
        go(HOOKS.get(name, ()))

    z.sm[...] = jnp.zeros_like(z.sm)
    loads["x"]().wait()
    ln1(z)
    loads["hw"]().wait()
    qkv(z, 0, 0, NH)
    after("qkv0")
    attn_fwd(z, 0, 0, NH, at("f0", NH // 2))
    before("qkv1a")
    for b in wb:
        b().wait_recv()
    arrive("hwA")
    qkv(z, 1, 0, 2)
    after("qkv1a")
    attn_fwd(z, 1, 0, 2, at("f1", range(0, 1)))
    before("qkv1b")
    arrive("hwB")
    qkv(z, 1, 2, 4)
    after("qkv1b")
    attn_fwd(z, 1, 2, 4, at("f1", range(1, 2)))
    before("out")
    arrive("ow")
    loads["ow"]().wait()
    out_proj(z)
    for n in ("cot", "uw", "dw"):
        loads[n]().wait()
    after("out")
    for part in (0, 1):
        for s in (1, 0):
            name = f"ffn{part}{s}"
            before(name + "_0")
            if s:
                arrive(f"u{part}")
                arrive(f"d{part}")
            ffn(z, part, s, at(name, z.nb // 2))
            d_down(z, part, s)
            after(f"dD{part}{s}")
            d_up(z, part, s)
            if part:
                d_upb(z, s)
            after(f"dU{part}{s}")
    for s in (1, 0):
        d_out(z, s)
        after(f"dO{s}")
    grad_mixed(z, 1)
    grad_mixed(z, 0)
    after("gm")
    attn_bwd(z, 1, at("b1", NH))
    attn_bwd(z, 0, at("b0", NH))
    d_headb(z, 0)
    d_headb(z, 1)
    after("hb")
    grad_in(z, after)
    s_ig().start()
    for r in range(z.nb):
        ffn_out(z, (r,))
        after(f"fo{r}")
    s_lo().start()
    after("tail")
    while small.steps:
        small.own()
    assert not any(v for v in relays.values()) and not any(jobs[n].own_steps for n in jobs if n != "S")
    z.smo[...] = z.sm[0:16, :]
    s_ig().wait()
    s_lo().wait()
    for n in jobs:
        if n != "S":
            jobs[n].wait_out()
    c.drain()


def main_call(args, T, ndp):
    scr = scratch(T, ndp)
    names = INS + OUTS + list(scr)

    def kernel(*refs):
        z = Refs()
        for n, r in zip(names, refs):
            setattr(z, n, r)
        z.nb = T // BLK
        run(z, ndp)

    S = jax.ShapeDtypeStruct
    outs = [S((T, D), BF16), S((T, D), BF16), S((NH, 768, 128), BF16), S((HALF, D), BF16), S((D, FH), BF16), S((FH, D), BF16),
            S((16, D), F32)]
    vm, hbm = pl.BlockSpec(memory_space=pltpu.VMEM), pl.BlockSpec(memory_space=pl.ANY)
    return pl.pallas_call(
        kernel, out_shape=outs, in_specs=[hbm] * 6 + [vm] * 7, out_specs=[hbm] * 6 + [vm], scratch_shapes=list(scr.values()),
        compiler_params=pltpu.CompilerParams(vmem_limit_bytes=VMEM_BYTES, collective_id=0, has_side_effects=True),
        name="layer")(*args)


def widen(FH_, FO_, FU_, FD_, sm, lo, ig):
    def kernel(h, o, u, d, m, l, g, ho, oo, uo, do, lo_, go, sc, sh, qb, vb, ob, ub, db, hv, ov, uv, dv, lv, gv, hf, of, uf, df, si, so):
        ins, outs = [], []

        def load(src, dst):
            c = pltpu.make_async_copy(src, dst, si.at[len(ins)])
            ins.append(c)
            c.start()
            return c

        def store(src, dst):
            c = pltpu.make_async_copy(src, dst, so.at[len(outs)])
            outs.append(c)
            c.start()

        top, bottom = slice(0, 512), slice(512, 1024)
        left, right = slice(0, 256), slice(256, 512)
        i_g, i_l = load(g, gv), load(l, lv)
        i_d0, i_h = load(d.at[top], dv.at[top]), load(h, hv)
        i_d1 = load(d.at[bottom], dv.at[bottom])
        i_u0, i_u1 = load(u.at[left], uv.at[left]), load(u.at[right], uv.at[right])
        i_o = load(o, ov)
        sc[...] = m[0:2, :]
        sh[...] = m[2:4, :]
        qb[...] = m[8:9, 0:HALF]
        vb[...] = m[8:9, HALF:D]
        ob[...] = m[4:5, :]
        ub[:, 0:D] = m[9:10, :]
        ub[:, D:FH] = m[10:11, :]
        db[...] = m[5:6, :]
        i_g.wait()
        store(gv, go)
        i_l.wait()
        store(lv, lo_)

        def piece(c, v, f, out, rows):
            c.wait()
            f[rows, :] = v[rows, :].astype(F32)
            store(f.at[rows], out.at[rows])

        piece(i_d0, dv, df, do, top)
        i_h.wait()
        for j in range(3):
            for q in range(4):
                for p in range(2):
                    rows = [hv[2 * p + i, q * 192 + j * HD : q * 192 + (j + 1) * HD, :] for i in range(2)]
                    hf[j, q * 128 : (q + 1) * 128, p * 128 : (p + 1) * 128] = jnp.concatenate(rows, 0).astype(F32).T
            store(hf.at[j], ho.at[j])
        piece(i_d1, dv, df, do, bottom)
        piece(i_u0, uv, uf, uo, left)
        piece(i_u1, uv, uf, uo, right)
        piece(i_o, ov, of, oo, left)
        for c in outs:
            c.wait()

    S, V = jax.ShapeDtypeStruct, pltpu.VMEM
    vm, hbm = pl.BlockSpec(memory_space=pltpu.VMEM), pl.BlockSpec(memory_space=pl.ANY)
    big = [(3, D, HALF), (HALF, D), (D, FH), (FH, D)]
    small = [(2, D), (2, D), (1, HALF), (1, HALF), (1, D), (1, FH), (1, D)]
    rows = S(lo.shape, BF16)
    out_shape = [S(t, F32) for t in big] + [rows, rows] + [S(t, F32) for t in small]
    bufs = [V((NH, 768, 128), BF16)] + [V(t, BF16) for t in big[1:]] + [V(lo.shape, BF16)] * 2 + [V(t, F32) for t in big]
    return pl.pallas_call(
        kernel, out_shape=out_shape, in_specs=[hbm] * 4 + [vm] + [hbm] * 2, out_specs=[hbm] * 6 + [vm] * 7,
        scratch_shapes=bufs + [pltpu.SemaphoreType.DMA((8,)), pltpu.SemaphoreType.DMA((10,))],
        compiler_params=pltpu.CompilerParams(vmem_limit_bytes=VMEM_BYTES), name="widen")(FH_, FO_, FU_, FD_, sm, lo, ig)


def solution(mesh):
    ndp = mesh.shape["dp"]

    def local(inputs, norm_scale, norm_shift, head_weight, query_bias, value_bias, out_weight, out_bias, up_weight, up_bias,
              down_weight, down_bias, cotangent):
        row = lambda b: b.reshape(1, b.shape[0])
        args = (inputs, cotangent, head_weight, out_weight, up_weight, down_weight, norm_scale, norm_shift, row(query_bias),
                row(value_bias), row(out_bias), row(up_bias), row(down_bias))
        lo, ig, gh, go, gu, gd, sm = main_call(args, inputs.shape[0], ndp)
        gh, go, gu, gd, lo, ig, sc, sh, qb, vb, ob, ub, db = widen(gh, go, gu, gd, sm, lo, ig)
        flat = lambda v: v.reshape(v.shape[1])
        return (lo, ig, sc, sh, gh, flat(qb), flat(vb), go, flat(ob), gu, flat(ub), gd, flat(db))

    rows, t0, t1 = P(("dp", "tensor"), None), P("tensor"), P(None, "tensor")
    tc = P("tensor", None)
    in_specs = (rows, P(), P(), P(None, None, "tensor"), t0, t0, tc, P(), t1, t0, tc, P(), rows)
    out_specs = (rows, rows, P(), P(), P(None, None, "tensor"), t0, t0, tc, P(), t1, t0, tc, P())
    return jax.shard_map(local, mesh=mesh, in_specs=in_specs, out_specs=out_specs, check_vma=False)
```

```python
import jax
import jax.numpy as jnp
from jax import lax
from jax.experimental import pallas as pl
from jax.experimental.pallas import tpu as pltpu
from jax.sharding import PartitionSpec as P

F32, BF16 = jnp.float32, jnp.bfloat16
NN, NT, TN = ((1,), (0,)), ((1,), (1,)), ((0,), (0,))
EPS = 1e-5
LOG2E = 1.4426950408889634
LN2 = 0.6931471805599453
C0, C1 = 0.7978845608, 0.044715
HD, BLK, D, HALF, FH, NH = 64, 256, 512, 256, 1024, 4
MESH = pl.DeviceIdType.MESH
VMEM_BYTES = 67043328


def dot(a, b, dims=NN):
    return lax.dot_general(a, b, (dims, ((), ())), preferred_element_type=F32)


def normed(v):
    c = jnp.mean(v, -1, keepdims=True)
    d = v - c
    r = lax.rsqrt(jnp.mean(d * d, -1, keepdims=True) + EPS)
    return d * r, r


def ln_back(g, xhat, r, gain):
    gx = g * gain
    return r * (gx - jnp.mean(gx, -1, keepdims=True) - xhat * jnp.mean(gx * xhat, -1, keepdims=True))


def rows_of(r):
    return pl.ds(pl.multiple_of(r * BLK, BLK), BLK)


def column(row):
    return jnp.broadcast_to(row, (8, row.shape[-1])).T[:, 0:1]


class Refs:
    pass


def ln1(z):
    def body(r, c):
        xh, _ = normed(z.x[rows_of(r), :].astype(F32))
        n = (xh * z.ns[0:1, :] + z.nsh[0:1, :]).astype(BF16)
        z.n1T[:, rows_of(r)] = n.T
        return c

    lax.fori_loop(0, z.nb, body, 0)


def qkv(z, s, h0, h1):
    cs = slice(h0 * HD, h1 * HD)
    qb, vb = column(z.qb[s][:, cs]), column(z.vb[s][:, cs])
    for b in range(z.nb):
        sl = slice(b * BLK, (b + 1) * BLK)
        nt = z.n1T[:, sl]
        q = dot(z.hw[s, 0, :, cs], nt, TN) + qb
        z.qT[s, cs, sl] = (q * (LOG2E / 8.0)).astype(BF16)
        z.kT[s, cs, sl] = dot(z.hw[s, 1, :, cs], nt, TN).astype(BF16)
        v = (dot(z.hw[s, 2, :, cs], nt, TN) + vb).astype(BF16)
        for h in range(h0, h1):
            z.vT[s, h, 0:HD, sl] = v[(h - h0) * HD : (h - h0 + 1) * HD]
            z.vT[s, h, HD : HD + 16, sl] = jnp.ones((16, BLK), BF16)


def attn_fwd(z, s, h0, h1, hook):
    def body(p, c):
        hrs = [pl.ds(pl.multiple_of(p * 2 * HD + j * HD, HD), HD) for j in (0, 1)]
        khs = [z.kT[s, hr, :].T for hr in hrs]

        def scores(j, b):
            return dot(khs[j][: BLK * (b + 1)], z.qT[s, hrs[j], b * BLK : (b + 1) * BLK])

        items = [(j, b) for j in (0, 1) for b in range(z.nb)]
        ahead = scores(*items[0])
        for i, (j, b) in enumerate(items):
            sc = ahead
            if i + 1 < len(items):
                ahead = scores(*items[i + 1])
            h, hr = 2 * p + j, hrs[j]
            nk = BLK * (b + 1)
            off = BLK * (b * (b + 1) // 2)
            sl = slice(b * BLK, nk)
            m = jnp.max(sc, 0, keepdims=True)
            e = jnp.exp2(sc - m).astype(BF16)
            z.E[s * NH + h, off : off + nk, :] = e
            o = dot(z.vT[s, h, :, 0:nk], e)
            rl = 1.0 / o[HD : HD + 1]
            z.rl[s * NH + h, 0:1, sl] = rl
            z.mixT[s, hr, sl] = (o[0:HD] * rl).astype(BF16)
        hook(p)
        return c

    lax.fori_loop(h0 // 2, h1 // 2, body, 0)


def out_proj(z):
    for r in range(z.nb):
        sl = slice(r * BLK, (r + 1) * BLK)
        t = dot(z.mixT[0, :, sl], z.ow[0], TN) + dot(z.mixT[1, :, sl], z.ow[1], TN)
        res = z.x[sl, :].astype(F32) + (t + z.ob[...])
        z.res[sl, :] = res
        z.oacc[sl, :] = res + z.db[...]
        xh, _ = normed(res)
        z.n2[sl, :] = (xh * z.ns[1:2, :] + z.nsh[1:2, :]).astype(BF16)


def ffn(z, part, s, hook):
    first, last = (part, s) == (0, 1), (part, s) == (1, 0)
    fs = slice(part * 512, part * 512 + 512)

    def products(rr):
        ct = z.cot[rr, :]
        return ct, dot(z.n2[rr, :], z.uw[s, :, fs]) + z.ub[s][:, fs], dot(ct, z.dw[s, fs, :], NT)

    def body(p, c):
        blocks = [rows_of(2 * p), rows_of(2 * p + 1)]
        ahead = products(blocks[0])
        for i, rr in enumerate(blocks):
            ct, u, da = ahead
            if i == 0:
                ahead = products(blocks[1])
            u2 = u * u
            t = jnp.tanh(u * (C0 + (C0 * C1) * u2))
            hp = 0.5 + 0.5 * t
            z.act[s, rr, fs] = (u * hp).astype(BF16)
            gp = hp + (u * (0.5 - 0.5 * t * t)) * (C0 + (3 * C0 * C1) * u2)
            dp = (da * gp).astype(BF16)
            z.dpre[s, rr, fs] = dp
            g = dot(dp, z.uw[s, :, fs], NT)
            g2 = g if first else z.g2[rr, :] + g
            if not last:
                z.g2[rr, :] = g2
            else:
                xh, rs = normed(z.res[rr, :])
                gres = ct.astype(F32) + ln_back(g2, xh, rs, z.ns[1:2, :])
                br = gres.astype(BF16)
                z.res[rr, :] = gres
                z.br[rr, :] = br
                c = (
                    c[0] + jnp.sum(g2 * xh, 0, keepdims=True),
                    c[1] + jnp.sum(g2, 0, keepdims=True),
                    c[2] + jnp.sum(br.astype(F32), 0, keepdims=True),
                    c[3] + jnp.sum(ct.astype(F32), 0, keepdims=True),
                )
        hook(p)
        return c

    zero = jnp.zeros((1, D), F32)
    c = lax.fori_loop(0, z.nb // 2, body, (zero,) * 4 if last else 0)
    if last:
        z.sm[1:2, :] = c[0]
        z.sm[3:4, :] = c[1]
        z.sm[4:5, :] = c[2]
        z.sm[5:6, :] = c[3]


def ffn_out(z, blocks):
    for r in blocks:
        rr = slice(r * BLK, (r + 1) * BLK)
        o = dot(z.act[0, rr, :], z.dw[0]) + dot(z.act[1, rr, :], z.dw[1])
        z.lo[rr, :] = (z.oacc[rr, :] + o).astype(BF16)


def d_down(z, part, s):
    for f in range(0, 512, 256):
        a = part * 512 + f
        z.GD[part][s][f : f + 256, :] = dot(z.act[s, :, a : a + 256], z.cot[...], TN).astype(BF16)


def d_up(z, part, s):
    z.GU[part][s][...] = dot(z.n2[...], z.dpre[s, :, part * 512 : part * 512 + 512], TN).astype(BF16)


def d_upb(z, s):
    ones = jnp.ones((8, z.dpre.shape[1]), BF16)
    for i in range(FH // 512):
        row = 9 + 8 * s + i
        z.sm[row : row + 1, :] = dot(ones, z.dpre[s, :, i * 512 : (i + 1) * 512])[0:1]


def d_out(z, s):
    z.GO[s][...] = dot(z.mixT[s], z.br[...]).astype(BF16)


def grad_mixed(z, s):
    for r in range(z.nb):
        sl = slice(r * BLK, (r + 1) * BLK)
        z.gmT[s, :, sl] = dot(z.ow[s], z.br[sl, :], NT).astype(BF16)


def attn_bwd(z, s, hook):
    def body(h, c):
        hr = pl.ds(pl.multiple_of(h * HD, HD), HD)
        hi = s * NH + h
        vh = z.vT[s, h, 0:HD, :].T
        gs = (z.gmT[s, hr, :].astype(F32) * z.rl[hi]).astype(BF16)
        delta = jnp.sum(gs.astype(F32) * z.mixT[s, hr, :].astype(F32), 0, keepdims=True)
        dprob = lambda b: dot(vh[: BLK * (b + 1)], gs[:, b * BLK : (b + 1) * BLK])
        head_grad = lambda b: dot(z.dh[:, b * BLK : (b + 1) * BLK], z.n1T[:, b * BLK : (b + 1) * BLK], NT)
        last = z.nb - 1
        ahead, g = dprob(last), None
        for b in range(last, -1, -1):
            dp = ahead
            if b:
                ahead = dprob(b - 1)
            nk = BLK * (b + 1)
            off = BLK * (b * (b + 1) // 2)
            sl = slice(b * BLK, nk)
            gq = gs[:, sl]
            e = z.E[hi, off : off + nk, :]
            dv = dot(gq, e, NT)
            if b < last:
                g = head_grad(b + 1) if g is None else g + head_grad(b + 1)
            ds = (e.astype(F32) * (dp - delta[:, sl])).astype(BF16)
            z.dh[0:HD, sl] = (dot(z.kT[s, hr, 0:nk], ds) * 0.125).astype(BF16)
            dk = dot(z.qT[s, hr, sl], ds, NT)
            if b < last:
                dv = dv + z.dva[:, 0:nk]
                dk = dk + z.dka[:, 0:nk]
            if b:
                z.dva[:, 0 : nk - BLK] = dv[:, 0 : nk - BLK]
                z.dka[:, 0 : nk - BLK] = dk[:, 0 : nk - BLK]
            z.dh[HD : 2 * HD, sl] = (dk[:, nk - BLK : nk] * LN2).astype(BF16)
            z.dh[2 * HD : 3 * HD, sl] = dv[:, nk - BLK : nk].astype(BF16)
        for j in range(3):
            z.dT[s, pl.ds(pl.multiple_of(j * HALF + h * HD, HD), HD), :] = z.dh[j * HD : (j + 1) * HD, :]
        g = ((g + head_grad(0)) if g is not None else head_grad(0)).astype(BF16)
        for q in range(4):
            z.GH[s][h, q * 192 : (q + 1) * 192, :] = g[:, q * 128 : (q + 1) * 128]
        hook(h)
        return c

    lax.fori_loop(0, NH, body, 0)


def d_headb(z, s):
    ones = jnp.ones((8, z.dT.shape[2]), BF16)
    for i, j in enumerate((0, 2)):
        row = 8 + 8 * s
        z.sm[row : row + 1, i * HALF : (i + 1) * HALF] = dot(ones, z.dT[s, j * HALF : (j + 1) * HALF, :], NT)[0:1]


def grad_in(z, hook):
    zero = jnp.zeros((1, D), F32)
    sc, sh = zero, zero
    for r in range(z.nb):
        sl = slice(r * BLK, (r + 1) * BLK)
        g = 0.0
        for s in (0, 1):
            for j in range(3):
                g = g + dot(z.hw[s, j], z.dT[s, j * HALF : (j + 1) * HALF, sl])
        g = g.T
        xh, rs = normed(z.x[sl, :].astype(F32))
        z.ig[sl, :] = (z.res[sl, :] + ln_back(g, xh, rs, z.ns[0:1, :])).astype(BF16)
        sc = sc + jnp.sum(g * xh, 0, keepdims=True)
        sh = sh + jnp.sum(g, 0, keepdims=True)
        if r == z.nb - 1:
            z.sm[0:1, :] = sc
            z.sm[2:3, :] = sh
        hook(f"gin{r}")


class Comm:
    def __init__(self, ndp, groups, send, recv, local):
        self.send, self.recv, self.local = send, recv, local
        self.count, self.local_count, self.pending = 0, 0, []
        me = lax.axis_index("dp")
        self.levels = [1 << i for i in range(ndp.bit_length() - 1)]
        self.bit = {b: (me // b) % 2 for b in self.levels}
        self.me = me
        self.greet = ["t"] + [([b], 1) for b in self.levels] + [(g, d) for g in groups for d in range(1, 1 << len(g)) if d & (d - 1)]
        self.peer = 1 - lax.axis_index("tensor")

    def where(self, axis):
        if axis == "t":
            return {"tensor": self.peer}
        bits, delta = axis
        return {"dp": self.me + sum(b - 2 * b * self.bit[b] for i, b in enumerate(bits) if delta >> i & 1)}

    def barrier_signal(self):
        sem = pltpu.get_barrier_semaphore()
        for axis in self.greet:
            pl.semaphore_signal(sem, inc=1, device_id=self.where(axis), device_id_type=MESH)

    def barrier_wait(self):
        pl.semaphore_wait(pltpu.get_barrier_semaphore(), len(self.greet))

    def copy(self, src, dst, axis, keep=True):
        i = self.count
        self.count += 1

        def make():
            return pltpu.make_async_remote_copy(
                src_ref=src(), dst_ref=dst(), send_sem=self.send.at[i], recv_sem=self.recv.at[i],
                device_id=self.where(axis), device_id_type=MESH)

        if keep:
            self.pending.append(make)
        return make

    def here(self, src, dst):
        i = self.local_count
        self.local_count += 1
        return lambda: pltpu.make_async_copy(src(), dst(), self.local.at[i])

    def drain(self, n=None):
        for make in self.pending[:n]:
            make().wait_send()
        self.pending = self.pending[n:] if n else []


def add_rows(dst, srcs, at, n, cols):
    ch = next(c for c in (384, 256, 192, 128, 96, 64, 48, 32, 16, 8, 4) if n % c == 0 and c * cols <= 49152)

    def body(i, c):
        o = pl.ds(pl.multiple_of(at + i * ch, ch), ch)
        f = pl.ds(pl.multiple_of(i * ch, ch), ch)
        if len(srcs) == 1:
            dst[o, :] = dst[o, :] + srcs[0][f, :]
        else:
            dst[o, :] = pairwise([dst[o, :].astype(F32)] + [s[f, :].astype(F32) for s in srcs]).astype(dst.dtype)
        return c

    lax.fori_loop(0, n // ch, body, 0)


def pairwise(v):
    while len(v) > 1:
        v = [v[i] + v[i + 1] for i in range(0, len(v), 2)]
    return v[0]


def sizes_of(rows, stages):
    n = [rows]
    for bits in stages:
        n.append(n[-1] >> len(bits))
    return n


def job_scratch(rows, cols, stages, pre, extra):
    V = pltpu.VMEM
    n = sizes_of(rows, stages)
    bufs = lambda ss: [V((n[k + 1], cols), BF16) for k in range(ss) for _ in range((1 << len(stages[k])) - 1)]
    return bufs(len(stages)) + bufs(pre) + [V((n[pre], cols), BF16)] + [V((n[-1], cols), BF16) for _ in range(extra)] + [V((rows, cols), BF16)]


class Job:
    def __init__(self, c, own, peer, refs, rows, cols, stages, pre, out):
        S = len(stages)
        done = sum(len(b) for b in stages)
        extra = c.levels[done:]
        n = sizes_of(rows, stages)
        refs = list(refs)
        take = lambda m: [refs.pop(0) for _ in range(m)]
        r_own = [take((1 << len(b)) - 1) for b in stages]
        r_peer = [take((1 << len(b)) - 1) for b in stages[:pre]]
        r_t, r_x, full = take(1)[0], take(len(extra)), refs.pop(0)

        def code(bits, delta):
            return sum((c.bit[b] if not delta >> i & 1 else 1 - c.bit[b]) * (1 << i) for i, b in enumerate(bits))

        lo = [0]
        for k, b in enumerate(stages):
            lo.append(lo[k] + code(b, 0) * n[k + 1])
        at = lambda k: pl.ds(pl.multiple_of(lo[k], n[k]) if k else 0, n[k])
        theirs = lambda k, d: pl.ds(pl.multiple_of(lo[k] + code(stages[k], d) * n[k + 1], n[k + 1]), n[k + 1])

        def scatter(g, bufs, k):
            return [c.copy(lambda d=d: g().at[theirs(k, d)], lambda d=d: bufs[d - 1], (stages[k], d)) for d in range(1, len(bufs) + 1)]

        s_own = [scatter(own, r_own[k], k) for k in range(S)]
        s_peer = [scatter(peer, r_peer[k], k) for k in range(pre)]
        s_t = c.copy(lambda: peer().at[at(pre)], lambda: r_t, "t")
        s_x = [c.copy(lambda: own().at[at(S)], lambda i=i: r_x[i], ([b], 1), False) for i, b in enumerate(extra)]
        s_g = [[c.copy(lambda k=k: full.at[at(k + 1)], lambda k=k: full.at[at(k + 1)], (stages[k], d)) for d in range(1, 1 << len(stages[k]))]
               for k in range(S)]
        s_out = c.here(lambda: full, lambda: out())
        self.wait_out = lambda: s_out().wait()
        start = lambda ss: [s().start() for s in ss]
        arrived = lambda ss: [s().wait_recv() for s in ss]

        def end(s, g, buf, k):
            arrived(s[k])
            add_rows(g(), buf[k], lo[k + 1], n[k + 1], cols)

        def peer_step(i):
            if i:
                end(s_peer, peer, r_peer, i - 1)
            start(s_peer[i] if i < pre else [s_t])

        def own_step(i):
            if i == 0:
                start(s_own[0])
            elif i <= S:
                end(s_own, own, r_own, i - 1)
                if i == pre:
                    assert not self.peer_steps
                    s_t().wait_recv()
                    add_rows(own(), [r_t], lo[pre], n[pre], cols)
                if i < S:
                    start(s_own[i])
                    return
                for j in range(len(extra)):
                    s_x[j]().start()
                    s_x[j]().wait()
                    add_rows(own(), [r_x[j]], lo[S], n[S], cols)
                full[at(S), :] = own()[at(S), :]
                start(s_g[S - 1])
            else:
                k = 2 * S - i
                arrived(s_g[k])
                if k:
                    start(s_g[k - 1])
                else:
                    s_out().start()

        self.peer_steps = [lambda i=i: peer_step(i) for i in range(pre + 1)]
        self.own_steps = [lambda i=i: own_step(i) for i in range(2 * S + 1)]

    def own(self):
        self.own_steps.pop(0)()

    def peer(self):
        self.peer_steps.pop(0)()


SMALL_STAGES = [[1], [2], [4, 8]]


class Small:
    def __init__(self, c, sm, bufs):
        bufs = list(bufs)
        r_t = bufs.pop(0)
        st = SMALL_STAGES + [[b] for b in c.levels[4:]]
        s_t = [c.copy(lambda: sm.at[0:8], lambda: r_t.at[0:8], "t", False), c.copy(lambda: sm.at[16:24], lambda: r_t.at[8:16], "t", False)]
        rs, ss = [[r_t]], [s_t]
        for bits in st:
            r = [bufs.pop(0) for _ in range((1 << len(bits)) - 1)]
            rs.append(r)
            ss.append([c.copy(lambda: sm.at[0:16], lambda b=b: b, (bits, d + 1), False) for d, b in enumerate(r)])

        def step(i):
            if i:
                for s in ss[i - 1]:
                    s().wait()
                sm[0:16, :] = pairwise([sm[0:16, :]] + [r[...] for r in rs[i - 1]])
            if i < len(ss):
                for s in ss[i]:
                    s().start()

        self.steps = [lambda i=i: step(i) for i in range(len(ss) + 1)]

    def own(self):
        self.steps.pop(0)()


INS = ["x_h", "cot_h", "hw_h", "ow_h", "uw_h", "dw_h", "ns", "nsh", "qb_o", "vb_o", "ob", "ub_o", "db"]
OUTS = ["lo_h", "ig_h", "FH_h", "FO_h", "FU_h", "FD_h", "smo"]
Y4, Z14, G8 = [[1], [2], [4, 8]], [[1], [4], [2], [8]], [[1], [2, 4, 8]]
JOBS = [("D0", 512, 512, [[1], [2], [4, 8]], 1),
        ("U0", 512, 512, [[1], [2], [4, 8]], 2),
        ("D1", 512, 512, [[1], [2], [4, 8]], 1),
        ("U1", 512, 512, [[1], [2], [4, 8]], 2),
        ("O", 256, 512, [[1], [2], [4, 8]], 2),
        ("H0", 768, 128, [[1], [2], [4, 8]], 2),
        ("H1", 768, 128, [[1], [2], [4, 8]], 1),
        ("H2", 768, 128, [[1], [2], [4, 8]], 2),
        ("H3", 768, 128, [[1], [2], [4, 8]], 2)]

HOOKS = {
    "f0_0": ["WhwA"],
    "f0_1": ["WhwB", "Wow"],
    "qkv1a": ["Wu0"],
    "f1_0": ["Wd0", "WhwB", "Wow"],
    "qkv1b": ["Wu1", "Wu0"],
    "f1_1": ["Wd0", "Wd1"],
    "ffn01_0": ["Wu1"],
    "dD01": ["D0p"],
    "dU01": ["Wd1", "U0p"],
    "ffn00_0": ["D0p"],
    "ffn00_1": ["U0p"],
    "dD00": ["D0o"],
    "dU00": ["U0o"],
    "ffn11_1": ["U0o"],
    "dD11": ["D1p", "U0p"],
    "dU11": ["U1p"],
    "ffn10_0": ["D0o", "D1p", "U1p"],
    "dD10": ["D1o"],
    "dU10": ["U0o", "U1o"],
    "dO0": ["Op", "Oo"],
    "gm": ["U1o", "D0o"],
    "b1_0": ["Op", "Oo"],
    "b1_1": ["U0o", "U1p", "D1o", "H1p"],
    "b1_2": ["H2p", "D0o", "H1p", "H0p", "Op"],
    "b1_3": ["H2p", "H3p", "U1o"],
    "b0_0": ["U0o", "H3p", "D1o", "H0p", "H0o"],
    "b0_1": ["H2p", "D0o", "H1o", "Oo", "H0o"],
    "b0_2": ["U0o", "H1o", "U1o", "H2o"],
    "b0_3": ["U0o", "H3p", "D1o", "H0p", "H2o", "H3o"],
    "gin0": ["Oo"],
    "gin1": ["H3o"],
    "gin2": ["D0o"],
    "gin3": ["So", "U1o", "H0o"],
    "fo0": ["D0o", "H1o"],
    "fo2": ["H2o"],
    "fo3": ["So", "H3o", "D1o"],
    "tail": ["So", "Oo", "H0o", "U1o", "H1o", "U1o", "H2o", "H3o", "D1o", "H0o", "D1o", "H1o", "Oo", "So", "H2o", "Oo", "H0o", "H3o", "H1o", "H0o", "H2o", "H1o", "H3o", "H2o", "So", "H3o"],
}
BEFORE = {
    "qkv1a": ["WhwA"],
}

GROUPS = [g for g in ([4, 8], [2, 4, 8]) if any(g in st for _, _, _, st, _ in JOBS) or g in SMALL_STAGES]


def scratch(T, ndp):
    nb = T // BLK
    V = pltpu.VMEM
    lv = ndp.bit_length() - 1
    s = dict(
        x=V((T, D), BF16), cot=V((T, D), BF16), hw=V((2, 3, D, HALF), BF16), ow=V((2, HALF, D), BF16),
        uw=V((2, D, FH), BF16), dw=V((2, FH, D), BF16),
        qb_p=V((1, HALF), F32), vb_p=V((1, HALF), F32), ub_p=V((1, FH), F32),
        n1T=V((D, T), BF16), qT=V((2, HALF, T), BF16), kT=V((2, HALF, T), BF16), vT=V((2, NH, 80, T), BF16),
        E=V((2 * NH, BLK * nb * (nb + 1) // 2, BLK), BF16), rl=V((2 * NH, 1, T), F32), mixT=V((2, HALF, T), BF16),
        res=V((T, D), F32), n2=V((T, D), BF16), act=V((2, T, FH), BF16), dpre=V((2, T, FH), BF16),
        oacc=V((T, D), F32), g2=V((T, D), F32), br=V((T, D), BF16), gmT=V((2, HALF, T), BF16),
        dh=V((3 * HD, T), BF16), dva=V((HD, T), F32), dka=V((HD, T), F32), sm=V((24, D), F32),
        GD0o=V((FH // 2, D), BF16), GD0p=V((FH // 2, D), BF16), GD1o=V((FH // 2, D), BF16), GD1p=V((FH // 2, D), BF16),
        GU0o=V((D, FH // 2), BF16), GU0p=V((D, FH // 2), BF16), GU1o=V((D, FH // 2), BF16), GU1p=V((D, FH // 2), BF16),
        GOo=V((HALF, D), BF16), GOp=V((HALF, D), BF16), GHo=V((NH, 768, 128), BF16), GHp=V((NH, 768, 128), BF16),
        s0=V((16, D), F32))
    for i in range(5 + lv - 4):
        s[f"s{i + 1}"] = V((16, D), F32)
    for name, rows, cols, stages, pre in JOBS:
        for i, v in enumerate(job_scratch(rows, cols, stages, pre, lv - 4)):
            s[f"{name}_{i}"] = v
    s["send"] = pltpu.SemaphoreType.DMA((224 + 24 * (lv - 4),))
    s["recv"] = pltpu.SemaphoreType.DMA((224 + 24 * (lv - 4),))
    s["local"] = pltpu.SemaphoreType.DMA((32,))
    return s


def run(z, ndp):
    c = Comm(ndp, GROUPS, z.send, z.recv, z.local)
    lv = c.levels
    c.barrier_signal()
    slot0 = lambda r: r.at[0]
    loads = {n: c.here(lambda n=n: getattr(z, n + "_h"), lambda n=n, d=d: d(getattr(z, n)))
             for n, d in (("x", lambda r: r), ("hw", slot0), ("cot", lambda r: r), ("ow", slot0), ("uw", slot0), ("dw", slot0))}
    for n in ("x", "hw", "ow", "cot", "uw", "dw"):
        loads[n]().start()

    pieces = {"hwA": ("hw", D, 0, slice(0, 128)), "hwB": ("hw", D, 0, slice(128, 256)), "ow": ("ow", HALF, 0, slice(None)),
              "u0": ("uw", D, 0, slice(0, 512)), "d0": ("dw", 512, 0, slice(None)), "u1": ("uw", D, 0, slice(512, 1024)),
              "d1": ("dw", 512, 512, slice(None))}

    def view(name, flip, lead):
        n, m, base, cols = pieces[name]
        q = (c.bit[1] if not flip & 1 else 1 - c.bit[1]) + 2 * (c.bit[2] if not flip & 2 else 1 - c.bit[2])
        rows = pl.ds(pl.multiple_of(base + q * (m // 4), m // 4), m // 4)
        r = getattr(z, n).at[1] if lead else getattr(z, n + "_h")
        return r.at[:, rows, cols] if n == "hw" else r.at[rows, cols]

    W = {}
    for name in pieces:
        put = lambda flip, name=name: view(name, flip, True)
        W[name] = dict(
            x=c.copy(lambda name=name: view(name, 0, False), lambda put=put: put(0), "t"),
            s=c.copy(lambda put=put: put(0), lambda put=put: put(0), ([1], 1)),
            y=c.copy(lambda put=put: put(0), lambda put=put: put(0), ([2], 1)),
            r=c.copy(lambda put=put: put(2), lambda put=put: put(2), ([1], 1)))
    wb = [c.copy(lambda n=n: getattr(z, n + "_o"), lambda n=n: getattr(z, n + "_p"), "t") for n in ("qb", "vb", "ub")]

    def relay1(n):
        W[n]["x"]().wait_recv()
        W[n]["y"]().start()
        W[n]["s"]().start()

    def relay2(n):
        W[n]["y"]().wait_recv()
        W[n]["r"]().start()

    def arrive(n):
        W[n]["s"]().wait_recv()
        W[n]["r"]().wait_recv()

    c.barrier_wait()
    W["hwA"]["x"]().start()
    for b in wb:
        b().start()
    for n in list(pieces)[1:]:
        W[n]["x"]().start()

    z.qb, z.vb, z.ub = (z.qb_o, z.qb_p), (z.vb_o, z.vb_p), (z.ub_o, z.ub_p)
    z.GD = ((z.GD0o, z.GD0p), (z.GD1o, z.GD1p))
    z.GU = ((z.GU0o, z.GU0p), (z.GU1o, z.GU1p))
    z.GO, z.GH = (z.GOo, z.GOp), (z.GHo, z.GHp)
    z.dT, z.lo, z.ig = z.dpre, z.br, z.n2
    ends = dict(D0=lambda: z.FD_h.at[0 : FH // 2], D1=lambda: z.FD_h.at[FH // 2 : FH], U0=lambda: z.FU_h.at[:, 0 : FH // 2],
                U1=lambda: z.FU_h.at[:, FH // 2 : FH], O=lambda: z.FO_h)
    srcs = dict(D0=(lambda: z.GD0o, lambda: z.GD0p), D1=(lambda: z.GD1o, lambda: z.GD1p), U0=(lambda: z.GU0o, lambda: z.GU0p),
                U1=(lambda: z.GU1o, lambda: z.GU1p), O=(lambda: z.GOo, lambda: z.GOp))
    for i in range(NH):
        ends[f"H{i}"] = lambda i=i: z.FH_h.at[i]
        srcs[f"H{i}"] = (lambda i=i: z.GHo.at[i], lambda i=i: z.GHp.at[i])
    jobs = {}
    for name, rows, cols, stages, pre in JOBS:
        refs = [getattr(z, f"{name}_{i}") for i in range(len(job_scratch(rows, cols, stages, pre, len(lv) - 4)))]
        jobs[name] = Job(c, *srcs[name], refs, rows, cols, stages, pre, ends[name])
    jobs["S"] = small = Small(c, z.sm, [getattr(z, f"s{i}") for i in range(6 + len(lv) - 4)])
    s_lo, s_ig = c.here(lambda: z.lo, lambda: z.lo_h), c.here(lambda: z.ig, lambda: z.ig_h)

    relays = {n: [relay1, relay2] for n in W}

    def go(words):
        for word in words:
            if word[1:] in relays:
                relays[word[1:]].pop(0)(word[1:])
            else:
                (jobs[word[:-1]].own if word[-1] == "o" else jobs[word[:-1]].peer)()

    def at(name, n):
        table = {k: HOOKS.get(f"{name}_{k}", ()) for k in (range(n) if isinstance(n, int) else n)}

        def hook(h):
            for k, what in table.items():
                if what:
                    @pl.when(h == k)
                    def _():
                        go(what)
        return hook

    def before(name):
        go(BEFORE.get(name, ()))

    def after(name):
        go(HOOKS.get(name, ()))

    z.sm[...] = jnp.zeros_like(z.sm)
    loads["x"]().wait()
    ln1(z)
    loads["hw"]().wait()
    qkv(z, 0, 0, NH)
    after("qkv0")
    attn_fwd(z, 0, 0, NH, at("f0", NH // 2))
    before("qkv1a")
    for b in wb:
        b().wait_recv()
    arrive("hwA")
    qkv(z, 1, 0, 2)
    after("qkv1a")
    attn_fwd(z, 1, 0, 2, at("f1", range(0, 1)))
    before("qkv1b")
    arrive("hwB")
    qkv(z, 1, 2, 4)
    after("qkv1b")
    attn_fwd(z, 1, 2, 4, at("f1", range(1, 2)))
    before("out")
    arrive("ow")
    loads["ow"]().wait()
    out_proj(z)
    for n in ("cot", "uw", "dw"):
        loads[n]().wait()
    after("out")
    for part in (0, 1):
        for s in (1, 0):
            name = f"ffn{part}{s}"
            before(name + "_0")
            if s:
                arrive(f"u{part}")
                arrive(f"d{part}")
            ffn(z, part, s, at(name, z.nb // 2))
            d_down(z, part, s)
            after(f"dD{part}{s}")
            d_up(z, part, s)
            if part:
                d_upb(z, s)
            after(f"dU{part}{s}")
    for s in (1, 0):
        d_out(z, s)
        after(f"dO{s}")
    grad_mixed(z, 1)
    grad_mixed(z, 0)
    after("gm")
    attn_bwd(z, 1, at("b1", NH))
    attn_bwd(z, 0, at("b0", NH))
    d_headb(z, 0)
    d_headb(z, 1)
    after("hb")
    c.drain(31)
    grad_in(z, after)
    s_ig().start()
    for r in range(z.nb):
        ffn_out(z, (r,))
        after(f"fo{r}")
    s_lo().start()
    after("tail")
    while small.steps:
        small.own()
    assert not any(v for v in relays.values()) and not any(jobs[n].own_steps for n in jobs if n != "S")
    z.smo[...] = z.sm[0:16, :]
    s_ig().wait()
    s_lo().wait()
    for n in jobs:
        if n != "S":
            jobs[n].wait_out()
    c.drain()


def main_call(args, T, ndp):
    scr = scratch(T, ndp)
    names = INS + OUTS + list(scr)

    def kernel(*refs):
        z = Refs()
        for n, r in zip(names, refs):
            setattr(z, n, r)
        z.nb = T // BLK
        run(z, ndp)

    S = jax.ShapeDtypeStruct
    outs = [S((T, D), BF16), S((T, D), BF16), S((NH, 768, 128), BF16), S((HALF, D), BF16), S((D, FH), BF16), S((FH, D), BF16),
            S((16, D), F32)]
    vm, hbm = pl.BlockSpec(memory_space=pltpu.VMEM), pl.BlockSpec(memory_space=pl.ANY)
    return pl.pallas_call(
        kernel, out_shape=outs, in_specs=[hbm] * 6 + [vm] * 7, out_specs=[hbm] * 6 + [vm], scratch_shapes=list(scr.values()),
        compiler_params=pltpu.CompilerParams(vmem_limit_bytes=VMEM_BYTES, collective_id=0, has_side_effects=True),
        name="layer")(*args)


def widen(FH_, FO_, FU_, FD_, sm, lo, ig):
    def kernel(h, o, u, d, m, l, g, ho, oo, uo, do, lo_, go, sc, sh, qb, vb, ob, ub, db, hv, ov, uv, dv, lv, gv, hf, of, uf, df, si, so):
        ins, outs = [], []

        def load(src, dst):
            c = pltpu.make_async_copy(src, dst, si.at[len(ins)])
            ins.append(c)
            c.start()
            return c

        def store(src, dst):
            c = pltpu.make_async_copy(src, dst, so.at[len(outs)])
            outs.append(c)
            c.start()

        top, bottom = slice(0, 512), slice(512, 1024)
        left, right = slice(0, 256), slice(256, 512)
        i_g, i_l = load(g, gv), load(l, lv)
        i_d0, i_h = load(d.at[top], dv.at[top]), load(h, hv)
        i_d1 = load(d.at[bottom], dv.at[bottom])
        i_u0, i_u1 = load(u.at[left], uv.at[left]), load(u.at[right], uv.at[right])
        i_o = load(o, ov)
        sc[...] = m[0:2, :]
        sh[...] = m[2:4, :]
        qb[...] = m[8:9, 0:HALF]
        vb[...] = m[8:9, HALF:D]
        ob[...] = m[4:5, :]
        ub[:, 0:D] = m[9:10, :]
        ub[:, D:FH] = m[10:11, :]
        db[...] = m[5:6, :]
        i_g.wait()
        store(gv, go)
        i_l.wait()
        store(lv, lo_)

        def piece(c, v, f, out, rows):
            c.wait()
            f[rows, :] = v[rows, :].astype(F32)
            store(f.at[rows], out.at[rows])

        piece(i_d0, dv, df, do, top)
        i_h.wait()
        for j in range(3):
            for q in range(4):
                for p in range(2):
                    rows = [hv[2 * p + i, q * 192 + j * HD : q * 192 + (j + 1) * HD, :] for i in range(2)]
                    hf[j, q * 128 : (q + 1) * 128, p * 128 : (p + 1) * 128] = jnp.concatenate(rows, 0).astype(F32).T
            store(hf.at[j], ho.at[j])
        piece(i_d1, dv, df, do, bottom)
        piece(i_u0, uv, uf, uo, left)
        piece(i_u1, uv, uf, uo, right)
        piece(i_o, ov, of, oo, left)
        for c in outs:
            c.wait()

    S, V = jax.ShapeDtypeStruct, pltpu.VMEM
    vm, hbm = pl.BlockSpec(memory_space=pltpu.VMEM), pl.BlockSpec(memory_space=pl.ANY)
    big = [(3, D, HALF), (HALF, D), (D, FH), (FH, D)]
    small = [(2, D), (2, D), (1, HALF), (1, HALF), (1, D), (1, FH), (1, D)]
    rows = S(lo.shape, BF16)
    out_shape = [S(t, F32) for t in big] + [rows, rows] + [S(t, F32) for t in small]
    bufs = [V((NH, 768, 128), BF16)] + [V(t, BF16) for t in big[1:]] + [V(lo.shape, BF16)] * 2 + [V(t, F32) for t in big]
    return pl.pallas_call(
        kernel, out_shape=out_shape, in_specs=[hbm] * 4 + [vm] + [hbm] * 2, out_specs=[hbm] * 6 + [vm] * 7,
        scratch_shapes=bufs + [pltpu.SemaphoreType.DMA((8,)), pltpu.SemaphoreType.DMA((10,))],
        compiler_params=pltpu.CompilerParams(vmem_limit_bytes=VMEM_BYTES), name="widen")(FH_, FO_, FU_, FD_, sm, lo, ig)


def solution(mesh):
    ndp = mesh.shape["dp"]

    def local(inputs, norm_scale, norm_shift, head_weight, query_bias, value_bias, out_weight, out_bias, up_weight, up_bias,
              down_weight, down_bias, cotangent):
        row = lambda b: b.reshape(1, b.shape[0])
        args = (inputs, cotangent, head_weight, out_weight, up_weight, down_weight, norm_scale, norm_shift, row(query_bias),
                row(value_bias), row(out_bias), row(up_bias), row(down_bias))
        lo, ig, gh, go, gu, gd, sm = main_call(args, inputs.shape[0], ndp)
        gh, go, gu, gd, lo, ig, sc, sh, qb, vb, ob, ub, db = widen(gh, go, gu, gd, sm, lo, ig)
        flat = lambda v: v.reshape(v.shape[1])
        return (lo, ig, sc, sh, gh, flat(qb), flat(vb), go, flat(ob), gu, flat(ub), gd, flat(db))

    rows, t0, t1 = P(("dp", "tensor"), None), P("tensor"), P(None, "tensor")
    tc = P("tensor", None)
    in_specs = (rows, P(), P(), P(None, None, "tensor"), t0, t0, tc, P(), t1, t0, tc, P(), rows)
    out_specs = (rows, rows, P(), P(), P(None, None, "tensor"), t0, t0, tc, P(), t1, t0, tc, P())
    return jax.shard_map(local, mesh=mesh, in_specs=in_specs, out_specs=out_specs, check_vma=False)
```

```python
import jax
import jax.numpy as jnp
from jax import lax
from jax.experimental import pallas as pl
from jax.experimental.pallas import tpu as pltpu
from jax.sharding import PartitionSpec as P

F32, BF16 = jnp.float32, jnp.bfloat16
NN, NT, TN = ((1,), (0,)), ((1,), (1,)), ((0,), (0,))
EPS = 1e-5
LOG2E = 1.4426950408889634
LN2 = 0.6931471805599453
C0, C1 = 0.7978845608, 0.044715
HD, BLK, D, HALF, FH, NH = 64, 256, 512, 256, 1024, 4
MESH = pl.DeviceIdType.MESH
VMEM_BYTES = 67043328


def dot(a, b, dims=NN):
    return lax.dot_general(a, b, (dims, ((), ())), preferred_element_type=F32)


def normed(v):
    c = jnp.mean(v, -1, keepdims=True)
    d = v - c
    r = lax.rsqrt(jnp.mean(d * d, -1, keepdims=True) + EPS)
    return d * r, r


def ln_back(g, xhat, r, gain):
    gx = g * gain
    return r * (gx - jnp.mean(gx, -1, keepdims=True) - xhat * jnp.mean(gx * xhat, -1, keepdims=True))


def rows_of(r):
    return pl.ds(pl.multiple_of(r * BLK, BLK), BLK)


def column(row):
    return jnp.broadcast_to(row, (8, row.shape[-1])).T[:, 0:1]


class Refs:
    pass


def ln1(z):
    def body(r, c):
        xh, _ = normed(z.x[rows_of(r), :].astype(F32))
        n = (xh * z.ns[0:1, :] + z.nsh[0:1, :]).astype(BF16)
        z.n1T[:, rows_of(r)] = n.T
        return c

    lax.fori_loop(0, z.nb, body, 0)


def qkv(z, s, h0, h1):
    cs = slice(h0 * HD, h1 * HD)
    qb, vb = column(z.qb[s][:, cs]), column(z.vb[s][:, cs])
    for b in range(z.nb):
        sl = slice(b * BLK, (b + 1) * BLK)
        nt = z.n1T[:, sl]
        q = dot(z.hw[s, 0, :, cs], nt, TN) + qb
        z.qT[s, cs, sl] = (q * (LOG2E / 8.0)).astype(BF16)
        z.kT[s, cs, sl] = dot(z.hw[s, 1, :, cs], nt, TN).astype(BF16)
        v = (dot(z.hw[s, 2, :, cs], nt, TN) + vb).astype(BF16)
        for h in range(h0, h1):
            z.vT[s, h, 0:HD, sl] = v[(h - h0) * HD : (h - h0 + 1) * HD]
            z.vT[s, h, HD : HD + 16, sl] = jnp.ones((16, BLK), BF16)


def attn_fwd(z, s, h0, h1, hook):
    def body(p, c):
        hrs = [pl.ds(pl.multiple_of(p * 2 * HD + j * HD, HD), HD) for j in (0, 1)]
        khs = [z.kT[s, hr, :].T for hr in hrs]

        def scores(j, b):
            return dot(khs[j][: BLK * (b + 1)], z.qT[s, hrs[j], b * BLK : (b + 1) * BLK])

        items = [(j, b) for j in (0, 1) for b in range(z.nb)]
        ahead = scores(*items[0])
        for i, (j, b) in enumerate(items):
            sc = ahead
            if i + 1 < len(items):
                ahead = scores(*items[i + 1])
            h, hr = 2 * p + j, hrs[j]
            nk = BLK * (b + 1)
            off = BLK * (b * (b + 1) // 2)
            sl = slice(b * BLK, nk)
            m = jnp.max(sc, 0, keepdims=True)
            e = jnp.exp2(sc - m).astype(BF16)
            z.E[s * NH + h, off : off + nk, :] = e
            o = dot(z.vT[s, h, :, 0:nk], e)
            rl = 1.0 / o[HD : HD + 1]
            z.rl[s * NH + h, 0:1, sl] = rl
            z.mixT[s, hr, sl] = (o[0:HD] * rl).astype(BF16)
        hook(p)
        return c

    lax.fori_loop(h0 // 2, h1 // 2, body, 0)


def out_proj(z):
    for r in range(z.nb):
        sl = slice(r * BLK, (r + 1) * BLK)
        t = dot(z.mixT[0, :, sl], z.ow[0], TN) + dot(z.mixT[1, :, sl], z.ow[1], TN)
        res = z.x[sl, :].astype(F32) + (t + z.ob[...])
        z.res[sl, :] = res
        z.oacc[sl, :] = res + z.db[...]
        xh, _ = normed(res)
        z.n2[sl, :] = (xh * z.ns[1:2, :] + z.nsh[1:2, :]).astype(BF16)


def ffn(z, part, s, hook):
    first, last = (part, s) == (0, 1), (part, s) == (1, 0)
    fs = slice(part * 512, part * 512 + 512)

    def products(rr):
        ct = z.cot[rr, :]
        return ct, dot(z.n2[rr, :], z.uw[s, :, fs]) + z.ub[s][:, fs], dot(ct, z.dw[s, fs, :], NT)

    def body(p, c):
        blocks = [rows_of(2 * p), rows_of(2 * p + 1)]
        ahead = products(blocks[0])
        for i, rr in enumerate(blocks):
            ct, u, da = ahead
            if i == 0:
                ahead = products(blocks[1])
            u2 = u * u
            t = jnp.tanh(u * (C0 + (C0 * C1) * u2))
            hp = 0.5 + 0.5 * t
            z.act[s, rr, fs] = (u * hp).astype(BF16)
            gp = hp + (u * (0.5 - 0.5 * t * t)) * (C0 + (3 * C0 * C1) * u2)
            dp = (da * gp).astype(BF16)
            z.dpre[s, rr, fs] = dp
            g = dot(dp, z.uw[s, :, fs], NT)
            g2 = g if first else z.g2[rr, :] + g
            if not last:
                z.g2[rr, :] = g2
            else:
                xh, rs = normed(z.res[rr, :])
                gres = ct.astype(F32) + ln_back(g2, xh, rs, z.ns[1:2, :])
                br = gres.astype(BF16)
                z.res[rr, :] = gres
                z.br[rr, :] = br
                c = (
                    c[0] + jnp.sum(g2 * xh, 0, keepdims=True),
                    c[1] + jnp.sum(g2, 0, keepdims=True),
                    c[2] + jnp.sum(br.astype(F32), 0, keepdims=True),
                    c[3] + jnp.sum(ct.astype(F32), 0, keepdims=True),
                )
        hook(p)
        return c

    zero = jnp.zeros((1, D), F32)
    c = lax.fori_loop(0, z.nb // 2, body, (zero,) * 4 if last else 0)
    if last:
        z.sm[1:2, :] = c[0]
        z.sm[3:4, :] = c[1]
        z.sm[4:5, :] = c[2]
        z.sm[5:6, :] = c[3]


def ffn_out(z, blocks):
    for r in blocks:
        rr = slice(r * BLK, (r + 1) * BLK)
        o = dot(z.act[0, rr, :], z.dw[0]) + dot(z.act[1, rr, :], z.dw[1])
        z.lo[rr, :] = (z.oacc[rr, :] + o).astype(BF16)


def d_down(z, part, s):
    for f in range(0, 512, 256):
        a = part * 512 + f
        z.GD[part][s][f : f + 256, :] = dot(z.act[s, :, a : a + 256], z.cot[...], TN).astype(BF16)


def d_up(z, part, s):
    z.GU[part][s][...] = dot(z.n2[...], z.dpre[s, :, part * 512 : part * 512 + 512], TN).astype(BF16)


def d_upb(z, s):
    ones = jnp.ones((8, z.dpre.shape[1]), BF16)
    for i in range(FH // 512):
        row = 9 + 8 * s + i
        z.sm[row : row + 1, :] = dot(ones, z.dpre[s, :, i * 512 : (i + 1) * 512])[0:1]


def d_out(z, s):
    z.GO[s][...] = dot(z.mixT[s], z.br[...]).astype(BF16)


def grad_mixed(z, s):
    for r in range(z.nb):
        sl = slice(r * BLK, (r + 1) * BLK)
        z.gmT[s, :, sl] = dot(z.ow[s], z.br[sl, :], NT).astype(BF16)


def attn_bwd(z, s, hook):
    def body(h, c):
        hr = pl.ds(pl.multiple_of(h * HD, HD), HD)
        hi = s * NH + h
        vh = z.vT[s, h, 0:HD, :].T
        gs = (z.gmT[s, hr, :].astype(F32) * z.rl[hi]).astype(BF16)
        delta = jnp.sum(gs.astype(F32) * z.mixT[s, hr, :].astype(F32), 0, keepdims=True)
        dprob = lambda b: dot(vh[: BLK * (b + 1)], gs[:, b * BLK : (b + 1) * BLK])
        head_grad = lambda b: dot(z.dh[:, b * BLK : (b + 1) * BLK], z.n1T[:, b * BLK : (b + 1) * BLK], NT)
        last = z.nb - 1
        ahead, g = dprob(last), None
        for b in range(last, -1, -1):
            dp = ahead
            if b:
                ahead = dprob(b - 1)
            nk = BLK * (b + 1)
            off = BLK * (b * (b + 1) // 2)
            sl = slice(b * BLK, nk)
            gq = gs[:, sl]
            e = z.E[hi, off : off + nk, :]
            dv = dot(gq, e, NT)
            if b < last:
                g = head_grad(b + 1) if g is None else g + head_grad(b + 1)
            ds = (e.astype(F32) * (dp - delta[:, sl])).astype(BF16)
            z.dh[0:HD, sl] = (dot(z.kT[s, hr, 0:nk], ds) * 0.125).astype(BF16)
            dk = dot(z.qT[s, hr, sl], ds, NT)
            if b < last:
                dv = dv + z.dva[:, 0:nk]
                dk = dk + z.dka[:, 0:nk]
            if b:
                z.dva[:, 0 : nk - BLK] = dv[:, 0 : nk - BLK]
                z.dka[:, 0 : nk - BLK] = dk[:, 0 : nk - BLK]
            z.dh[HD : 2 * HD, sl] = (dk[:, nk - BLK : nk] * LN2).astype(BF16)
            z.dh[2 * HD : 3 * HD, sl] = dv[:, nk - BLK : nk].astype(BF16)
        for j in range(3):
            z.dT[s, pl.ds(pl.multiple_of(j * HALF + h * HD, HD), HD), :] = z.dh[j * HD : (j + 1) * HD, :]
        g = ((g + head_grad(0)) if g is not None else head_grad(0)).astype(BF16)
        for q in range(4):
            z.GH[s][h, q * 192 : (q + 1) * 192, :] = g[:, q * 128 : (q + 1) * 128]
        hook(h)
        return c

    lax.fori_loop(0, NH, body, 0)


def d_headb(z, s):
    ones = jnp.ones((8, z.dT.shape[2]), BF16)
    for i, j in enumerate((0, 2)):
        row = 8 + 8 * s
        z.sm[row : row + 1, i * HALF : (i + 1) * HALF] = dot(ones, z.dT[s, j * HALF : (j + 1) * HALF, :], NT)[0:1]


def grad_in(z, hook):
    zero = jnp.zeros((1, D), F32)
    sc, sh = zero, zero
    for r in range(z.nb):
        sl = slice(r * BLK, (r + 1) * BLK)
        g = 0.0
        for s in (0, 1):
            for j in range(3):
                g = g + dot(z.hw[s, j], z.dT[s, j * HALF : (j + 1) * HALF, sl])
        g = g.T
        xh, rs = normed(z.x[sl, :].astype(F32))
        z.ig[sl, :] = (z.res[sl, :] + ln_back(g, xh, rs, z.ns[0:1, :])).astype(BF16)
        sc = sc + jnp.sum(g * xh, 0, keepdims=True)
        sh = sh + jnp.sum(g, 0, keepdims=True)
        if r == z.nb - 1:
            z.sm[0:1, :] = sc
            z.sm[2:3, :] = sh
        hook(f"gin{r}")


class Comm:
    def __init__(self, ndp, groups, send, recv, local):
        self.send, self.recv, self.local = send, recv, local
        self.count, self.local_count, self.pending = 0, 0, []
        me = lax.axis_index("dp")
        self.levels = [1 << i for i in range(ndp.bit_length() - 1)]
        self.bit = {b: (me // b) % 2 for b in self.levels}
        self.me = me
        self.greet = ["t"] + [([b], 1) for b in self.levels] + [(g, d) for g in groups for d in range(1, 1 << len(g)) if d & (d - 1)]
        self.peer = 1 - lax.axis_index("tensor")

    def where(self, axis):
        if axis == "t":
            return {"tensor": self.peer}
        bits, delta = axis
        return {"dp": self.me + sum(b - 2 * b * self.bit[b] for i, b in enumerate(bits) if delta >> i & 1)}

    def barrier_signal(self):
        sem = pltpu.get_barrier_semaphore()
        for axis in self.greet:
            pl.semaphore_signal(sem, inc=1, device_id=self.where(axis), device_id_type=MESH)

    def barrier_wait(self):
        pl.semaphore_wait(pltpu.get_barrier_semaphore(), len(self.greet))

    def copy(self, src, dst, axis, keep=True):
        i = self.count
        self.count += 1

        def make():
            return pltpu.make_async_remote_copy(
                src_ref=src(), dst_ref=dst(), send_sem=self.send.at[i], recv_sem=self.recv.at[i],
                device_id=self.where(axis), device_id_type=MESH)

        if keep:
            self.pending.append(make)
        return make

    def here(self, src, dst):
        i = self.local_count
        self.local_count += 1
        return lambda: pltpu.make_async_copy(src(), dst(), self.local.at[i])

    def drain(self, n=None):
        for make in self.pending[:n]:
            make().wait_send()
        self.pending = self.pending[n:] if n else []


def add_rows(dst, srcs, at, n, cols):
    ch = next(c for c in (384, 256, 192, 128, 96, 64, 48, 32, 16, 8, 4) if n % c == 0 and c * cols <= 49152)

    def body(i, c):
        o = pl.ds(pl.multiple_of(at + i * ch, ch), ch)
        f = pl.ds(pl.multiple_of(i * ch, ch), ch)
        if len(srcs) == 1:
            dst[o, :] = dst[o, :] + srcs[0][f, :]
        else:
            dst[o, :] = pairwise([dst[o, :].astype(F32)] + [s[f, :].astype(F32) for s in srcs]).astype(dst.dtype)
        return c

    lax.fori_loop(0, n // ch, body, 0)


def pairwise(v):
    while len(v) > 1:
        v = [v[i] + v[i + 1] for i in range(0, len(v), 2)]
    return v[0]


def sizes_of(rows, stages):
    n = [rows]
    for bits in stages:
        n.append(n[-1] >> len(bits))
    return n


def job_scratch(rows, cols, stages, pre, extra):
    V = pltpu.VMEM
    n = sizes_of(rows, stages)
    bufs = lambda ss: [V((n[k + 1], cols), BF16) for k in range(ss) for _ in range((1 << len(stages[k])) - 1)]
    return bufs(len(stages)) + bufs(pre) + [V((n[pre], cols), BF16)] + [V((n[-1], cols), BF16) for _ in range(extra)] + [V((rows, cols), BF16)]


class Job:
    def __init__(self, c, own, peer, refs, rows, cols, stages, pre, out):
        S = len(stages)
        done = sum(len(b) for b in stages)
        extra = c.levels[done:]
        n = sizes_of(rows, stages)
        refs = list(refs)
        take = lambda m: [refs.pop(0) for _ in range(m)]
        r_own = [take((1 << len(b)) - 1) for b in stages]
        r_peer = [take((1 << len(b)) - 1) for b in stages[:pre]]
        r_t, r_x, full = take(1)[0], take(len(extra)), refs.pop(0)

        def code(bits, delta):
            return sum((c.bit[b] if not delta >> i & 1 else 1 - c.bit[b]) * (1 << i) for i, b in enumerate(bits))

        lo = [0]
        for k, b in enumerate(stages):
            lo.append(lo[k] + code(b, 0) * n[k + 1])
        at = lambda k: pl.ds(pl.multiple_of(lo[k], n[k]) if k else 0, n[k])
        theirs = lambda k, d: pl.ds(pl.multiple_of(lo[k] + code(stages[k], d) * n[k + 1], n[k + 1]), n[k + 1])

        def scatter(g, bufs, k):
            return [c.copy(lambda d=d: g().at[theirs(k, d)], lambda d=d: bufs[d - 1], (stages[k], d)) for d in range(1, len(bufs) + 1)]

        s_own = [scatter(own, r_own[k], k) for k in range(S)]
        s_peer = [scatter(peer, r_peer[k], k) for k in range(pre)]
        s_t = c.copy(lambda: peer().at[at(pre)], lambda: r_t, "t")
        s_x = [c.copy(lambda: own().at[at(S)], lambda i=i: r_x[i], ([b], 1), False) for i, b in enumerate(extra)]
        s_g = [[c.copy(lambda k=k: full.at[at(k + 1)], lambda k=k: full.at[at(k + 1)], (stages[k], d)) for d in range(1, 1 << len(stages[k]))]
               for k in range(S)]
        s_out = c.here(lambda: full, lambda: out())
        self.wait_out = lambda: s_out().wait()
        start = lambda ss: [s().start() for s in ss]
        arrived = lambda ss: [s().wait_recv() for s in ss]

        def end(s, g, buf, k):
            arrived(s[k])
            add_rows(g(), buf[k], lo[k + 1], n[k + 1], cols)

        def peer_step(i):
            if i:
                end(s_peer, peer, r_peer, i - 1)
            start(s_peer[i] if i < pre else [s_t])

        def own_step(i):
            if i == 0:
                start(s_own[0])
            elif i <= S:
                end(s_own, own, r_own, i - 1)
                if i == pre:
                    assert not self.peer_steps
                    s_t().wait_recv()
                    add_rows(own(), [r_t], lo[pre], n[pre], cols)
                if i < S:
                    start(s_own[i])
                    return
                for j in range(len(extra)):
                    s_x[j]().start()
                    s_x[j]().wait()
                    add_rows(own(), [r_x[j]], lo[S], n[S], cols)
                full[at(S), :] = own()[at(S), :]
                start(s_g[S - 1])
            else:
                k = 2 * S - i
                arrived(s_g[k])
                if k:
                    start(s_g[k - 1])
                else:
                    s_out().start()

        self.peer_steps = [lambda i=i: peer_step(i) for i in range(pre + 1)]
        self.own_steps = [lambda i=i: own_step(i) for i in range(2 * S + 1)]

    def own(self):
        self.own_steps.pop(0)()

    def peer(self):
        self.peer_steps.pop(0)()


SMALL_STAGES = [[1], [2], [4, 8]]


class Small:
    def __init__(self, c, sm, bufs):
        bufs = list(bufs)
        r_t = bufs.pop(0)
        st = SMALL_STAGES + [[b] for b in c.levels[4:]]
        s_t = [c.copy(lambda: sm.at[0:8], lambda: r_t.at[0:8], "t", False), c.copy(lambda: sm.at[16:24], lambda: r_t.at[8:16], "t", False)]
        rs, ss = [[r_t]], [s_t]
        for bits in st:
            r = [bufs.pop(0) for _ in range((1 << len(bits)) - 1)]
            rs.append(r)
            ss.append([c.copy(lambda: sm.at[0:16], lambda b=b: b, (bits, d + 1), False) for d, b in enumerate(r)])

        def step(i):
            if i:
                for s in ss[i - 1]:
                    s().wait()
                sm[0:16, :] = pairwise([sm[0:16, :]] + [r[...] for r in rs[i - 1]])
            if i < len(ss):
                for s in ss[i]:
                    s().start()

        self.steps = [lambda i=i: step(i) for i in range(len(ss) + 1)]

    def own(self):
        self.steps.pop(0)()


INS = ["x_h", "cot_h", "hw_h", "ow_h", "uw_h", "dw_h", "ns", "nsh", "qb_o", "vb_o", "ob", "ub_o", "db"]
OUTS = ["lo_h", "ig_h", "FH_h", "FO_h", "FU_h", "FD_h", "smo"]
Y4, Z14, G8 = [[1], [2], [4, 8]], [[1], [4], [2], [8]], [[1], [2, 4, 8]]
JOBS = [("D0", 512, 512, [[1], [2], [4, 8]], 1),
        ("U0", 512, 512, [[1], [2], [4, 8]], 2),
        ("D1", 512, 512, [[1], [2], [4, 8]], 1),
        ("U1", 512, 512, [[1], [2], [4, 8]], 2),
        ("O", 256, 512, [[1], [2], [4, 8]], 1),
        ("H0", 768, 128, [[1], [2], [4, 8]], 1),
        ("H1", 768, 128, [[1], [2], [4, 8]], 2),
        ("H2", 768, 128, [[1], [2], [4, 8]], 1),
        ("H3", 768, 128, [[1], [2], [4, 8]], 2)]

HOOKS = {
    "f0_0": ["WhwA"],
    "f0_1": ["WhwB", "Wow"],
    "qkv1a": ["Wu0"],
    "f1_0": ["Wd0", "WhwB", "Wow"],
    "qkv1b": ["Wu1", "Wu0"],
    "f1_1": ["Wd0", "Wd1"],
    "ffn01_0": ["Wu1"],
    "dD01": ["D0p"],
    "dU01": ["Wd1", "U0p"],
    "ffn00_0": ["D0p"],
    "ffn00_1": ["U0p"],
    "dD00": ["D0o"],
    "dU00": ["U0o"],
    "ffn11_1": ["U0o"],
    "dD11": ["U0p", "D1p"],
    "dU11": ["U1p"],
    "ffn10_0": ["D0o", "D1p", "U1p"],
    "dD10": ["D1o"],
    "dU10": ["U0o", "U1o"],
    "dO1": ["Op"],
    "gm": ["D0o", "U1o", "Op"],
    "b1_0": ["H0p"],
    "b1_1": ["U0o", "U1p", "D1o", "H1p", "H0p"],
    "b1_2": ["Oo", "D0o", "H1p"],
    "b1_3": ["Oo", "H2p", "U1o", "H3p", "D1o"],
    "b0_0": ["H2p", "H1p", "H3p", "H0o"],
    "b0_1": ["H0o", "Oo", "H1o", "D0o"],
    "b0_2": ["H1o", "H2o", "U0o", "H3p", "U1o"],
    "b0_3": ["H3o", "H2o", "D1o"],
    "gin0": ["Oo", "D0o", "H3o"],
    "gin1": ["H1o", "H0o"],
    "gin2": ["D0o"],
    "gin3": ["U1o", "So"],
    "fo1": ["U0o"],
    "fo3": ["H2o"],
    "tail": ["So", "D1o", "U0o", "H3o", "So", "Oo", "H1o", "U1o", "H0o", "H2o", "U1o", "H3o", "H1o", "So", "D1o", "H0o", "Oo", "D1o", "H2o", "Oo", "H1o", "H3o", "H0o", "H1o", "H2o", "H0o", "So", "H3o", "H2o", "H3o"],
}
BEFORE = {
    "qkv1a": ["WhwA"],
}

GROUPS = [g for g in ([4, 8], [2, 4, 8]) if any(g in st for _, _, _, st, _ in JOBS) or g in SMALL_STAGES]


def scratch(T, ndp):
    nb = T // BLK
    V = pltpu.VMEM
    lv = ndp.bit_length() - 1
    s = dict(
        x=V((T, D), BF16), cot=V((T, D), BF16), hw=V((2, 3, D, HALF), BF16), ow=V((2, HALF, D), BF16),
        uw=V((2, D, FH), BF16), dw=V((2, FH, D), BF16),
        qb_p=V((1, HALF), F32), vb_p=V((1, HALF), F32), ub_p=V((1, FH), F32),
        n1T=V((D, T), BF16), qT=V((2, HALF, T), BF16), kT=V((2, HALF, T), BF16), vT=V((2, NH, 80, T), BF16),
        E=V((2 * NH, BLK * nb * (nb + 1) // 2, BLK), BF16), rl=V((2 * NH, 1, T), F32), mixT=V((2, HALF, T), BF16),
        res=V((T, D), F32), n2=V((T, D), BF16), act=V((2, T, FH), BF16), dpre=V((2, T, FH), BF16),
        oacc=V((T, D), F32), g2=V((T, D), F32), br=V((T, D), BF16), gmT=V((2, HALF, T), BF16),
        dh=V((3 * HD, T), BF16), dva=V((HD, T), F32), dka=V((HD, T), F32), sm=V((24, D), F32),
        GD0o=V((FH // 2, D), BF16), GD0p=V((FH // 2, D), BF16), GD1o=V((FH // 2, D), BF16), GD1p=V((FH // 2, D), BF16),
        GU0o=V((D, FH // 2), BF16), GU0p=V((D, FH // 2), BF16), GU1o=V((D, FH // 2), BF16), GU1p=V((D, FH // 2), BF16),
        GOo=V((HALF, D), BF16), GOp=V((HALF, D), BF16), GHo=V((NH, 768, 128), BF16), GHp=V((NH, 768, 128), BF16),
        s0=V((16, D), F32))
    for i in range(5 + lv - 4):
        s[f"s{i + 1}"] = V((16, D), F32)
    for name, rows, cols, stages, pre in JOBS:
        for i, v in enumerate(job_scratch(rows, cols, stages, pre, lv - 4)):
            s[f"{name}_{i}"] = v
    s["send"] = pltpu.SemaphoreType.DMA((224 + 24 * (lv - 4),))
    s["recv"] = pltpu.SemaphoreType.DMA((224 + 24 * (lv - 4),))
    s["local"] = pltpu.SemaphoreType.DMA((32,))
    return s


def run(z, ndp):
    c = Comm(ndp, GROUPS, z.send, z.recv, z.local)
    lv = c.levels
    c.barrier_signal()
    slot0 = lambda r: r.at[0]
    loads = {n: c.here(lambda n=n: getattr(z, n + "_h"), lambda n=n, d=d: d(getattr(z, n)))
             for n, d in (("x", lambda r: r), ("hw", slot0), ("cot", lambda r: r), ("ow", slot0), ("uw", slot0), ("dw", slot0))}
    for n in ("x", "hw", "ow", "cot", "uw", "dw"):
        loads[n]().start()

    pieces = {"hwA": ("hw", D, 0, slice(0, 128)), "hwB": ("hw", D, 0, slice(128, 256)), "ow": ("ow", HALF, 0, slice(None)),
              "u0": ("uw", D, 0, slice(0, 512)), "d0": ("dw", 512, 0, slice(None)), "u1": ("uw", D, 0, slice(512, 1024)),
              "d1": ("dw", 512, 512, slice(None))}

    def view(name, flip, lead):
        n, m, base, cols = pieces[name]
        q = (c.bit[1] if not flip & 1 else 1 - c.bit[1]) + 2 * (c.bit[2] if not flip & 2 else 1 - c.bit[2])
        rows = pl.ds(pl.multiple_of(base + q * (m // 4), m // 4), m // 4)
        r = getattr(z, n).at[1] if lead else getattr(z, n + "_h")
        return r.at[:, rows, cols] if n == "hw" else r.at[rows, cols]

    W = {}
    for name in pieces:
        put = lambda flip, name=name: view(name, flip, True)
        W[name] = dict(
            x=c.copy(lambda name=name: view(name, 0, False), lambda put=put: put(0), "t"),
            s=c.copy(lambda put=put: put(0), lambda put=put: put(0), ([1], 1)),
            y=c.copy(lambda put=put: put(0), lambda put=put: put(0), ([2], 1)),
            r=c.copy(lambda put=put: put(2), lambda put=put: put(2), ([1], 1)))
    wb = [c.copy(lambda n=n: getattr(z, n + "_o"), lambda n=n: getattr(z, n + "_p"), "t") for n in ("qb", "vb", "ub")]

    def relay1(n):
        W[n]["x"]().wait_recv()
        W[n]["y"]().start()
        W[n]["s"]().start()

    def relay2(n):
        W[n]["y"]().wait_recv()
        W[n]["r"]().start()

    def arrive(n):
        W[n]["s"]().wait_recv()
        W[n]["r"]().wait_recv()

    c.barrier_wait()
    W["hwA"]["x"]().start()
    for b in wb:
        b().start()
    for n in list(pieces)[1:]:
        W[n]["x"]().start()

    z.qb, z.vb, z.ub = (z.qb_o, z.qb_p), (z.vb_o, z.vb_p), (z.ub_o, z.ub_p)
    z.GD = ((z.GD0o, z.GD0p), (z.GD1o, z.GD1p))
    z.GU = ((z.GU0o, z.GU0p), (z.GU1o, z.GU1p))
    z.GO, z.GH = (z.GOo, z.GOp), (z.GHo, z.GHp)
    z.dT, z.lo, z.ig = z.dpre, z.br, z.n2
    ends = dict(D0=lambda: z.FD_h.at[0 : FH // 2], D1=lambda: z.FD_h.at[FH // 2 : FH], U0=lambda: z.FU_h.at[:, 0 : FH // 2],
                U1=lambda: z.FU_h.at[:, FH // 2 : FH], O=lambda: z.FO_h)
    srcs = dict(D0=(lambda: z.GD0o, lambda: z.GD0p), D1=(lambda: z.GD1o, lambda: z.GD1p), U0=(lambda: z.GU0o, lambda: z.GU0p),
                U1=(lambda: z.GU1o, lambda: z.GU1p), O=(lambda: z.GOo, lambda: z.GOp))
    for i in range(NH):
        ends[f"H{i}"] = lambda i=i: z.FH_h.at[i]
        srcs[f"H{i}"] = (lambda i=i: z.GHo.at[i], lambda i=i: z.GHp.at[i])
    jobs = {}
    for name, rows, cols, stages, pre in JOBS:
        refs = [getattr(z, f"{name}_{i}") for i in range(len(job_scratch(rows, cols, stages, pre, len(lv) - 4)))]
        jobs[name] = Job(c, *srcs[name], refs, rows, cols, stages, pre, ends[name])
    jobs["S"] = small = Small(c, z.sm, [getattr(z, f"s{i}") for i in range(6 + len(lv) - 4)])
    s_lo, s_ig = c.here(lambda: z.lo, lambda: z.lo_h), c.here(lambda: z.ig, lambda: z.ig_h)

    relays = {n: [relay1, relay2] for n in W}

    def go(words):
        for word in words:
            if word[1:] in relays:
                relays[word[1:]].pop(0)(word[1:])
            else:
                (jobs[word[:-1]].own if word[-1] == "o" else jobs[word[:-1]].peer)()

    def at(name, n):
        table = {k: HOOKS.get(f"{name}_{k}", ()) for k in (range(n) if isinstance(n, int) else n)}

        def hook(h):
            for k, what in table.items():
                if what:
                    @pl.when(h == k)
                    def _():
                        go(what)
        return hook

    def before(name):
        go(BEFORE.get(name, ()))

    def after(name):
        go(HOOKS.get(name, ()))

    z.sm[...] = jnp.zeros_like(z.sm)
    loads["x"]().wait()
    ln1(z)
    loads["hw"]().wait()
    qkv(z, 0, 0, NH)
    after("qkv0")
    attn_fwd(z, 0, 0, NH, at("f0", NH // 2))
    before("qkv1a")
    for b in wb:
        b().wait_recv()
    arrive("hwA")
    qkv(z, 1, 0, 2)
    after("qkv1a")
    attn_fwd(z, 1, 0, 2, at("f1", range(0, 1)))
    before("qkv1b")
    arrive("hwB")
    qkv(z, 1, 2, 4)
    after("qkv1b")
    attn_fwd(z, 1, 2, 4, at("f1", range(1, 2)))
    before("out")
    arrive("ow")
    loads["ow"]().wait()
    out_proj(z)
    for n in ("cot", "uw", "dw"):
        loads[n]().wait()
    after("out")
    for part in (0, 1):
        for s in (1, 0):
            name = f"ffn{part}{s}"
            before(name + "_0")
            if s:
                arrive(f"u{part}")
                arrive(f"d{part}")
            ffn(z, part, s, at(name, z.nb // 2))
            d_down(z, part, s)
            after(f"dD{part}{s}")
            d_up(z, part, s)
            if part:
                d_upb(z, s)
            after(f"dU{part}{s}")
    for s in (1, 0):
        d_out(z, s)
        after(f"dO{s}")
    grad_mixed(z, 1)
    grad_mixed(z, 0)
    after("gm")
    attn_bwd(z, 1, at("b1", NH))
    attn_bwd(z, 0, at("b0", NH))
    d_headb(z, 0)
    d_headb(z, 1)
    after("hb")
    c.drain(31)
    grad_in(z, after)
    s_ig().start()
    for r in range(z.nb):
        ffn_out(z, (r,))
        after(f"fo{r}")
    s_lo().start()
    after("tail")
    while small.steps:
        small.own()
    assert not any(v for v in relays.values()) and not any(jobs[n].own_steps for n in jobs if n != "S")
    z.smo[...] = z.sm[0:16, :]
    s_ig().wait()
    s_lo().wait()
    for n in jobs:
        if n != "S":
            jobs[n].wait_out()
    c.drain()


def main_call(args, T, ndp):
    scr = scratch(T, ndp)
    names = INS + OUTS + list(scr)

    def kernel(*refs):
        z = Refs()
        for n, r in zip(names, refs):
            setattr(z, n, r)
        z.nb = T // BLK
        run(z, ndp)

    S = jax.ShapeDtypeStruct
    outs = [S((T, D), BF16), S((T, D), BF16), S((NH, 768, 128), BF16), S((HALF, D), BF16), S((D, FH), BF16), S((FH, D), BF16),
            S((16, D), F32)]
    vm, hbm = pl.BlockSpec(memory_space=pltpu.VMEM), pl.BlockSpec(memory_space=pl.ANY)
    return pl.pallas_call(
        kernel, out_shape=outs, in_specs=[hbm] * 6 + [vm] * 7, out_specs=[hbm] * 6 + [vm], scratch_shapes=list(scr.values()),
        compiler_params=pltpu.CompilerParams(vmem_limit_bytes=VMEM_BYTES, collective_id=0, has_side_effects=True),
        name="layer")(*args)


def widen(FH_, FO_, FU_, FD_, sm, lo, ig):
    def kernel(h, o, u, d, m, l, g, ho, oo, uo, do, lo_, go, sc, sh, qb, vb, ob, ub, db, hv, ov, uv, dv, lv, gv, hf, of, uf, df, si, so):
        ins, outs = [], []

        def load(src, dst):
            c = pltpu.make_async_copy(src, dst, si.at[len(ins)])
            ins.append(c)
            c.start()
            return c

        def store(src, dst):
            c = pltpu.make_async_copy(src, dst, so.at[len(outs)])
            outs.append(c)
            c.start()

        top, bottom = slice(0, 512), slice(512, 1024)
        left, right = slice(0, 256), slice(256, 512)
        i_g, i_l = load(g, gv), load(l, lv)
        i_d0, i_h = load(d.at[top], dv.at[top]), load(h, hv)
        i_d1 = load(d.at[bottom], dv.at[bottom])
        i_u0, i_u1 = load(u.at[left], uv.at[left]), load(u.at[right], uv.at[right])
        i_o = load(o, ov)
        sc[...] = m[0:2, :]
        sh[...] = m[2:4, :]
        qb[...] = m[8:9, 0:HALF]
        vb[...] = m[8:9, HALF:D]
        ob[...] = m[4:5, :]
        ub[:, 0:D] = m[9:10, :]
        ub[:, D:FH] = m[10:11, :]
        db[...] = m[5:6, :]
        i_g.wait()
        store(gv, go)
        i_l.wait()
        store(lv, lo_)

        def piece(c, v, f, out, rows):
            c.wait()
            f[rows, :] = v[rows, :].astype(F32)
            store(f.at[rows], out.at[rows])

        piece(i_d0, dv, df, do, top)
        i_h.wait()
        for j in range(3):
            for q in range(4):
                for p in range(2):
                    rows = [hv[2 * p + i, q * 192 + j * HD : q * 192 + (j + 1) * HD, :] for i in range(2)]
                    hf[j, q * 128 : (q + 1) * 128, p * 128 : (p + 1) * 128] = jnp.concatenate(rows, 0).astype(F32).T
            store(hf.at[j], ho.at[j])
        piece(i_d1, dv, df, do, bottom)
        piece(i_u0, uv, uf, uo, left)
        piece(i_u1, uv, uf, uo, right)
        piece(i_o, ov, of, oo, left)
        for c in outs:
            c.wait()

    S, V = jax.ShapeDtypeStruct, pltpu.VMEM
    vm, hbm = pl.BlockSpec(memory_space=pltpu.VMEM), pl.BlockSpec(memory_space=pl.ANY)
    big = [(3, D, HALF), (HALF, D), (D, FH), (FH, D)]
    small = [(2, D), (2, D), (1, HALF), (1, HALF), (1, D), (1, FH), (1, D)]
    rows = S(lo.shape, BF16)
    out_shape = [S(t, F32) for t in big] + [rows, rows] + [S(t, F32) for t in small]
    bufs = [V((NH, 768, 128), BF16)] + [V(t, BF16) for t in big[1:]] + [V(lo.shape, BF16)] * 2 + [V(t, F32) for t in big]
    return pl.pallas_call(
        kernel, out_shape=out_shape, in_specs=[hbm] * 4 + [vm] + [hbm] * 2, out_specs=[hbm] * 6 + [vm] * 7,
        scratch_shapes=bufs + [pltpu.SemaphoreType.DMA((8,)), pltpu.SemaphoreType.DMA((10,))],
        compiler_params=pltpu.CompilerParams(vmem_limit_bytes=VMEM_BYTES), name="widen")(FH_, FO_, FU_, FD_, sm, lo, ig)


def solution(mesh):
    ndp = mesh.shape["dp"]

    def local(inputs, norm_scale, norm_shift, head_weight, query_bias, value_bias, out_weight, out_bias, up_weight, up_bias,
              down_weight, down_bias, cotangent):
        row = lambda b: b.reshape(1, b.shape[0])
        args = (inputs, cotangent, head_weight, out_weight, up_weight, down_weight, norm_scale, norm_shift, row(query_bias),
                row(value_bias), row(out_bias), row(up_bias), row(down_bias))
        lo, ig, gh, go, gu, gd, sm = main_call(args, inputs.shape[0], ndp)
        gh, go, gu, gd, lo, ig, sc, sh, qb, vb, ob, ub, db = widen(gh, go, gu, gd, sm, lo, ig)
        flat = lambda v: v.reshape(v.shape[1])
        return (lo, ig, sc, sh, gh, flat(qb), flat(vb), go, flat(ob), gu, flat(ub), gd, flat(db))

    rows, t0, t1 = P(("dp", "tensor"), None), P("tensor"), P(None, "tensor")
    tc = P("tensor", None)
    in_specs = (rows, P(), P(), P(None, None, "tensor"), t0, t0, tc, P(), t1, t0, tc, P(), rows)
    out_specs = (rows, rows, P(), P(), P(None, None, "tensor"), t0, t0, tc, P(), t1, t0, tc, P())
    return jax.shard_map(local, mesh=mesh, in_specs=in_specs, out_specs=out_specs, check_vma=False)
```
